32 devices in a mesh: blk: 4 (over z), acc: 4 (over x, core), tail: 2 (over y).
Axes of the slice: x: 2, y: 2, z: 4, core: 2. Of those that a mesh axis runs over, the one named last changes fastest.
Arguments:
- reciprocal_spectra: float32 [4, 2, 64, 4096], P(None, None, 'acc'), may hold values from -6 to 6
- divisor: float32 [8, 131072], P(('blk', 'tail'), 'acc'), may hold values from -1 to 1
Outputs:
- middle_product: float32 [8, 131072], P(('blk', 'tail'), 'acc')
The draws below stay inside these ranges and needn't reach their ends.
All inputs are finite; a program needn't handle non-finite values.
Results may differ from the reference program's by a relative error of at most 0.0003.
Values sent between devices are 32-bit elements; how exact they have to be, the bound alone decides.
No kernel may reach another device: no remote copies, remote signals or barrier semaphores. Data moves between devices by JAX's collectives and lax.ppermute only.
A program may use at most 64 MiB of HBM per device.

```python
import jax
import jax.numpy as jnp
from jax import lax

RADIX = 64
ROUNDS = 4
LIMBS = 131072
NBLOCKS = 8
STRIDE = 2


def steps_of(own_key, extent, split, smallest, largest):
    factor_of, own = 1.0, jax.random.fold_in(own_key, 6)
    for dim, parts in split:
        steps = jnp.exp(jax.random.uniform(jax.random.fold_in(own, dim), (parts,), jnp.float32, smallest / len(split), largest / len(split)))
        factor_of = factor_of * jnp.repeat(steps, extent[dim] // parts).reshape([-1 if axis == dim else 1 for axis in range(len(extent))])
    return factor_of


def centred(stream_key, extent, width, bound, pieces=(), held_as=jnp.bfloat16):
    result = jax.random.normal(stream_key, extent, jnp.float32) * width
    if len(pieces) > 0:
        result = steps_of(stream_key, extent, pieces, -0.22, 0.18) * result
    return jnp.clip(result, min=-bound, max=bound).astype(held_as)


def setup_inputs(seed: int = 0) -> dict:
    key_of = jax.random.split(jax.random.key(seed), 3)
    reciprocal_spectra = centred(key_of[0], (ROUNDS, 2, RADIX, RADIX * RADIX), 1.0, 6.0, ((2, 4),), jnp.float32)
    divisor = jnp.clip(jax.random.uniform(key_of[1], (NBLOCKS, LIMBS), jnp.float32, -1.0, 1.0) * steps_of(key_of[1], (NBLOCKS, LIMBS), ((0, 8), (1, 4)), -0.4, 0.0), -1.0, 1.0)
    return dict(reciprocal_spectra=reciprocal_spectra, divisor=divisor)


def reference(reciprocal_spectra, divisor):
    length = RADIX ** 3
    ordered = reciprocal_spectra.reshape(ROUNDS, 2, RADIX, RADIX, RADIX).transpose(0, 1, 4, 3, 2).reshape(ROUNDS, 2, length)
    recip_full = ordered[:, 0] + 1j * ordered[:, 1]
    divisor_spectra = jnp.fft.fft(divisor, n=length, axis=-1)

    def one_block(block_index):
        total = jnp.zeros((length,), divisor_spectra.dtype)
        for step_index in range(ROUNDS):
            source = (block_index - step_index * STRIDE) % NBLOCKS
            picked = lax.dynamic_index_in_dim(divisor_spectra, source, 0, keepdims=False)
            total = total + recip_full[step_index] * picked
        return jnp.real(jnp.fft.ifft(total)).astype(jnp.float32)

    block_products = lax.map(one_block, jnp.arange(NBLOCKS, dtype=jnp.int32))
    lower_part = block_products[:, :LIMBS]
    upper_part = block_products[:, LIMBS:]
    return (lower_part + jnp.roll(upper_part, 1, axis=0)).astype(jnp.float32)
```

```python
import math

import jax
import jax.numpy as jnp
import numpy as np
from jax import lax
from jax.experimental import pallas as pl
from jax.experimental.pallas import tpu as pltpu
from jax.sharding import PartitionSpec as P


LANES = 128


class Plan:
    def __init__(self, freq_rows, plane, quarters, groups, rounds):
        self.rounds = rounds
        self.quarters = quarters
        self.groups = groups
        self.freq_rows = freq_rows
        self.radix = freq_rows * quarters
        self.plane = plane
        self.length = self.radix * plane
        self.side = math.isqrt(self.length)
        self.m_los = self.side // self.radix
        self.m_his = self.radix // self.m_los
        self.rows = self.m_los * freq_rows
        self.n1s = self.side // 2
        self.chunk = self.n1s // quarters
        self.cols = self.side // LANES
        self.slice_rows = self.rows // groups
        self.per = groups // self.m_los


def tables(plan):
    row = (np.arange(plan.m_los)[:, None] * plan.radix + np.arange(plan.freq_rows)[None, :]).reshape(-1)
    part = np.arange(plan.quarters) * plan.freq_rows
    n1 = np.arange(plan.n1s)
    n2 = np.arange(plan.side)
    f2 = (np.arange(plan.m_his)[:, None] + plan.m_los * np.arange(plan.radix)[None, :]).reshape(-1)

    def wave(first, second, modulus):
        angle = (first[:, None] * second[None, :] % modulus) * (-2.0 * math.pi / modulus)
        return np.stack([np.cos(angle), np.sin(angle)])

    first_rows = wave(row, n1, plan.side)
    first_part = wave(part, n1, plan.side)
    twist_rows = wave(row, n2, plan.length)
    twist_part = wave(part, n2, plan.length)
    second = wave(n2, f2, plan.side)
    second[1] *= -1.0
    second_high = second.astype(jnp.bfloat16)
    second_low = (second - second_high.astype(np.float64)).astype(jnp.bfloat16)
    single = lambda value: value.astype(np.float32)
    return (
        single(first_rows),
        single(first_part.transpose(1, 0, 2)),
        single(twist_rows),
        single(twist_part.transpose(1, 0, 2)),
        np.stack([second_high, second_low]),
    )


def split(value):
    high = value.astype(jnp.bfloat16)
    low = (value - high.astype(jnp.float32)).astype(jnp.bfloat16)
    return high, low


def product(first, second, transposed=False):
    dims = (((1,), (1 if transposed else 0,)), ((), ()))
    dot = lambda a, b: lax.dot_general(a, b, dims, preferred_element_type=jnp.float32)
    return dot(first[0], second[0]) + (dot(first[1], second[0]) + dot(first[0], second[1]))


def prepare(plan):
    def kernel(at, first_rows, first_part, twist_rows, twist_part, spectra, first, last, twist, own, held, sems):
        place = at[0]
        m_lo = at[1]
        lane_at = m_lo * plan.radix
        copies = []
        for m_hi in range(plan.m_his):
            start = pl.multiple_of((m_hi * plan.m_los * plan.radix + lane_at) // LANES * LANES, LANES)
            copy = pltpu.make_async_copy(spectra.at[:, :, pl.ds(start, LANES)], held.at[m_hi], sems.at[m_hi])
            copy.start()
            copies.append(copy)
        part_cos = first_part[pl.ds(place, 1), 0, :]
        part_sin = first_part[pl.ds(place, 1), 1, :]
        real = first_rows[0] * part_cos - first_rows[1] * part_sin
        imag = first_rows[0] * part_sin + first_rows[1] * part_cos
        both = jnp.concatenate([real, imag], axis=0)
        first[0], first[1] = split(both)
        last[0], last[1] = split(both.T)
        part_cos = twist_part[pl.ds(place, 1), 0, :]
        part_sin = twist_part[pl.ds(place, 1), 1, :]
        twist[0] = twist_rows[0] * part_cos - twist_rows[1] * part_sin
        twist[1] = twist_rows[0] * part_sin + twist_rows[1] * part_cos
        for copy in copies:
            copy.wait()
        lane = lax.broadcasted_iota(jnp.int32, (plan.freq_rows, LANES), 1)
        within = lane_at % LANES
        each = LANES // plan.radix
        scale = 1.0 / plan.length
        for index in range(2 * plan.rounds):
            for column in range(plan.side // LANES):
                value = jnp.zeros((plan.freq_rows, LANES), jnp.float32)
                for piece in range(each):
                    turned = pltpu.roll(held[column * each + piece, index], (piece * plan.radix - within) % LANES, 1)
                    inside = (lane >= piece * plan.radix) & (lane < (piece + 1) * plan.radix)
                    value = jnp.where(inside, turned, value)
                own[index, :, column * LANES : (column + 1) * LANES] = value * scale

    vmem = pl.BlockSpec(memory_space=pltpu.VMEM)
    width = 2 * plan.rows
    return pl.pallas_call(
        kernel,
        out_shape=(
            jax.ShapeDtypeStruct((2, width, plan.n1s), jnp.bfloat16),
            jax.ShapeDtypeStruct((2, plan.n1s, width), jnp.bfloat16),
            jax.ShapeDtypeStruct((2, plan.rows, plan.side), jnp.float32),
            jax.ShapeDtypeStruct((2 * plan.rounds, plan.freq_rows, plan.side), jnp.float32),
        ),
        in_specs=[pl.BlockSpec(memory_space=pltpu.SMEM)] + [vmem] * 4 + [pl.BlockSpec(memory_space=pl.ANY)],
        out_specs=(vmem,) * 4,
        scratch_shapes=[
            pltpu.VMEM((plan.m_his, 2 * plan.rounds, plan.freq_rows, LANES), jnp.float32),
            pltpu.SemaphoreType.DMA((plan.m_his,)),
        ],
        cost_estimate=pl.CostEstimate(flops=8_000_000, bytes_accessed=2_000_000, transcendentals=0),
        name="prepare",
    )


def forward(plan):
    def kernel(at, *refs):
        limbs = refs[: plan.quarters]
        first, twist, second, out, matrix = refs[plan.quarters :]
        place = at[0]
        for index in range(plan.quarters):
            start = pl.multiple_of((place ^ index) * plan.chunk, 8)
            for column in range(plan.cols):
                matrix[pl.ds(start, plan.chunk), column * LANES : (column + 1) * LANES] = limbs[index][
                    pl.ds(column, plan.chunk, stride=plan.cols), :
                ]
        value = product((first[0], first[1]), split(matrix[...]))
        real, imag = value[: plan.rows], value[plan.rows :]
        turned = jnp.concatenate([real * twist[0] - imag * twist[1], real * twist[1] + imag * twist[0]], axis=0)
        turned = split(turned)
        by_cos = product(turned, (second[0, 0], second[1, 0]))
        by_sin = product(turned, (second[0, 1], second[1, 1]))
        real = by_cos[: plan.rows] + by_sin[plan.rows :]
        imag = by_cos[plan.rows :] - by_sin[: plan.rows]
        for group in range(plan.groups):
            out[group, 0] = real[group * plan.slice_rows : (group + 1) * plan.slice_rows]
            out[group, 1] = imag[group * plan.slice_rows : (group + 1) * plan.slice_rows]

    vmem = pl.BlockSpec(memory_space=pltpu.VMEM)
    return pl.pallas_call(
        kernel,
        out_shape=jax.ShapeDtypeStruct((plan.groups, 2, plan.slice_rows, plan.side), jnp.float32),
        in_specs=[pl.BlockSpec(memory_space=pltpu.SMEM)] + [vmem] * (plan.quarters + 3),
        out_specs=vmem,
        scratch_shapes=[pltpu.VMEM((plan.n1s, plan.side), jnp.float32)],
        name="forward",
    )


def combine(plan, stride):
    def kernel(at, spectra, own, out):
        first_row = at[2]
        row = lax.broadcasted_iota(jnp.int32, (plan.slice_rows, plan.side), 0) + first_row
        sign = jnp.where(row % 2 == 0, 1.0, -1.0)

        def one_block(block, carry):
            real = jnp.zeros((plan.slice_rows, plan.side), jnp.float32)
            imag = jnp.zeros((plan.slice_rows, plan.side), jnp.float32)
            for step in range(plan.rounds):
                here = lax.rem(block + (plan.rounds * stride * plan.groups - step * stride), plan.groups)
                before = lax.rem(here + (plan.groups - 1), plan.groups)
                left = spectra[here, 0] + sign * spectra[before, 0]
                right = spectra[here, 1] + sign * spectra[before, 1]
                real = real + own[2 * step] * left - own[2 * step + 1] * right
                imag = imag + own[2 * step] * right + own[2 * step + 1] * left
            out[block, 0] = real
            out[block, 1] = imag
            return carry

        lax.fori_loop(0, plan.groups, one_block, 0)

    vmem = pl.BlockSpec(memory_space=pltpu.VMEM)
    return pl.pallas_call(
        kernel,
        out_shape=jax.ShapeDtypeStruct((plan.groups, 2, plan.slice_rows, plan.side), jnp.float32),
        in_specs=[pl.BlockSpec(memory_space=pltpu.SMEM), vmem, vmem],
        out_specs=vmem,
        name="combine",
    )


def backward(plan):
    def kernel(at, spectra, last, twist, second, out, matrix):
        place = at[0]
        both = [
            jnp.concatenate([spectra[group, part] for group in range(plan.groups)], axis=0) for part in range(2)
        ]
        value = split(jnp.concatenate(both, axis=0))
        by_cos = product(value, (second[0, 0], second[1, 0]), True)
        by_sin = product(value, (second[0, 1], second[1, 1]), True)
        real = by_cos[: plan.rows] - by_sin[plan.rows :]
        imag = by_cos[plan.rows :] + by_sin[: plan.rows]
        turned = jnp.concatenate([real * twist[0] + imag * twist[1], imag * twist[0] - real * twist[1]], axis=0)
        matrix[...] = product((last[0], last[1]), split(turned))
        for index in range(plan.quarters):
            start = pl.multiple_of((place ^ index) * plan.chunk, 8)
            for column in range(plan.cols):
                out[index, pl.ds(column, plan.chunk, stride=plan.cols), :] = matrix[
                    pl.ds(start, plan.chunk), column * LANES : (column + 1) * LANES
                ]

    vmem = pl.BlockSpec(memory_space=pltpu.VMEM)
    return pl.pallas_call(
        kernel,
        out_shape=jax.ShapeDtypeStruct((plan.quarters, plan.chunk * plan.cols, LANES), jnp.float32),
        in_specs=[pl.BlockSpec(memory_space=pltpu.SMEM)] + [vmem] * 4,
        out_specs=vmem,
        scratch_shapes=[pltpu.VMEM((plan.n1s, plan.side), jnp.float32)],
        name="backward",
    )


def swapped(value, bit):
    count = lax.axis_size("acc")
    return lax.ppermute(value, "acc", [(source, source ^ bit) for source in range(count)])


STRIDE = 2


def per_device(reciprocal_spectra, divisor):
    rounds, _, freq_rows, plane = reciprocal_spectra.shape
    quarters = lax.axis_size("acc")
    groups = lax.axis_size("blk") * lax.axis_size("tail")
    plan = Plan(freq_rows, plane, quarters, groups, rounds)
    place = lax.axis_index("acc")
    group = lax.axis_index(("blk", "tail"))
    first_row = group % plan.per * plan.slice_rows
    at = jnp.stack([place, group // plan.per, first_row + place * freq_rows]).astype(jnp.int32)
    first_rows, first_part, twist_rows, twist_part, second = (jnp.asarray(table) for table in tables(plan))

    limbs = divisor.reshape(plan.chunk * plan.cols, LANES)
    pieces = {0: limbs}
    bit = quarters // 2
    while bit:
        pieces.update({index | bit: swapped(piece, bit) for index, piece in list(pieces.items())})
        bit //= 2
    spectra = reciprocal_spectra.reshape(2 * rounds, freq_rows, plane)
    first, last, twist, own = prepare(plan)(at, first_rows, first_part, twist_rows, twist_part, spectra)
    if plan.per > 1:
        own = lax.dynamic_slice_in_dim(own, first_row, plan.slice_rows, 1)

    own_spectrum = forward(plan)(at, *[pieces[index] for index in range(quarters)], first, twist, second)
    every = lax.all_to_all(own_spectrum, ("blk", "tail"), 0, 0, tiled=True)
    sums = combine(plan, STRIDE)(at, every, own)
    back = lax.all_to_all(sums, ("blk", "tail"), 0, 0, tiled=True)
    slots = backward(plan)(at, back, last, twist, second)

    held = {index: slots[index] for index in range(quarters)}
    bit = 1
    while bit < quarters:
        sent = sorted(index for index in held if index & bit)
        arrived = swapped(jnp.stack([held[index] for index in sent]), bit)
        held = {index ^ bit: held[index ^ bit] + arrived[where] for where, index in enumerate(sent)}
        bit *= 2
    return held[0].reshape(divisor.shape)


def solution(mesh):
    in_specs = (P(None, None, "acc", None), P(("blk", "tail"), "acc"))
    out_specs = P(("blk", "tail"), "acc")
    return jax.shard_map(
        per_device, mesh=mesh, in_specs=in_specs, out_specs=out_specs, check_vma=False
    )
```

```python
import math

import jax
import jax.numpy as jnp
import numpy as np
from jax import lax
from jax.experimental import pallas as pl
from jax.experimental.pallas import tpu as pltpu
from jax.sharding import PartitionSpec as P


LANES = 128
EXTRA = 8
GRANT = 16 * 1024 * 1024
STRIDE = 2


class Plan:
    def __init__(self, freq_rows, plane, quarters, groups, rounds):
        self.rounds = rounds
        self.quarters = quarters
        self.groups = groups
        self.freq_rows = freq_rows
        self.radix = freq_rows * quarters
        self.plane = plane
        self.length = self.radix * plane
        self.side = math.isqrt(self.length)
        self.half = self.side // 2
        self.m_los = self.side // self.radix
        self.m_his = self.radix // self.m_los
        self.rows = self.m_los * freq_rows
        self.n1s = self.side // 2
        self.chunk = self.n1s // quarters
        self.cols = self.side // LANES
        self.half_cols = self.half // LANES
        self.slice_rows = self.rows // groups
        self.per = groups // self.m_los
        self.packed = 2 * self.half_cols * self.slice_rows + EXTRA


def tables(plan):
    row = (np.arange(plan.m_los)[:, None] * plan.radix + np.arange(plan.freq_rows)[None, :]).reshape(-1)
    part = np.arange(plan.quarters) * plan.freq_rows
    n1 = np.arange(plan.n1s)
    n2 = np.arange(plan.side)
    f2 = (np.arange(plan.m_his)[:, None] + plan.m_los * np.arange(plan.radix // 2)[None, :]).reshape(-1)

    def wave(first, second, modulus):
        angle = (first[:, None] * second[None, :] % modulus) * (-2.0 * math.pi / modulus)
        return np.stack([np.cos(angle), np.sin(angle)])

    first_rows = wave(row, n1, plan.side)
    first_part = wave(part, n1, plan.side)
    twist_rows = wave(row, n2, plan.length)
    twist_part = wave(part, n2, plan.length)
    cosine, sine = wave(n2, f2, plan.side)
    second = np.concatenate([cosine, -sine], axis=1)
    second_high = second.astype(jnp.bfloat16)
    second_low = (second - second_high.astype(np.float64)).astype(jnp.bfloat16)
    single = lambda value: value.astype(np.float32)
    return (
        single(first_rows),
        single(first_part.transpose(1, 0, 2)),
        single(twist_rows),
        single(twist_part.transpose(1, 0, 2)),
        np.stack([second_high, second_low]),
    )


def far(value):
    return pltpu.with_memory_space_constraint(value, pltpu.HBM)


def split(value):
    high = value.astype(jnp.bfloat16)
    low = (value - high.astype(jnp.float32)).astype(jnp.bfloat16)
    return high, low


def product(first, second, transposed=False):
    dims = (((1,), (1 if transposed else 0,)), ((), ()))
    dot = lambda a, b: lax.dot_general(a, b, dims, preferred_element_type=jnp.float32)
    return dot(first[0], second[0]) + (dot(first[1], second[0]) + dot(first[0], second[1]))


def call(kernel, name, out_shape, memory, scratch=(), flops=1_000_000, moved=1_000_000):
    where = {"smem": pltpu.SMEM, "vmem": pltpu.VMEM, "hbm": pltpu.HBM}
    vmem = pl.BlockSpec(memory_space=pltpu.VMEM)
    return pl.pallas_call(
        kernel,
        out_shape=out_shape,
        in_specs=[pl.BlockSpec(memory_space=where[kind]) for kind in memory],
        out_specs=jax.tree.map(lambda _: vmem, out_shape),
        scratch_shapes=scratch,
        cost_estimate=pl.CostEstimate(flops=flops, bytes_accessed=moved, transcendentals=0),
        compiler_params=pltpu.CompilerParams(vmem_limit_bytes=GRANT),
        name=name,
    )


def fetch(plan, spectra, held, sems, m_lo):
    copies = []
    for m_hi in range(plan.m_his):
        start = pl.multiple_of((m_hi * plan.m_los + m_lo) * plan.radix // LANES * LANES, LANES)
        copies.append(pltpu.make_async_copy(spectra.at[:, :, pl.ds(start, LANES)], held.at[m_hi], sems.at[m_hi]))
        copies[-1].start()
    return copies


def gathered(plan, held, index, column, within, count):
    piece_lanes = plan.radix // 2
    each = LANES // piece_lanes
    lane = lax.broadcasted_iota(jnp.int32, (count, LANES), 1)
    value = jnp.zeros((count, LANES), jnp.float32)
    for piece in range(each):
        tile = held[column * each + piece, index, :count]
        turned = pltpu.roll(tile, (piece * piece_lanes - within + LANES) % LANES, 1)
        value = jnp.where((lane >= piece * piece_lanes) & (lane < (piece + 1) * piece_lanes), turned, value)
    return value


def held_scratch(plan):
    return [
        pltpu.VMEM((plan.m_his, 2 * plan.rounds, plan.freq_rows, LANES), jnp.float32),
        pltpu.SemaphoreType.DMA((plan.m_his,)),
    ]


def opposite(plan):
    def kernel(at, spectra, out, held, sems):
        m_lo = plan.m_los - 1 - at[1]
        for copy in fetch(plan, spectra, held, sems, m_lo):
            copy.wait()
        within = m_lo * plan.radix % LANES + plan.radix // 2
        for index in range(2 * plan.rounds):
            for column in range(plan.half_cols):
                out[index, :, column * LANES : (column + 1) * LANES] = gathered(
                    plan, held, index, column, within, plan.freq_rows
                )

    shape = jax.ShapeDtypeStruct((2 * plan.rounds, plan.freq_rows, plan.half), jnp.float32)
    return call(kernel, "opposite", shape, ["smem", "hbm"], held_scratch(plan))


def prepare(plan):
    def kernel(at, *refs):
        tables_in = refs[:4]
        spectra, first, last, twist, own, own_real, own_imag = refs[4:11]
        first_rows, first_part, twist_rows, twist_part = refs[11:15]
        table_sems, held, sems = refs[15:]
        place = at[0]
        m_lo = at[1]
        tables_copy = [
            pltpu.make_async_copy(source, target, table_sems.at[index])
            for index, (source, target) in enumerate(zip(tables_in, refs[11:15]))
        ]
        for copy in tables_copy:
            copy.start()
        spectra_copy = fetch(plan, spectra, held, sems, m_lo)
        for copy in tables_copy:
            copy.wait()
        part_cos = first_part[pl.ds(place, 1), 0, :]
        part_sin = first_part[pl.ds(place, 1), 1, :]
        real = first_rows[0] * part_cos - first_rows[1] * part_sin
        imag = first_rows[0] * part_sin + first_rows[1] * part_cos
        both = jnp.concatenate([real, imag], axis=0)
        first[0], first[1] = split(both)
        last[0], last[1] = split(both.T)
        part_cos = twist_part[pl.ds(place, 1), 0, :]
        part_sin = twist_part[pl.ds(place, 1), 1, :]
        twist[0] = twist_rows[0] * part_cos - twist_rows[1] * part_sin
        twist[1] = twist_rows[0] * part_sin + twist_rows[1] * part_cos
        for copy in spectra_copy:
            copy.wait()
        within = m_lo * plan.radix % LANES
        for index in range(2 * plan.rounds):
            step, imaginary = divmod(index, 2)
            for column in range(plan.half_cols):
                own[index, column] = gathered(plan, held, index, column, within, plan.freq_rows)
                upper = gathered(plan, held, index, column, within + plan.radix // 2, 1)
                kept = at[3].astype(jnp.float32) / plan.length
                upper = upper * kept
                for turn in range(EXTRA // plan.half_cols):
                    row = turn * plan.half_cols + column
                    if imaginary:
                        own_imag[step, row : row + 1] = upper if turn % 2 else -upper
                    else:
                        own_real[step, row : row + 1] = upper

    shape = jax.ShapeDtypeStruct
    width = 2 * plan.rows
    out_shape = (
        shape((2, width, plan.n1s), jnp.bfloat16),
        shape((2, plan.n1s, width), jnp.bfloat16),
        shape((2, plan.rows, plan.side), jnp.float32),
        shape((2 * plan.rounds, plan.half_cols, plan.freq_rows, LANES), jnp.float32),
        shape((plan.rounds, EXTRA, LANES), jnp.float32),
        shape((plan.rounds, EXTRA, LANES), jnp.float32),
    )
    scratch = [
        pltpu.VMEM((2, plan.rows, plan.n1s), jnp.float32),
        pltpu.VMEM((plan.quarters, 2, plan.n1s), jnp.float32),
        pltpu.VMEM((2, plan.rows, plan.side), jnp.float32),
        pltpu.VMEM((plan.quarters, 2, plan.side), jnp.float32),
        pltpu.SemaphoreType.DMA((4,)),
    ] + held_scratch(plan)
    return call(kernel, "prepare", out_shape, ["smem"] + ["hbm"] * 5, scratch)


def blend(plan):
    def kernel(own, arrived, out):
        count = 2 * plan.rounds * plan.freq_rows
        row = lax.broadcasted_iota(jnp.int32, (count, count), 0)
        column = lax.broadcasted_iota(jnp.int32, (count, count), 1)
        within = row % plan.freq_rows
        turn = (row + column == 2 * (row - within) + plan.freq_rows) & (within != 0)
        turn = jnp.where(turn, 1.0, 0.0).astype(jnp.bfloat16)
        row = lax.broadcasted_iota(jnp.int32, (plan.half, plan.half), 0)
        column = lax.broadcasted_iota(jnp.int32, (plan.half, plan.half), 1)
        flip = jnp.where(row + column == plan.half - 1, 1.0, 0.0).astype(jnp.bfloat16)
        total = None
        for value in split(arrived[...].reshape(count, plan.half)):
            turned = jnp.dot(turn, value, preferred_element_type=jnp.float32).astype(jnp.bfloat16)
            turned = jnp.dot(turned, flip, preferred_element_type=jnp.float32)
            total = turned if total is None else total + turned
        scale = 1.0 / plan.length
        for index in range(2 * plan.rounds):
            sign = -1.0 if index % 2 else 1.0
            for column in range(plan.half_cols):
                there = total[
                    index * plan.freq_rows : (index + 1) * plan.freq_rows, column * LANES : (column + 1) * LANES
                ]
                out[index, column] = (own[index, column] + sign * there) * scale

    shape = jax.ShapeDtypeStruct((2 * plan.rounds, plan.half_cols, plan.freq_rows, LANES), jnp.float32)
    return call(kernel, "blend", shape, ["vmem"] * 2)


def alternating(plan, count):
    lane = lax.broadcasted_iota(jnp.int32, (count, plan.side), 1)
    return jnp.where(lane % 2 == 0, 1.0, -1.0)


def packed_rows(plan, part, column):
    start = (part * plan.half_cols + column) * plan.slice_rows
    return slice(start, start + plan.slice_rows)


def forward(plan):
    def kernel(at, *refs):
        limbs = refs[: plan.quarters]
        first, twist, second, out, matrix, turned = refs[plan.quarters :]
        place = at[0]
        for index in range(plan.quarters):
            start = pl.multiple_of((place ^ index) * plan.chunk, 8)
            for column in range(plan.cols):
                matrix[pl.ds(start, plan.chunk), column * LANES : (column + 1) * LANES] = limbs[index][
                    pl.ds(column, plan.chunk, stride=plan.cols), :
                ]
        value = product((first[0], first[1]), split(matrix[...]))
        rows, whole, few = plan.rows, 2 * plan.rows, plan.m_los
        real, imag = value[:rows], value[rows:]
        turned[:rows] = real * twist[0] - imag * twist[1]
        turned[rows:whole] = real * twist[1] + imag * twist[0]
        sign = alternating(plan, 1)
        for part in range(2):
            for m_lo in range(few):
                row, start = part * rows + m_lo * plan.freq_rows, whole + part * few + m_lo
                turned[start : start + 1] = turned[row : row + 1] * sign
        value = product(split(turned[...]), (second[0], second[1]))
        by_cos, by_sin = value[:, : plan.half], value[:, plan.half :]
        main = (by_cos[:rows] + by_sin[rows:whole], by_cos[rows:whole] - by_sin[:rows])
        extra = (by_cos[whole : whole + few] + by_sin[whole + few :], by_cos[whole + few :] - by_sin[whole : whole + few])
        base = plan.packed - EXTRA
        for group in range(plan.groups):
            for part in range(2):
                for column in range(plan.half_cols):
                    lanes = slice(column * LANES, (column + 1) * LANES)
                    out[group, packed_rows(plan, part, column)] = main[part][
                        group * plan.slice_rows : (group + 1) * plan.slice_rows, lanes
                    ]
                    m_lo = group // plan.per
                    for turn in range(EXTRA // (2 * plan.half_cols)):
                        row = base + (turn * 2 + part) * plan.half_cols + column
                        out[group, row : row + 1] = extra[part][m_lo : m_lo + 1, lanes]

    shape = jax.ShapeDtypeStruct((plan.groups, plan.packed, LANES), jnp.float32)
    scratch = [
        pltpu.VMEM((plan.n1s, plan.side), jnp.float32),
        pltpu.VMEM((2 * plan.rows + 2 * plan.m_los, plan.side), jnp.float32),
    ]
    return call(kernel, "forward", shape, ["smem"] + ["vmem"] * (plan.quarters + 3), scratch)


def combine(plan):
    def kernel(at, spectra, own, own_real, own_imag, out):
        row = lax.broadcasted_iota(jnp.int32, (plan.slice_rows, LANES), 0) + at[2]
        sign = jnp.where(row % 2 == 0, 1.0, -1.0)
        row = lax.broadcasted_iota(jnp.int32, (EXTRA, LANES), 0) * 0 + at[0] * plan.freq_rows
        extra_sign = jnp.where(row % 2 == 0, 1.0, -1.0)
        base = plan.packed - EXTRA

        def one_block(block, carry):
            sums = [jnp.zeros((plan.slice_rows, LANES), jnp.float32) for _ in range(2 * plan.half_cols)]
            extra = jnp.zeros((EXTRA, LANES), jnp.float32)
            for step in range(plan.rounds):
                here = lax.rem(block + (plan.rounds * STRIDE * plan.groups - step * STRIDE), plan.groups)
                before = lax.rem(here + (plan.groups - 1), plan.groups)
                for column in range(plan.half_cols):
                    real, imag = (
                        spectra[here, packed_rows(plan, part, column)]
                        + sign * spectra[before, packed_rows(plan, part, column)]
                        for part in range(2)
                    )
                    own_r, own_i = own[2 * step, column], own[2 * step + 1, column]
                    sums[column] = sums[column] + own_r * real - own_i * imag
                    sums[plan.half_cols + column] = sums[plan.half_cols + column] + own_r * imag + own_i * real
                both = spectra[here, base:] + extra_sign * spectra[before, base:]
                extra = extra + own_real[step] * both + own_imag[step] * pltpu.roll(both, plan.half_cols, 0)
            for part in range(2):
                for column in range(plan.half_cols):
                    out[block, packed_rows(plan, part, column)] = sums[part * plan.half_cols + column]
            out[block, base:] = extra
            return carry

        lax.fori_loop(0, plan.groups, one_block, 0)

    shape = jax.ShapeDtypeStruct((plan.groups, plan.packed, LANES), jnp.float32)
    return call(kernel, "combine", shape, ["smem"] + ["vmem"] * 4)


def backward(plan):
    def kernel(at, spectra, last, twist, second, out, stack, spread, matrix):
        place = at[0]
        rows, whole, few = plan.rows, 2 * plan.rows, plan.m_los
        base = plan.packed - EXTRA
        for part in range(2):
            for column in range(plan.half_cols):
                lanes = slice(column * LANES, (column + 1) * LANES)
                for group in range(plan.groups):
                    start = part * rows + group * plan.slice_rows
                    stack[start : start + plan.slice_rows, lanes] = spectra[group, packed_rows(plan, part, column)]
                for m_lo in range(few):
                    row = base + part * plan.half_cols + column
                    start = whole + part * few + m_lo
                    stack[start : start + 1, lanes] = spectra[m_lo * plan.per, row : row + 1]
        value = split(stack[...])
        by_cos = product(value, (second[0, :, : plan.half], second[1, :, : plan.half]), True)
        by_sin = product(value, (second[0, :, plan.half :], second[1, :, plan.half :]), True)
        spread[:rows] = by_cos[:rows] - by_sin[rows:whole]
        spread[rows:] = by_cos[rows:whole] + by_sin[:rows]
        sign = alternating(plan, few)
        extra = (
            (by_cos[whole : whole + few] - by_sin[whole + few :]) * sign,
            (by_cos[whole + few :] + by_sin[whole : whole + few]) * sign,
        )
        for part in range(2):
            for m_lo in range(few):
                row = part * rows + m_lo * plan.freq_rows
                spread[row : row + 1] = spread[row : row + 1] + extra[part][m_lo : m_lo + 1]
        real, imag = spread[:rows], spread[rows:]
        turned = jnp.concatenate([real * twist[0] + imag * twist[1], imag * twist[0] - real * twist[1]], axis=0)
        matrix[...] = product((last[0], last[1]), split(turned))
        for index in range(plan.quarters):
            start = pl.multiple_of((place ^ index) * plan.chunk, 8)
            for column in range(plan.cols):
                out[index, pl.ds(column, plan.chunk, stride=plan.cols), :] = matrix[
                    pl.ds(start, plan.chunk), column * LANES : (column + 1) * LANES
                ]

    shape = jax.ShapeDtypeStruct((plan.quarters, plan.chunk * plan.cols, LANES), jnp.float32)
    scratch = [
        pltpu.VMEM((2 * plan.rows + 2 * plan.m_los, plan.half), jnp.float32),
        pltpu.VMEM((2 * plan.rows, plan.side), jnp.float32),
        pltpu.VMEM((plan.n1s, plan.side), jnp.float32),
    ]
    return call(kernel, "backward", shape, ["smem"] + ["vmem"] * 4, scratch)


def swapped(value, bit):
    count = lax.axis_size("acc")
    return lax.ppermute(value, "acc", [(source, source ^ bit) for source in range(count)])


def per_device(reciprocal_spectra, divisor):
    rounds, _, freq_rows, plane = reciprocal_spectra.shape
    quarters = lax.axis_size("acc")
    groups = lax.axis_size("blk") * lax.axis_size("tail")
    plan = Plan(freq_rows, plane, quarters, groups, rounds)
    place = lax.axis_index("acc")
    group = lax.axis_index(("blk", "tail"))
    first_row = group % plan.per * plan.slice_rows
    has_first = jnp.where(first_row == 0, 1, 0)
    at = jnp.stack([place, group // plan.per, first_row + place * freq_rows, has_first]).astype(jnp.int32)
    *small, second = (jnp.asarray(table) for table in tables(plan))

    limbs = divisor.reshape(plan.chunk * plan.cols, LANES)
    pieces = {0: limbs}
    bit = quarters // 2
    while bit:
        pieces.update({index | bit: swapped(piece, bit) for index, piece in list(pieces.items())})
        bit //= 2
    spectra = far(reciprocal_spectra.reshape(2 * rounds, freq_rows, plane))
    facing = swapped(opposite(plan)(at, spectra), quarters - 1)
    first, last, twist, own, own_real, own_imag = prepare(plan)(at, *map(far, small), spectra)

    own_spectrum = forward(plan)(at, *[pieces[index] for index in range(quarters)], first, twist, second)
    own = blend(plan)(own, facing)
    if plan.per > 1:
        own = lax.dynamic_slice_in_dim(own, first_row, plan.slice_rows, 2)
    every = lax.all_to_all(own_spectrum, ("blk", "tail"), 0, 0, tiled=True)
    sums = combine(plan)(at, every, own, own_real, own_imag)
    back = lax.all_to_all(sums, ("blk", "tail"), 0, 0, tiled=True)
    slots = backward(plan)(at, back, last, twist, second)

    held = {index: slots[index] for index in range(quarters)}
    bit = 1
    while bit < quarters:
        sent = sorted(index for index in held if index & bit)
        arrived = swapped(jnp.stack([held[index] for index in sent]), bit)
        held = {index ^ bit: held[index ^ bit] + arrived[where] for where, index in enumerate(sent)}
        bit *= 2
    return held[0].reshape(divisor.shape)


def solution(mesh):
    in_specs = (P(None, None, "acc", None), P(("blk", "tail"), "acc"))
    out_specs = P(("blk", "tail"), "acc")
    return jax.shard_map(
        per_device, mesh=mesh, in_specs=in_specs, out_specs=out_specs, check_vma=False
    )
```

```python
import math

import jax
import jax.numpy as jnp
import numpy as np
from jax import lax
from jax.experimental import pallas as pl
from jax.experimental.pallas import tpu as pltpu
from jax.sharding import PartitionSpec as P


LANES = 128
EXTRA = 8
GRANT = 16 * 1024 * 1024
STRIDE = 2


class Plan:
    def __init__(self, freq_rows, plane, quarters, groups, rounds):
        self.rounds = rounds
        self.quarters = quarters
        self.groups = groups
        self.freq_rows = freq_rows
        self.radix = freq_rows * quarters
        self.length = self.radix * plane
        self.side = math.isqrt(self.length)
        self.half = self.side // 2
        self.m_los = self.side // self.radix
        self.m_his = self.radix // self.m_los
        self.rows = self.m_los * freq_rows
        self.n1s = self.side // 2
        self.chunk = self.n1s // quarters
        self.cols = self.side // LANES
        self.half_cols = self.half // LANES
        self.slice_rows = self.rows // groups
        self.per = groups // self.m_los
        self.packed = 2 * self.half_cols * self.slice_rows + EXTRA


def tables(plan):
    row = (np.arange(plan.m_los)[:, None] * plan.radix + np.arange(plan.freq_rows)[None, :]).reshape(-1)
    part = np.arange(plan.quarters) * plan.freq_rows
    n1 = np.arange(plan.n1s)
    n2 = np.arange(plan.side)
    f2 = (np.arange(plan.m_his)[:, None] + plan.m_los * np.arange(plan.radix // 2)[None, :]).reshape(-1)

    def wave(first, second, modulus):
        angle = (first[:, None] * second[None, :] % modulus) * (-2.0 * math.pi / modulus)
        return np.stack([np.cos(angle), np.sin(angle)])

    first_rows = wave(row, n1, plan.side)
    first_part = wave(part, n1, plan.side)
    twist_rows = wave(row, n2, plan.length)
    twist_part = wave(part, n2, plan.length)
    cosine, sine = wave(n2, f2, plan.side)
    second = np.concatenate([cosine, -sine], axis=1)
    second_high = second.astype(jnp.bfloat16)
    second_low = (second - second_high.astype(np.float64)).astype(jnp.bfloat16)
    single = lambda value: value.astype(np.float32)
    return (
        single(first_rows),
        single(first_part.transpose(1, 0, 2)),
        single(twist_rows),
        single(twist_part.transpose(1, 0, 2)),
        np.stack([second_high, second_low]),
    )


def far(value):
    return pltpu.with_memory_space_constraint(value, pltpu.HBM)


def split(value):
    high = value.astype(jnp.bfloat16)
    low = (value - high.astype(jnp.float32)).astype(jnp.bfloat16)
    return high, low


def product(first, second, transposed=False):
    dims = (((1,), (1 if transposed else 0,)), ((), ()))
    dot = lambda a, b: lax.dot_general(a, b, dims, preferred_element_type=jnp.float32)
    return dot(first[0], second[0]) + (dot(first[1], second[0]) + dot(first[0], second[1]))


def call(kernel, out_shape, memory, scratch=(), flops=1_000_000, moved=1_000_000):
    where = {"smem": pltpu.SMEM, "vmem": pltpu.VMEM, "hbm": pltpu.HBM}
    vmem = pl.BlockSpec(memory_space=pltpu.VMEM)
    return pl.pallas_call(
        kernel,
        out_shape=out_shape,
        in_specs=[pl.BlockSpec(memory_space=where[kind]) for kind in memory],
        out_specs=jax.tree.map(lambda _: vmem, out_shape),
        scratch_shapes=scratch,
        cost_estimate=pl.CostEstimate(flops=flops, bytes_accessed=moved, transcendentals=0),
        compiler_params=pltpu.CompilerParams(vmem_limit_bytes=GRANT),
    )


def fetch(plan, spectra, held, sems, m_lo):
    copies = []
    for m_hi in range(plan.m_his):
        start = pl.multiple_of((m_hi * plan.m_los + m_lo) * plan.radix // LANES * LANES, LANES)
        copies.append(pltpu.make_async_copy(spectra.at[:, :, pl.ds(start, LANES)], held.at[m_hi], sems.at[m_hi]))
        copies[-1].start()
    return copies


def gathered(plan, held, index, column, within, count):
    piece_lanes = plan.radix // 2
    each = LANES // piece_lanes
    lane = lax.broadcasted_iota(jnp.int32, (count, LANES), 1)
    value = jnp.zeros((count, LANES), jnp.float32)
    for piece in range(each):
        tile = held[column * each + piece, index, :count]
        turned = pltpu.roll(tile, (piece * piece_lanes - within + LANES) % LANES, 1)
        value = jnp.where((lane >= piece * piece_lanes) & (lane < (piece + 1) * piece_lanes), turned, value)
    return value


def held_scratch(plan):
    return [
        pltpu.VMEM((plan.m_his, 2 * plan.rounds, plan.freq_rows, LANES), jnp.float32),
        pltpu.SemaphoreType.DMA((plan.m_his,)),
    ]


def opposite(plan):
    def kernel(at, spectra, out, held, sems):
        m_lo = plan.m_los - 1 - at[1]
        for copy in fetch(plan, spectra, held, sems, m_lo):
            copy.wait()
        within = m_lo * plan.radix % LANES + plan.radix // 2
        for index in range(2 * plan.rounds):
            for column in range(plan.half_cols):
                out[index, :, column * LANES : (column + 1) * LANES] = gathered(
                    plan, held, index, column, within, plan.freq_rows
                )

    shape = jax.ShapeDtypeStruct((2 * plan.rounds, plan.freq_rows, plan.half), jnp.float32)
    return call(kernel, shape, ["smem", "hbm"], held_scratch(plan))


def prepare(plan):
    def kernel(at, *refs):
        first, twist, second, near = refs[6:10]
        first_rows, first_part, twist_rows, twist_part = refs[10:14]
        sems = refs[14]
        place = at[0]
        targets = (first_rows, first_part, twist_rows, twist_part, second, near)
        copies = [
            pltpu.make_async_copy(source, target, sems.at[index])
            for index, (source, target) in enumerate(zip(refs[:6], targets))
        ]
        for copy in copies:
            copy.start()
        copies[0].wait()
        copies[1].wait()
        part_cos = first_part[pl.ds(place, 1), 0, :]
        part_sin = first_part[pl.ds(place, 1), 1, :]
        rows = plan.rows
        first[0, :rows], first[1, :rows] = split(first_rows[0] * part_cos - first_rows[1] * part_sin)
        first[0, rows:], first[1, rows:] = split(first_rows[0] * part_sin + first_rows[1] * part_cos)
        copies[2].wait()
        copies[3].wait()
        part_cos = twist_part[pl.ds(place, 1), 0, :]
        part_sin = twist_part[pl.ds(place, 1), 1, :]
        twist[0] = twist_rows[0] * part_cos - twist_rows[1] * part_sin
        twist[1] = twist_rows[0] * part_sin + twist_rows[1] * part_cos
        copies[4].wait()
        copies[5].wait()

    shape = jax.ShapeDtypeStruct
    out_shape = (
        shape((2, 2 * plan.rows, plan.n1s), jnp.bfloat16),
        shape((2, plan.rows, plan.side), jnp.float32),
        shape((2, plan.side, 2 * plan.half), jnp.bfloat16),
        shape((plan.chunk * plan.cols, LANES), jnp.float32),
    )
    scratch = [
        pltpu.VMEM((2, plan.rows, plan.n1s), jnp.float32),
        pltpu.VMEM((plan.quarters, 2, plan.n1s), jnp.float32),
        pltpu.VMEM((2, plan.rows, plan.side), jnp.float32),
        pltpu.VMEM((plan.quarters, 2, plan.side), jnp.float32),
        pltpu.SemaphoreType.DMA((6,)),
    ]
    return call(kernel, out_shape, ["smem"] + ["hbm"] * 6, scratch)


def resident(plan):
    def kernel(at, first, spectra, last, own, own_real, own_imag, held, sems):
        m_lo = at[1]
        copies = fetch(plan, spectra, held, sems, m_lo)
        last[0], last[1] = split((first[0].astype(jnp.float32) + first[1].astype(jnp.float32)).T)
        for copy in copies:
            copy.wait()
        within = m_lo * plan.radix % LANES
        kept = at[3].astype(jnp.float32) / plan.length
        for index in range(2 * plan.rounds):
            step, imaginary = divmod(index, 2)
            for column in range(plan.half_cols):
                own[index, column] = gathered(plan, held, index, column, within, plan.freq_rows)
                upper = gathered(plan, held, index, column, within + plan.radix // 2, 1) * kept
                for turn in range(EXTRA // plan.half_cols):
                    row = turn * plan.half_cols + column
                    if imaginary:
                        own_imag[step, row : row + 1] = upper if turn % 2 else -upper
                    else:
                        own_real[step, row : row + 1] = upper

    shape = jax.ShapeDtypeStruct
    out_shape = (
        shape((2, plan.n1s, 2 * plan.rows), jnp.bfloat16),
        shape((2 * plan.rounds, plan.half_cols, plan.freq_rows, LANES), jnp.float32),
        shape((plan.rounds, EXTRA, LANES), jnp.float32),
        shape((plan.rounds, EXTRA, LANES), jnp.float32),
    )
    return call(kernel, out_shape, ["smem", "vmem", "hbm"], held_scratch(plan))


def blend(plan):
    def kernel(own, arrived, out):
        count = 2 * plan.rounds * plan.freq_rows
        row = lax.broadcasted_iota(jnp.int32, (count, count), 0)
        column = lax.broadcasted_iota(jnp.int32, (count, count), 1)
        within = row % plan.freq_rows
        turn = (row + column == 2 * (row - within) + plan.freq_rows) & (within != 0)
        turn = jnp.where(turn, 1.0, 0.0).astype(jnp.bfloat16)
        row = lax.broadcasted_iota(jnp.int32, (plan.half, plan.half), 0)
        column = lax.broadcasted_iota(jnp.int32, (plan.half, plan.half), 1)
        flip = jnp.where(row + column == plan.half - 1, 1.0, 0.0).astype(jnp.bfloat16)
        total = None
        for value in split(arrived[...].reshape(count, plan.half)):
            turned = jnp.dot(turn, value, preferred_element_type=jnp.float32).astype(jnp.bfloat16)
            turned = jnp.dot(turned, flip, preferred_element_type=jnp.float32)
            total = turned if total is None else total + turned
        scale = 1.0 / plan.length
        for index in range(2 * plan.rounds):
            sign = -1.0 if index % 2 else 1.0
            for column in range(plan.half_cols):
                there = total[
                    index * plan.freq_rows : (index + 1) * plan.freq_rows, column * LANES : (column + 1) * LANES
                ]
                out[index, column] = (own[index, column] + sign * there) * scale

    shape = jax.ShapeDtypeStruct((2 * plan.rounds, plan.half_cols, plan.freq_rows, LANES), jnp.float32)
    return call(kernel, shape, ["vmem"] * 2)


def alternating(plan, count):
    lane = lax.broadcasted_iota(jnp.int32, (count, plan.side), 1)
    return jnp.where(lane % 2 == 0, 1.0, -1.0)


def packed_rows(plan, part, column):
    start = (part * plan.half_cols + column) * plan.slice_rows
    return slice(start, start + plan.slice_rows)


def forward(plan):
    def kernel(at, *refs):
        limbs = refs[: plan.quarters]
        first, twist, second, out, matrix, turned = refs[plan.quarters :]
        place = at[0]
        for index in range(plan.quarters):
            start = pl.multiple_of((place ^ index) * plan.chunk, 8)
            for column in range(plan.cols):
                matrix[pl.ds(start, plan.chunk), column * LANES : (column + 1) * LANES] = limbs[index][
                    pl.ds(column, plan.chunk, stride=plan.cols), :
                ]
        value = product((first[0], first[1]), split(matrix[...]))
        rows, whole, few = plan.rows, 2 * plan.rows, plan.m_los
        real, imag = value[:rows], value[rows:]
        turned[:rows] = real * twist[0] - imag * twist[1]
        turned[rows:whole] = real * twist[1] + imag * twist[0]
        sign = alternating(plan, 1)
        for part in range(2):
            for m_lo in range(few):
                row, start = part * rows + m_lo * plan.freq_rows, whole + part * few + m_lo
                turned[start : start + 1] = turned[row : row + 1] * sign
        value = product(split(turned[...]), (second[0], second[1]))
        by_cos, by_sin = value[:, : plan.half], value[:, plan.half :]
        main = (by_cos[:rows] + by_sin[rows:whole], by_cos[rows:whole] - by_sin[:rows])
        extra = (by_cos[whole : whole + few] + by_sin[whole + few :], by_cos[whole + few :] - by_sin[whole : whole + few])
        base = plan.packed - EXTRA
        for group in range(plan.groups):
            for part in range(2):
                for column in range(plan.half_cols):
                    lanes = slice(column * LANES, (column + 1) * LANES)
                    out[group, packed_rows(plan, part, column)] = main[part][
                        group * plan.slice_rows : (group + 1) * plan.slice_rows, lanes
                    ]
                    m_lo = group // plan.per
                    for turn in range(EXTRA // (2 * plan.half_cols)):
                        row = base + (turn * 2 + part) * plan.half_cols + column
                        out[group, row : row + 1] = extra[part][m_lo : m_lo + 1, lanes]

    shape = jax.ShapeDtypeStruct((plan.groups, plan.packed, LANES), jnp.float32)
    scratch = [
        pltpu.VMEM((plan.n1s, plan.side), jnp.float32),
        pltpu.VMEM((2 * plan.rows + 2 * plan.m_los, plan.side), jnp.float32),
    ]
    return call(kernel, shape, ["smem"] + ["vmem"] * (plan.quarters + 3), scratch)


def combine(plan):
    def kernel(at, spectra, own, own_real, own_imag, out):
        row = lax.broadcasted_iota(jnp.int32, (plan.slice_rows, LANES), 0) + at[2]
        sign = jnp.where(row % 2 == 0, 1.0, -1.0)
        row = lax.broadcasted_iota(jnp.int32, (EXTRA, LANES), 0) * 0 + at[0] * plan.freq_rows
        extra_sign = jnp.where(row % 2 == 0, 1.0, -1.0)
        base = plan.packed - EXTRA

        def one_block(block, carry):
            sums = [jnp.zeros((plan.slice_rows, LANES), jnp.float32) for _ in range(2 * plan.half_cols)]
            extra = jnp.zeros((EXTRA, LANES), jnp.float32)
            for step in range(plan.rounds):
                here = lax.rem(block + (plan.rounds * STRIDE * plan.groups - step * STRIDE), plan.groups)
                before = lax.rem(here + (plan.groups - 1), plan.groups)
                for column in range(plan.half_cols):
                    real, imag = (
                        spectra[here, packed_rows(plan, part, column)]
                        + sign * spectra[before, packed_rows(plan, part, column)]
                        for part in range(2)
                    )
                    own_r, own_i = own[2 * step, column], own[2 * step + 1, column]
                    sums[column] = sums[column] + own_r * real - own_i * imag
                    sums[plan.half_cols + column] = sums[plan.half_cols + column] + own_r * imag + own_i * real
                both = spectra[here, base:] + extra_sign * spectra[before, base:]
                extra = extra + own_real[step] * both + own_imag[step] * pltpu.roll(both, plan.half_cols, 0)
            for part in range(2):
                for column in range(plan.half_cols):
                    out[block, packed_rows(plan, part, column)] = sums[part * plan.half_cols + column]
            out[block, base:] = extra
            return carry

        lax.fori_loop(0, plan.groups, one_block, 0)

    shape = jax.ShapeDtypeStruct((plan.groups, plan.packed, LANES), jnp.float32)
    return call(kernel, shape, ["smem"] + ["vmem"] * 4)


def backward(plan):
    def kernel(at, spectra, last, twist, second, out, stack, spread, matrix):
        place = at[0]
        rows, whole, few = plan.rows, 2 * plan.rows, plan.m_los
        base = plan.packed - EXTRA
        for part in range(2):
            for column in range(plan.half_cols):
                lanes = slice(column * LANES, (column + 1) * LANES)
                for group in range(plan.groups):
                    start = part * rows + group * plan.slice_rows
                    stack[start : start + plan.slice_rows, lanes] = spectra[group, packed_rows(plan, part, column)]
                for m_lo in range(few):
                    row = base + part * plan.half_cols + column
                    start = whole + part * few + m_lo
                    stack[start : start + 1, lanes] = spectra[m_lo * plan.per, row : row + 1]
        value = split(stack[...])
        by_cos = product(value, (second[0, :, : plan.half], second[1, :, : plan.half]), True)
        by_sin = product(value, (second[0, :, plan.half :], second[1, :, plan.half :]), True)
        spread[:rows] = by_cos[:rows] - by_sin[rows:whole]
        spread[rows:] = by_cos[rows:whole] + by_sin[:rows]
        sign = alternating(plan, few)
        extra = (
            (by_cos[whole : whole + few] - by_sin[whole + few :]) * sign,
            (by_cos[whole + few :] + by_sin[whole : whole + few]) * sign,
        )
        for part in range(2):
            for m_lo in range(few):
                row = part * rows + m_lo * plan.freq_rows
                spread[row : row + 1] = spread[row : row + 1] + extra[part][m_lo : m_lo + 1]
        real, imag = spread[:rows], spread[rows:]
        turned = jnp.concatenate([real * twist[0] + imag * twist[1], imag * twist[0] - real * twist[1]], axis=0)
        matrix[...] = product((last[0], last[1]), split(turned))
        for index in range(plan.quarters):
            start = pl.multiple_of((place ^ index) * plan.chunk, 8)
            for column in range(plan.cols):
                out[index, pl.ds(column, plan.chunk, stride=plan.cols), :] = matrix[
                    pl.ds(start, plan.chunk), column * LANES : (column + 1) * LANES
                ]

    shape = jax.ShapeDtypeStruct((plan.quarters, plan.chunk * plan.cols, LANES), jnp.float32)
    scratch = [
        pltpu.VMEM((2 * plan.rows + 2 * plan.m_los, plan.half), jnp.float32),
        pltpu.VMEM((2 * plan.rows, plan.side), jnp.float32),
        pltpu.VMEM((plan.n1s, plan.side), jnp.float32),
    ]
    return call(kernel, shape, ["smem"] + ["vmem"] * 4, scratch)


def swapped(value, bit):
    count = lax.axis_size("acc")
    return lax.ppermute(value, "acc", [(source, source ^ bit) for source in range(count)])


def per_device(reciprocal_spectra, divisor):
    rounds, _, freq_rows, plane = reciprocal_spectra.shape
    quarters = lax.axis_size("acc")
    groups = lax.axis_size("blk") * lax.axis_size("tail")
    plan = Plan(freq_rows, plane, quarters, groups, rounds)
    place = lax.axis_index("acc")
    group = lax.axis_index(("blk", "tail"))
    first_row = group % plan.per * plan.slice_rows
    has_first = jnp.where(first_row == 0, 1, 0)
    at = jnp.stack([place, group // plan.per, first_row + place * freq_rows, has_first]).astype(jnp.int32)
    constants = [jnp.asarray(table) for table in tables(plan)]

    limbs = divisor.reshape(plan.chunk * plan.cols, LANES)
    pieces = {0: limbs}
    bit = quarters // 2
    while bit:
        pieces.update({index | bit: swapped(piece, bit) for index, piece in list(pieces.items())})
        bit //= 2
    spectra = far(reciprocal_spectra.reshape(2 * rounds, freq_rows, plane))
    first, twist, second, near = prepare(plan)(at, *map(far, constants + [limbs]))
    pieces[0] = near
    facing = swapped(opposite(plan)(at, spectra), quarters - 1)
    last, own, own_real, own_imag = resident(plan)(at, first, spectra)

    own_spectrum = forward(plan)(at, *[pieces[index] for index in range(quarters)], first, twist, second)
    own = blend(plan)(own, facing)
    if plan.per > 1:
        own = lax.dynamic_slice_in_dim(own, first_row, plan.slice_rows, 2)
    every = lax.all_to_all(own_spectrum, ("blk", "tail"), 0, 0, tiled=True)
    sums = combine(plan)(at, every, own, own_real, own_imag)
    back = lax.all_to_all(sums, ("blk", "tail"), 0, 0, tiled=True)
    slots = backward(plan)(at, back, last, twist, second)

    held = {index: slots[index] for index in range(quarters)}
    bit = 1
    while bit < quarters:
        sent = sorted(index for index in held if index & bit)
        arrived = swapped(jnp.stack([held[index] for index in sent]), bit)
        held = {index ^ bit: held[index ^ bit] + arrived[where] for where, index in enumerate(sent)}
        bit *= 2
    return held[0].reshape(divisor.shape)


def solution(mesh):
    in_specs = (P(None, None, "acc", None), P(("blk", "tail"), "acc"))
    out_specs = P(("blk", "tail"), "acc")
    return jax.shard_map(per_device, mesh=mesh, in_specs=in_specs, out_specs=out_specs, check_vma=False)
```

```python
import math

import jax
import jax.numpy as jnp
import numpy as np
from jax import lax
from jax.experimental import pallas as pl
from jax.experimental.pallas import tpu as pltpu
from jax.sharding import PartitionSpec as P


LANES = 128
EXTRA = 8
GRANT = 16 * 1024 * 1024
STRIDE = 2


class Plan:
    def __init__(self, freq_rows, plane, quarters, groups, rounds):
        self.rounds = rounds
        self.quarters = quarters
        self.groups = groups
        self.freq_rows = freq_rows
        self.radix = freq_rows * quarters
        self.length = self.radix * plane
        self.side = math.isqrt(self.length)
        self.half = self.side // 2
        self.m_los = self.side // self.radix
        self.m_his = self.radix // self.m_los
        self.rows = self.m_los * freq_rows
        self.n1s = self.side // 2
        self.chunk = self.n1s // quarters
        self.cols = self.side // LANES
        self.half_cols = self.half // LANES
        self.slice_rows = self.rows // groups
        self.per = groups // self.m_los
        self.packed = 2 * self.half_cols * self.slice_rows + EXTRA


def tables(plan):
    row = (np.arange(plan.m_los)[:, None] * plan.radix + np.arange(plan.freq_rows)[None, :]).reshape(-1)
    part = np.arange(plan.quarters) * plan.freq_rows
    n1 = np.arange(plan.n1s)
    n2 = np.arange(plan.side)
    f2 = (np.arange(plan.m_his)[:, None] + plan.m_los * np.arange(plan.radix // 2)[None, :]).reshape(-1)

    def wave(first, second, modulus):
        angle = (first[:, None] * second[None, :] % modulus) * (-2.0 * math.pi / modulus)
        return np.stack([np.cos(angle), np.sin(angle)])

    first_rows = wave(row, n1, plan.side)
    first_part = wave(part, n1, plan.side)
    twist_rows = wave(row, n2, plan.length)
    twist_part = wave(part, n2, plan.length)
    cosine, sine = wave(n2, f2, plan.side)
    second = np.concatenate([cosine, -sine], axis=1)
    second_high = second.astype(jnp.bfloat16)
    second_low = (second - second_high.astype(np.float64)).astype(jnp.bfloat16)
    single = lambda value: value.astype(np.float32)
    return (
        single(first_rows),
        single(first_part.transpose(1, 0, 2)),
        single(twist_rows),
        single(twist_part.transpose(1, 0, 2)),
        np.stack([second_high, second_low]),
    )


def spot(plan):
    place = lax.axis_index("acc")
    group = lax.axis_index("blk") * lax.axis_size("tail") + lax.axis_index("tail")
    if plan.per == 1:
        return place, group, 0, True
    first_row = lax.rem(group, plan.per) * plan.slice_rows
    return place, lax.div(group, plan.per), first_row, first_row == 0


def far(value):
    return pltpu.with_memory_space_constraint(value, pltpu.HBM)


def split(value):
    high = value.astype(jnp.bfloat16)
    low = (value - high.astype(jnp.float32)).astype(jnp.bfloat16)
    return high, low


def product(first, second, transposed=False):
    dims = (((1,), (1 if transposed else 0,)), ((), ()))
    dot = lambda a, b: lax.dot_general(a, b, dims, preferred_element_type=jnp.float32)
    return dot(first[0], second[0]) + (dot(first[1], second[0]) + dot(first[0], second[1]))


def call(kernel, out_shape, memory, scratch=(), flops=1_000_000, moved=1_000_000):
    where = {"vmem": pltpu.VMEM, "hbm": pltpu.HBM}
    vmem = pl.BlockSpec(memory_space=pltpu.VMEM)
    return pl.pallas_call(
        kernel,
        out_shape=out_shape,
        in_specs=[pl.BlockSpec(memory_space=where[kind]) for kind in memory],
        out_specs=jax.tree.map(lambda _: vmem, out_shape),
        scratch_shapes=scratch,
        cost_estimate=pl.CostEstimate(flops=flops, bytes_accessed=moved, transcendentals=0),
        compiler_params=pltpu.CompilerParams(vmem_limit_bytes=GRANT),
    )


def fetch(plan, spectra, held, sems, m_lo):
    copies = []
    for m_hi in range(plan.m_his):
        start = pl.multiple_of((m_hi * plan.m_los + m_lo) * plan.radix // LANES * LANES, LANES)
        copies.append(pltpu.make_async_copy(spectra.at[:, :, pl.ds(start, LANES)], held.at[m_hi], sems.at[m_hi]))
    return copies


def gathered(plan, held, index, column, within, count):
    piece_lanes = plan.radix // 2
    each = LANES // piece_lanes
    lane = lax.broadcasted_iota(jnp.int32, (count, LANES), 1)
    value = jnp.zeros((count, LANES), jnp.float32)
    for piece in range(each):
        tile = held[column * each + piece, index, :count]
        turned = pltpu.roll(tile, (piece * piece_lanes - within + LANES) % LANES, 1)
        value = jnp.where((lane >= piece * piece_lanes) & (lane < (piece + 1) * piece_lanes), turned, value)
    return value


def held_shape(plan):
    return jax.ShapeDtypeStruct((plan.m_his, 2 * plan.rounds, plan.freq_rows, LANES), jnp.float32)


def opposite(plan):
    def kernel(held, out):
        m_lo = plan.m_los - 1 - spot(plan)[1]
        within = m_lo * plan.radix % LANES + plan.radix // 2
        for index in range(2 * plan.rounds):
            for column in range(plan.half_cols):
                out[index, :, column * LANES : (column + 1) * LANES] = gathered(
                    plan, held, index, column, within, plan.freq_rows
                )

    shape = jax.ShapeDtypeStruct((2 * plan.rounds, plan.freq_rows, plan.half), jnp.float32)
    return call(kernel, shape, ["vmem"])


def prepare(plan):
    def kernel(*refs):
        first, twist, second, near, held, facing = refs[7:13]
        first_rows, first_part, twist_rows, twist_part = refs[13:17]
        sems, held_sems, facing_sems = refs[17:]
        place, m_lo, _, _ = spot(plan)
        targets = (first_rows, first_part, twist_rows, twist_part, second, near)
        copies = [
            pltpu.make_async_copy(source, target, sems.at[index])
            for index, (source, target) in enumerate(zip(refs[:6], targets))
        ]
        copies += fetch(plan, refs[6], facing, facing_sems, plan.m_los - 1 - m_lo)
        copies += fetch(plan, refs[6], held, held_sems, m_lo)
        for copy in copies:
            copy.start()
        copies[0].wait()
        copies[1].wait()
        part_cos = first_part[pl.ds(place, 1), 0, :]
        part_sin = first_part[pl.ds(place, 1), 1, :]
        rows = plan.rows
        first[0, :rows], first[1, :rows] = split(first_rows[0] * part_cos - first_rows[1] * part_sin)
        first[0, rows:], first[1, rows:] = split(first_rows[0] * part_sin + first_rows[1] * part_cos)
        copies[2].wait()
        copies[3].wait()
        part_cos = twist_part[pl.ds(place, 1), 0, :]
        part_sin = twist_part[pl.ds(place, 1), 1, :]
        twist[0] = twist_rows[0] * part_cos - twist_rows[1] * part_sin
        twist[1] = twist_rows[0] * part_sin + twist_rows[1] * part_cos
        for copy in copies[4:]:
            copy.wait()

    shape = jax.ShapeDtypeStruct
    out_shape = (
        shape((2, 2 * plan.rows, plan.n1s), jnp.bfloat16),
        shape((2, plan.rows, plan.side), jnp.float32),
        shape((2, plan.side, 2 * plan.half), jnp.bfloat16),
        shape((plan.chunk * plan.cols, LANES), jnp.float32),
        held_shape(plan),
        held_shape(plan),
    )
    scratch = [
        pltpu.VMEM((2, plan.rows, plan.n1s), jnp.float32),
        pltpu.VMEM((plan.quarters, 2, plan.n1s), jnp.float32),
        pltpu.VMEM((2, plan.rows, plan.side), jnp.float32),
        pltpu.VMEM((plan.quarters, 2, plan.side), jnp.float32),
        pltpu.SemaphoreType.DMA((6,)),
        pltpu.SemaphoreType.DMA((plan.m_his,)),
        pltpu.SemaphoreType.DMA((plan.m_his,)),
    ]
    return call(kernel, out_shape, ["hbm"] * 7, scratch)


def resident(plan):
    def kernel(first, held, last, own, own_real, own_imag):
        _, m_lo, _, unpaired = spot(plan)
        last[0], last[1] = split((first[0].astype(jnp.float32) + first[1].astype(jnp.float32)).T)
        within = m_lo * plan.radix % LANES
        kept = jnp.where(unpaired, 1.0 / plan.length, 0.0)
        for index in range(2 * plan.rounds):
            step, imaginary = divmod(index, 2)
            for column in range(plan.half_cols):
                own[index, column] = gathered(plan, held, index, column, within, plan.freq_rows)
                upper = gathered(plan, held, index, column, within + plan.radix // 2, 1) * kept
                for turn in range(EXTRA // plan.half_cols):
                    row = turn * plan.half_cols + column
                    if imaginary:
                        own_imag[step, row : row + 1] = upper if turn % 2 else -upper
                    else:
                        own_real[step, row : row + 1] = upper

    shape = jax.ShapeDtypeStruct
    out_shape = (
        shape((2, plan.n1s, 2 * plan.rows), jnp.bfloat16),
        shape((2 * plan.rounds, plan.half_cols, plan.freq_rows, LANES), jnp.float32),
        shape((plan.rounds, EXTRA, LANES), jnp.float32),
        shape((plan.rounds, EXTRA, LANES), jnp.float32),
    )
    return call(kernel, out_shape, ["vmem"] * 2)


def blend(plan):
    def kernel(own, arrived, out):
        count = 2 * plan.rounds * plan.freq_rows
        row = lax.broadcasted_iota(jnp.int32, (count, count), 0)
        column = lax.broadcasted_iota(jnp.int32, (count, count), 1)
        within = row % plan.freq_rows
        turn = (row + column == 2 * (row - within) + plan.freq_rows) & (within != 0)
        turn = jnp.where(turn, 1.0, 0.0).astype(jnp.bfloat16)
        row = lax.broadcasted_iota(jnp.int32, (plan.half, plan.half), 0)
        column = lax.broadcasted_iota(jnp.int32, (plan.half, plan.half), 1)
        flip = jnp.where(row + column == plan.half - 1, 1.0, 0.0).astype(jnp.bfloat16)
        total = None
        for value in split(arrived[...].reshape(count, plan.half)):
            turned = jnp.dot(turn, value, preferred_element_type=jnp.float32).astype(jnp.bfloat16)
            turned = jnp.dot(turned, flip, preferred_element_type=jnp.float32)
            total = turned if total is None else total + turned
        scale = 1.0 / plan.length
        for index in range(2 * plan.rounds):
            sign = -1.0 if index % 2 else 1.0
            for column in range(plan.half_cols):
                there = total[
                    index * plan.freq_rows : (index + 1) * plan.freq_rows, column * LANES : (column + 1) * LANES
                ]
                out[index, column] = (own[index, column] + sign * there) * scale

    shape = jax.ShapeDtypeStruct((2 * plan.rounds, plan.half_cols, plan.freq_rows, LANES), jnp.float32)
    return call(kernel, shape, ["vmem"] * 2)


def alternating(plan, count):
    lane = lax.broadcasted_iota(jnp.int32, (count, plan.side), 1)
    return jnp.where(lane % 2 == 0, 1.0, -1.0)


def packed_rows(plan, part, column):
    start = (part * plan.half_cols + column) * plan.slice_rows
    return slice(start, start + plan.slice_rows)


def forward(plan):
    def kernel(*refs):
        limbs = refs[: plan.quarters]
        first, twist, second, out, matrix, turned = refs[plan.quarters :]
        place = spot(plan)[0]
        for index in range(plan.quarters):
            start = pl.multiple_of((place ^ index) * plan.chunk, 8)
            for column in range(plan.cols):
                matrix[pl.ds(start, plan.chunk), column * LANES : (column + 1) * LANES] = limbs[index][
                    pl.ds(column, plan.chunk, stride=plan.cols), :
                ]
        value = product((first[0], first[1]), split(matrix[...]))
        rows, whole, few = plan.rows, 2 * plan.rows, plan.m_los
        real, imag = value[:rows], value[rows:]
        turned[:rows] = real * twist[0] - imag * twist[1]
        turned[rows:whole] = real * twist[1] + imag * twist[0]
        sign = alternating(plan, 1)
        for part in range(2):
            for m_lo in range(few):
                row, start = part * rows + m_lo * plan.freq_rows, whole + part * few + m_lo
                turned[start : start + 1] = turned[row : row + 1] * sign
        value = product(split(turned[...]), (second[0], second[1]))
        by_cos, by_sin = value[:, : plan.half], value[:, plan.half :]
        main = (by_cos[:rows] + by_sin[rows:whole], by_cos[rows:whole] - by_sin[:rows])
        extra = (by_cos[whole : whole + few] + by_sin[whole + few :], by_cos[whole + few :] - by_sin[whole : whole + few])
        base = plan.packed - EXTRA
        for group in range(plan.groups):
            for part in range(2):
                for column in range(plan.half_cols):
                    lanes = slice(column * LANES, (column + 1) * LANES)
                    out[group, packed_rows(plan, part, column)] = main[part][
                        group * plan.slice_rows : (group + 1) * plan.slice_rows, lanes
                    ]
                    m_lo = group // plan.per
                    for turn in range(EXTRA // (2 * plan.half_cols)):
                        row = base + (turn * 2 + part) * plan.half_cols + column
                        out[group, row : row + 1] = extra[part][m_lo : m_lo + 1, lanes]

    shape = jax.ShapeDtypeStruct((plan.groups, plan.packed, LANES), jnp.float32)
    scratch = [
        pltpu.VMEM((plan.n1s, plan.side), jnp.float32),
        pltpu.VMEM((2 * plan.rows + 2 * plan.m_los, plan.side), jnp.float32),
    ]
    return call(kernel, shape, ["vmem"] * (plan.quarters + 3), scratch)


def combine(plan):
    def kernel(spectra, own, own_real, own_imag, out):
        place, _, first_row, _ = spot(plan)
        first_freq = place * plan.freq_rows
        row = lax.broadcasted_iota(jnp.int32, (plan.slice_rows, LANES), 0) + first_row + first_freq
        sign = jnp.where(row % 2 == 0, 1.0, -1.0)
        row = lax.broadcasted_iota(jnp.int32, (EXTRA, LANES), 0) * 0 + first_freq
        extra_sign = jnp.where(row % 2 == 0, 1.0, -1.0)
        base = plan.packed - EXTRA

        def one_block(block, carry):
            sums = [jnp.zeros((plan.slice_rows, LANES), jnp.float32) for _ in range(2 * plan.half_cols)]
            extra = jnp.zeros((EXTRA, LANES), jnp.float32)
            for step in range(plan.rounds):
                here = lax.rem(block + (plan.rounds * STRIDE * plan.groups - step * STRIDE), plan.groups)
                before = lax.rem(here + (plan.groups - 1), plan.groups)
                for column in range(plan.half_cols):
                    real, imag = (
                        spectra[here, packed_rows(plan, part, column)]
                        + sign * spectra[before, packed_rows(plan, part, column)]
                        for part in range(2)
                    )
                    own_r, own_i = own[2 * step, column], own[2 * step + 1, column]
                    sums[column] = sums[column] + own_r * real - own_i * imag
                    sums[plan.half_cols + column] = sums[plan.half_cols + column] + own_r * imag + own_i * real
                both = spectra[here, base:] + extra_sign * spectra[before, base:]
                extra = extra + own_real[step] * both + own_imag[step] * pltpu.roll(both, plan.half_cols, 0)
            for part in range(2):
                for column in range(plan.half_cols):
                    out[block, packed_rows(plan, part, column)] = sums[part * plan.half_cols + column]
            out[block, base:] = extra
            return carry

        lax.fori_loop(0, plan.groups, one_block, 0)

    shape = jax.ShapeDtypeStruct((plan.groups, plan.packed, LANES), jnp.float32)
    return call(kernel, shape, ["vmem"] * 4)


def backward(plan):
    def kernel(spectra, last, twist, second, out, stack, spread, matrix):
        place = spot(plan)[0]
        rows, whole, few = plan.rows, 2 * plan.rows, plan.m_los
        base = plan.packed - EXTRA
        for part in range(2):
            for column in range(plan.half_cols):
                lanes = slice(column * LANES, (column + 1) * LANES)
                for group in range(plan.groups):
                    start = part * rows + group * plan.slice_rows
                    stack[start : start + plan.slice_rows, lanes] = spectra[group, packed_rows(plan, part, column)]
                for m_lo in range(few):
                    row = base + part * plan.half_cols + column
                    start = whole + part * few + m_lo
                    stack[start : start + 1, lanes] = spectra[m_lo * plan.per, row : row + 1]
        value = split(stack[...])
        by_cos = product(value, (second[0, :, : plan.half], second[1, :, : plan.half]), True)
        by_sin = product(value, (second[0, :, plan.half :], second[1, :, plan.half :]), True)
        spread[:rows] = by_cos[:rows] - by_sin[rows:whole]
        spread[rows:] = by_cos[rows:whole] + by_sin[:rows]
        sign = alternating(plan, few)
        extra = (
            (by_cos[whole : whole + few] - by_sin[whole + few :]) * sign,
            (by_cos[whole + few :] + by_sin[whole : whole + few]) * sign,
        )
        for part in range(2):
            for m_lo in range(few):
                row = part * rows + m_lo * plan.freq_rows
                spread[row : row + 1] = spread[row : row + 1] + extra[part][m_lo : m_lo + 1]
        real, imag = spread[:rows], spread[rows:]
        turned = jnp.concatenate([real * twist[0] + imag * twist[1], imag * twist[0] - real * twist[1]], axis=0)
        matrix[...] = product((last[0], last[1]), split(turned))
        for index in range(plan.quarters):
            start = pl.multiple_of((place ^ index) * plan.chunk, 8)
            for column in range(plan.cols):
                out[index, pl.ds(column, plan.chunk, stride=plan.cols), :] = matrix[
                    pl.ds(start, plan.chunk), column * LANES : (column + 1) * LANES
                ]

    shape = jax.ShapeDtypeStruct((plan.quarters, plan.chunk * plan.cols, LANES), jnp.float32)
    scratch = [
        pltpu.VMEM((2 * plan.rows + 2 * plan.m_los, plan.half), jnp.float32),
        pltpu.VMEM((2 * plan.rows, plan.side), jnp.float32),
        pltpu.VMEM((plan.n1s, plan.side), jnp.float32),
    ]
    return call(kernel, shape, ["vmem"] * 4, scratch)


def swapped(value, bit):
    count = lax.axis_size("acc")
    return lax.ppermute(value, "acc", [(source, source ^ bit) for source in range(count)])


def per_device(reciprocal_spectra, divisor):
    rounds, _, freq_rows, plane = reciprocal_spectra.shape
    quarters = lax.axis_size("acc")
    groups = lax.axis_size("blk") * lax.axis_size("tail")
    plan = Plan(freq_rows, plane, quarters, groups, rounds)
    constants = [jnp.asarray(table) for table in tables(plan)]

    limbs = divisor.reshape(plan.chunk * plan.cols, LANES)
    pieces = {0: limbs}
    bit = quarters // 2
    while bit:
        pieces.update({index | bit: swapped(piece, bit) for index, piece in list(pieces.items())})
        bit //= 2
    spectra = reciprocal_spectra.reshape(2 * rounds, freq_rows, plane)
    first, twist, second, near, held, facing = prepare(plan)(*map(far, constants + [limbs, spectra]))
    pieces[0] = near
    facing = swapped(opposite(plan)(facing), quarters - 1)
    last, own, own_real, own_imag = resident(plan)(first, held)

    own_spectrum = forward(plan)(*[pieces[index] for index in range(quarters)], first, twist, second)
    own = blend(plan)(own, facing)
    if plan.per > 1:
        first_row = lax.axis_index(("blk", "tail")) % plan.per * plan.slice_rows
        own = lax.dynamic_slice_in_dim(own, first_row, plan.slice_rows, 2)
    every = lax.all_to_all(own_spectrum, ("blk", "tail"), 0, 0, tiled=True)
    sums = combine(plan)(every, own, own_real, own_imag)
    back = lax.all_to_all(sums, ("blk", "tail"), 0, 0, tiled=True)
    slots = backward(plan)(back, last, twist, second)

    held = {index: slots[index] for index in range(quarters)}
    bit = 1
    while bit < quarters:
        sent = sorted(index for index in held if index & bit)
        arrived = swapped(jnp.stack([held[index] for index in sent]), bit)
        held = {index ^ bit: held[index ^ bit] + arrived[where] for where, index in enumerate(sent)}
        bit *= 2
    return held[0].reshape(divisor.shape)


def solution(mesh):
    in_specs = (P(None, None, "acc", None), P(("blk", "tail"), "acc"))
    out_specs = P(("blk", "tail"), "acc")
    return jax.shard_map(per_device, mesh=mesh, in_specs=in_specs, out_specs=out_specs, check_vma=False)
```

```python
import math

import jax
import jax.numpy as jnp
import numpy as np
from jax import lax
from jax.experimental import pallas as pl
from jax.experimental.pallas import tpu as pltpu
from jax.sharding import PartitionSpec as P


LANES = 128
TILE = 8
GRANT = 16 * 1024 * 1024
STRIDE = 2


class Plan:
    def __init__(self, freq_rows, plane, quarters, groups, rounds):
        self.rounds = rounds
        self.quarters = quarters
        self.groups = groups
        self.freq_rows = freq_rows
        self.radix = freq_rows * quarters
        self.length = self.radix * plane
        self.side = math.isqrt(self.length)
        self.half = self.side // 2
        self.m_los = self.side // self.radix
        self.m_his = self.radix // self.m_los
        self.rows = self.m_los * freq_rows
        self.n1s = self.side // 2
        self.chunk = self.n1s // quarters
        self.cols = self.side // LANES
        self.half_cols = self.half // LANES
        self.slice_rows = self.rows // groups
        self.per = groups // self.m_los
        self.packed = 2 * self.half_cols * self.slice_rows


def tables(plan):
    row = (np.arange(plan.m_los)[:, None] * plan.radix + np.arange(plan.freq_rows)[None, :]).reshape(-1)
    part = np.arange(plan.quarters) * plan.freq_rows
    n1 = np.arange(plan.n1s)
    n2 = np.arange(plan.side)
    f2 = (np.arange(plan.m_his)[:, None] + plan.m_los * np.arange(plan.radix // 2)[None, :]).reshape(-1)

    def wave(first, second, modulus):
        angle = (first[:, None] * second[None, :] % modulus) * (-2.0 * math.pi / modulus)
        return np.stack([np.cos(angle), np.sin(angle)])

    first_rows = wave(row, n1, plan.side)
    first_part = wave(part, n1, plan.side)
    twist_rows = wave(row, n2, plan.length)
    twist_part = wave(part, n2, plan.length)
    cosine, sine = wave(n2, f2, plan.side)
    second = np.concatenate([cosine, -sine], axis=1)
    second_high = second.astype(jnp.bfloat16)
    second_low = (second - second_high.astype(np.float64)).astype(jnp.bfloat16)
    single = lambda value: value.astype(np.float32)
    return (
        single(first_rows),
        single(first_part.transpose(1, 0, 2)),
        single(twist_rows),
        single(twist_part.transpose(1, 0, 2)),
        np.stack([second_high, second_low]),
    )


def spot(plan):
    place = lax.axis_index("acc")
    group = lax.axis_index("blk") * lax.axis_size("tail") + lax.axis_index("tail")
    if plan.per == 1:
        return place, group, 0
    return place, lax.div(group, plan.per), lax.rem(group, plan.per) * plan.slice_rows


def rim_m_lo(plan, place, m_lo):
    return jnp.where(place == 0, lax.rem(plan.m_los - m_lo, plan.m_los), plan.m_los - 1 - m_lo)


def far(value):
    return pltpu.with_memory_space_constraint(value, pltpu.HBM)


def split(value):
    high = value.astype(jnp.bfloat16)
    low = (value - high.astype(jnp.float32)).astype(jnp.bfloat16)
    return high, low


def product(first, second, transposed=False):
    dims = (((1,), (1 if transposed else 0,)), ((), ()))
    dot = lambda a, b: lax.dot_general(a, b, dims, preferred_element_type=jnp.float32)
    return dot(first[0], second[0]) + (dot(first[1], second[0]) + dot(first[0], second[1]))


def call(kernel, out_shape, memory, scratch=(), flops=1_000_000, moved=1_000_000):
    where = {"vmem": pltpu.VMEM, "hbm": pltpu.HBM}
    vmem = pl.BlockSpec(memory_space=pltpu.VMEM)
    return pl.pallas_call(
        kernel,
        out_shape=out_shape,
        in_specs=[pl.BlockSpec(memory_space=where[kind]) for kind in memory],
        out_specs=jax.tree.map(lambda _: vmem, out_shape),
        scratch_shapes=scratch,
        cost_estimate=pl.CostEstimate(flops=flops, bytes_accessed=moved, transcendentals=0),
        compiler_params=pltpu.CompilerParams(vmem_limit_bytes=GRANT),
    )


def fetch(plan, spectra, held, sems, m_lo, rows):
    copies = []
    for m_hi in range(plan.m_his):
        start = pl.multiple_of((m_hi * plan.m_los + m_lo) * plan.radix // LANES * LANES, LANES)
        source = spectra.at[:, pl.ds(0, rows), pl.ds(start, LANES)]
        copies.append(pltpu.make_async_copy(source, held.at[m_hi], sems.at[m_hi]))
    return copies


def gathered(plan, held, index, column, within, count):
    piece_lanes = plan.radix // 2
    each = LANES // piece_lanes
    lane = lax.broadcasted_iota(jnp.int32, (count, LANES), 1)
    value = jnp.zeros((count, LANES), jnp.float32)
    for piece in range(each):
        tile = held[column * each + piece, index, :count]
        turned = pltpu.roll(tile, (piece * piece_lanes - within + LANES) % LANES, 1)
        value = jnp.where((lane >= piece * piece_lanes) & (lane < (piece + 1) * piece_lanes), turned, value)
    return value


def held_shape(plan, rows):
    return jax.ShapeDtypeStruct((plan.m_his, 2 * plan.rounds, rows, LANES), jnp.float32)


def bundle(plan):
    def kernel(near, held, out, rim):
        place, m_lo, _ = spot(plan)
        within = rim_m_lo(plan, place, m_lo) * plan.radix % LANES + plan.radix // 2
        base = plan.chunk * plan.cols
        out[:base] = near[...]
        for index in range(2 * plan.rounds):
            for column in range(plan.half_cols):
                row = index * plan.half_cols + column
                value = gathered(plan, held, index, column, within, 1)
                out[base + row : base + row + 1] = value
                rim[index : index + 1, column * LANES : (column + 1) * LANES] = value

    shape = jax.ShapeDtypeStruct
    rows = plan.chunk * plan.cols + 2 * plan.rounds * plan.half_cols
    out_shape = (shape((rows, LANES), jnp.float32), shape((2 * plan.rounds, plan.half), jnp.float32))
    return call(kernel, out_shape, ["vmem"] * 2)


def opposite(plan):
    def kernel(held, other, out):
        m_lo = plan.m_los - 1 - spot(plan)[1]
        within = m_lo * plan.radix % LANES + plan.radix // 2
        base = plan.chunk * plan.cols
        for index in range(2 * plan.rounds):
            for column in range(plan.half_cols):
                lanes = slice(column * LANES, (column + 1) * LANES)
                out[index, :, lanes] = gathered(plan, held, index, column, within, plan.freq_rows)
                row = base + index * plan.half_cols + column
                out[index, :1, lanes] = other[row : row + 1]

    shape = jax.ShapeDtypeStruct((2 * plan.rounds, plan.freq_rows, plan.half), jnp.float32)
    return call(kernel, shape, ["vmem"] * 2)


def prepare(plan):
    def kernel(*refs):
        first, twist, second, near, held, facing, rim = refs[7:14]
        first_rows, first_part, twist_rows, twist_part = refs[14:18]
        sems, held_sems, facing_sems, rim_sems = refs[18:]
        place, m_lo, _ = spot(plan)
        targets = (first_rows, first_part, twist_rows, twist_part, second, near)
        copies = [
            pltpu.make_async_copy(source, target, sems.at[index])
            for index, (source, target) in enumerate(zip(refs[:6], targets))
        ]
        copies += fetch(plan, refs[6], facing, facing_sems, plan.m_los - 1 - m_lo, plan.freq_rows)
        copies += fetch(plan, refs[6], held, held_sems, m_lo, plan.freq_rows)
        copies += fetch(plan, refs[6], rim, rim_sems, rim_m_lo(plan, place, m_lo), TILE)
        for copy in copies:
            copy.start()
        copies[0].wait()
        copies[1].wait()
        part_cos = first_part[pl.ds(place, 1), 0, :]
        part_sin = first_part[pl.ds(place, 1), 1, :]
        rows = plan.rows
        first[0, :rows], first[1, :rows] = split(first_rows[0] * part_cos - first_rows[1] * part_sin)
        first[0, rows:], first[1, rows:] = split(first_rows[0] * part_sin + first_rows[1] * part_cos)
        copies[2].wait()
        copies[3].wait()
        part_cos = twist_part[pl.ds(place, 1), 0, :]
        part_sin = twist_part[pl.ds(place, 1), 1, :]
        twist[0] = twist_rows[0] * part_cos - twist_rows[1] * part_sin
        twist[1] = twist_rows[0] * part_sin + twist_rows[1] * part_cos
        for copy in copies[4:]:
            copy.wait()

    shape = jax.ShapeDtypeStruct
    out_shape = (
        shape((2, 2 * plan.rows, plan.n1s), jnp.bfloat16),
        shape((2, plan.rows, plan.side), jnp.float32),
        shape((2, plan.side, 2 * plan.half), jnp.bfloat16),
        shape((plan.chunk * plan.cols, LANES), jnp.float32),
        held_shape(plan, plan.freq_rows),
        held_shape(plan, plan.freq_rows),
        held_shape(plan, TILE),
    )
    scratch = [
        pltpu.VMEM((2, plan.rows, plan.n1s), jnp.float32),
        pltpu.VMEM((plan.quarters, 2, plan.n1s), jnp.float32),
        pltpu.VMEM((2, plan.rows, plan.side), jnp.float32),
        pltpu.VMEM((plan.quarters, 2, plan.side), jnp.float32),
        pltpu.SemaphoreType.DMA((6,)),
        pltpu.SemaphoreType.DMA((plan.m_his,)),
        pltpu.SemaphoreType.DMA((plan.m_his,)),
        pltpu.SemaphoreType.DMA((plan.m_his,)),
    ]
    return call(kernel, out_shape, ["hbm"] * 7, scratch)


def resident(plan):
    def kernel(first, held, last, own):
        _, m_lo, _ = spot(plan)
        last[0], last[1] = split((first[0].astype(jnp.float32) + first[1].astype(jnp.float32)).T)
        within = m_lo * plan.radix % LANES
        for index in range(2 * plan.rounds):
            for column in range(plan.half_cols):
                own[index, column] = gathered(plan, held, index, column, within, plan.freq_rows)

    shape = jax.ShapeDtypeStruct
    out_shape = (
        shape((2, plan.n1s, 2 * plan.rows), jnp.bfloat16),
        shape((2 * plan.rounds, plan.half_cols, plan.freq_rows, LANES), jnp.float32),
    )
    return call(kernel, out_shape, ["vmem"] * 2)


def blend(plan, rides):
    def kernel(own, arrived, rim, out):
        place, m_lo, _ = spot(plan)
        special = (place == 0) & (m_lo == 0)
        count = 2 * plan.rounds * plan.freq_rows
        row = lax.broadcasted_iota(jnp.int32, (count, count), 0)
        column = lax.broadcasted_iota(jnp.int32, (count, count), 1)
        within = row % plan.freq_rows
        turn = (row + column == 2 * (row - within) + plan.freq_rows) & (within != 0)
        turn = jnp.where(turn, 1.0, 0.0).astype(jnp.bfloat16)
        row = lax.broadcasted_iota(jnp.int32, (plan.half, plan.half), 0)
        column = lax.broadcasted_iota(jnp.int32, (plan.half, plan.half), 1)
        flip = jnp.where(row + column == plan.half - 1, 1.0, 0.0).astype(jnp.bfloat16)
        dot = lambda a, b: jnp.dot(a, b, preferred_element_type=jnp.float32)
        high, low = split(arrived[...].reshape(count, plan.half))
        total = dot(dot(turn, high).astype(jnp.bfloat16), flip) + dot(dot(turn, low).astype(jnp.bfloat16), flip)
        paired = rim[...]
        if rides:
            top = jnp.concatenate([arrived[index, :1] for index in range(2 * plan.rounds)], axis=0)
            paired = jnp.where(lax.rem(place, 2) == 1, top, paired)
        high, low = split(paired)
        edge = dot(high, flip) + dot(low, flip)
        lane = lax.broadcasted_iota(jnp.int32, edge.shape, 1)
        later = pltpu.roll(edge, plan.radix // 2, 1)
        later = jnp.where(lane < plan.radix // 2, pltpu.roll(later, 1, 1), later)
        edge = jnp.where(special, later, edge)
        top = lax.broadcasted_iota(jnp.int32, (plan.freq_rows, LANES), 0) == 0
        corner = top & (lax.broadcasted_iota(jnp.int32, (plan.freq_rows, LANES), 1) == 0)
        corner = corner & special
        scale = 1.0 / plan.length
        for step in range(plan.rounds):
            for column in range(plan.half_cols):
                lanes = slice(column * LANES, (column + 1) * LANES)
                whole = []
                for part in range(2):
                    index = 2 * step + part
                    there = total[index * plan.freq_rows : (index + 1) * plan.freq_rows, lanes]
                    there = jnp.where(top, edge[index : index + 1, lanes], there)
                    here = own[index, column]
                    if column == 0:
                        there = jnp.where(corner, here if part else 0.0, there)
                    whole.append((here - there if part else here + there) * scale)
                out[3 * step, column] = whole[0]
                out[3 * step + 1, column] = whole[1]
                if column == 0:
                    whole[0] = jnp.where(corner, rim[2 * step : 2 * step + 1, lanes] * scale, whole[0])
                out[3 * step + 2, column] = whole[0]

    shape = jax.ShapeDtypeStruct((3 * plan.rounds, plan.half_cols, plan.freq_rows, LANES), jnp.float32)
    return call(kernel, shape, ["vmem"] * 3)


def alternating(plan, count):
    lane = lax.broadcasted_iota(jnp.int32, (count, plan.side), 1)
    return jnp.where(lane % 2 == 0, 1.0, -1.0)


def packed_rows(plan, part, column):
    start = (part * plan.half_cols + column) * plan.slice_rows
    return slice(start, start + plan.slice_rows)


def forward(plan):
    def kernel(*refs):
        limbs = refs[: plan.quarters]
        first, twist, second, out, matrix, turned = refs[plan.quarters :]
        place = spot(plan)[0]
        for index in range(plan.quarters):
            start = pl.multiple_of((place ^ index) * plan.chunk, 8)
            for column in range(plan.cols):
                matrix[pl.ds(start, plan.chunk), column * LANES : (column + 1) * LANES] = limbs[index][
                    pl.ds(column, plan.chunk, stride=plan.cols), :
                ]
        value = product((first[0], first[1]), split(matrix[...]))
        rows = plan.rows
        real, imag = value[:rows], value[rows:]
        turned[:rows] = real * twist[0] - imag * twist[1]
        turned[rows:] = real * twist[1] + imag * twist[0]
        middle = jnp.sum(turned[:1] * alternating(plan, 1), axis=1, keepdims=True)
        middle = jnp.where(place == 0, middle, 0.0)
        value = product(split(turned[...]), (second[0], second[1]))
        by_cos, by_sin = value[:, : plan.half], value[:, plan.half :]
        main = (by_cos[:rows] + by_sin[rows:], by_cos[rows:] - by_sin[:rows])
        corner = lax.broadcasted_iota(jnp.int32, (plan.slice_rows, LANES), 0) == 0
        corner = corner & (lax.broadcasted_iota(jnp.int32, (plan.slice_rows, LANES), 1) == 0)
        for group in range(plan.groups):
            for part in range(2):
                for column in range(plan.half_cols):
                    lanes = slice(column * LANES, (column + 1) * LANES)
                    tile = main[part][group * plan.slice_rows : (group + 1) * plan.slice_rows, lanes]
                    if (group, part, column) == (0, 1, 0):
                        tile = tile + jnp.where(corner, middle, 0.0)
                    out[group, packed_rows(plan, part, column)] = tile

    shape = jax.ShapeDtypeStruct((plan.groups, plan.packed, LANES), jnp.float32)
    scratch = [
        pltpu.VMEM((plan.n1s, plan.side), jnp.float32),
        pltpu.VMEM((2 * plan.rows, plan.side), jnp.float32),
    ]
    return call(kernel, shape, ["vmem"] * (plan.quarters + 3), scratch)


def combine(plan):
    def kernel(spectra, own, out):
        place, _, first_row = spot(plan)
        row = lax.broadcasted_iota(jnp.int32, (plan.slice_rows, LANES), 0) + first_row + place * plan.freq_rows
        sign = jnp.where(row % 2 == 0, 1.0, -1.0)

        def one_block(block, carry):
            sums = [jnp.zeros((plan.slice_rows, LANES), jnp.float32) for _ in range(2 * plan.half_cols)]
            for step in range(plan.rounds):
                here = lax.rem(block + (plan.rounds * STRIDE * plan.groups - step * STRIDE), plan.groups)
                before = lax.rem(here + (plan.groups - 1), plan.groups)
                for column in range(plan.half_cols):
                    real, imag = (
                        spectra[here, packed_rows(plan, part, column)]
                        + sign * spectra[before, packed_rows(plan, part, column)]
                        for part in range(2)
                    )
                    own_r, own_i, own_c = (own[3 * step + part, column] for part in range(3))
                    sums[column] = sums[column] + own_r * real - own_i * imag
                    sums[plan.half_cols + column] = sums[plan.half_cols + column] + own_c * imag + own_i * real
            for part in range(2):
                for column in range(plan.half_cols):
                    out[block, packed_rows(plan, part, column)] = sums[part * plan.half_cols + column]
            return carry

        lax.fori_loop(0, plan.groups, one_block, 0)

    shape = jax.ShapeDtypeStruct((plan.groups, plan.packed, LANES), jnp.float32)
    return call(kernel, shape, ["vmem"] * 2)


def backward(plan):
    def kernel(spectra, last, twist, second, out, stack, spread, matrix):
        place = spot(plan)[0]
        rows = plan.rows
        for part in range(2):
            for column in range(plan.half_cols):
                lanes = slice(column * LANES, (column + 1) * LANES)
                for group in range(plan.groups):
                    start = part * rows + group * plan.slice_rows
                    stack[start : start + plan.slice_rows, lanes] = spectra[group, packed_rows(plan, part, column)]
        value = split(stack[...])
        by_cos = product(value, (second[0, :, : plan.half], second[1, :, : plan.half]), True)
        by_sin = product(value, (second[0, :, plan.half :], second[1, :, plan.half :]), True)
        spread[:rows] = by_cos[:rows] - by_sin[rows:]
        spread[rows:] = by_cos[rows:] + by_sin[:rows]
        middle = jnp.where(place == 0, stack[rows : rows + 1, :1], 0.0)
        spread[:1] = spread[:1] + middle * alternating(plan, 1)
        real, imag = spread[:rows], spread[rows:]
        turned = jnp.concatenate([real * twist[0] + imag * twist[1], imag * twist[0] - real * twist[1]], axis=0)
        matrix[...] = product((last[0], last[1]), split(turned))
        for index in range(plan.quarters):
            start = pl.multiple_of((place ^ index) * plan.chunk, 8)
            for column in range(plan.cols):
                out[index, pl.ds(column, plan.chunk, stride=plan.cols), :] = matrix[
                    pl.ds(start, plan.chunk), column * LANES : (column + 1) * LANES
                ]

    shape = jax.ShapeDtypeStruct((plan.quarters, plan.chunk * plan.cols, LANES), jnp.float32)
    scratch = [
        pltpu.VMEM((2 * plan.rows, plan.half), jnp.float32),
        pltpu.VMEM((2 * plan.rows, plan.side), jnp.float32),
        pltpu.VMEM((plan.n1s, plan.side), jnp.float32),
    ]
    return call(kernel, shape, ["vmem"] * 4, scratch)


def swapped(value, bit):
    count = lax.axis_size("acc")
    return lax.ppermute(value, "acc", [(source, source ^ bit) for source in range(count)])


def per_device(reciprocal_spectra, divisor):
    rounds, _, freq_rows, plane = reciprocal_spectra.shape
    quarters = lax.axis_size("acc")
    groups = lax.axis_size("blk") * lax.axis_size("tail")
    plan = Plan(freq_rows, plane, quarters, groups, rounds)
    constants = [jnp.asarray(table) for table in tables(plan)]

    limbs = divisor.reshape(plan.chunk * plan.cols, LANES)
    spectra = reciprocal_spectra.reshape(2 * rounds, freq_rows, plane)
    first, twist, second, near, held, facing, rim = prepare(plan)(*map(far, constants + [limbs, spectra]))
    bundled, rim = bundle(plan)(near, rim)
    pieces = {0: limbs}
    bit = quarters // 2
    while bit:
        for index, piece in list(pieces.items()):
            pieces[index | bit] = swapped(bundled if bit == 1 and index == 0 else piece, bit)
        bit //= 2
    pieces[0] = near
    facing = swapped(opposite(plan)(facing, pieces[1]), quarters - 1)
    rides = quarters <= 4
    if not rides:
        rim = lax.ppermute(rim, "acc", [(source, -source % quarters) for source in range(quarters)])
    last, own = resident(plan)(first, held)

    own_spectrum = forward(plan)(*[pieces[index] for index in range(quarters)], first, twist, second)
    own = blend(plan, rides)(own, facing, rim)
    if plan.per > 1:
        first_row = lax.axis_index(("blk", "tail")) % plan.per * plan.slice_rows
        own = lax.dynamic_slice_in_dim(own, first_row, plan.slice_rows, 2)
    every = lax.all_to_all(own_spectrum, ("blk", "tail"), 0, 0, tiled=True)
    sums = combine(plan)(every, own)
    back = lax.all_to_all(sums, ("blk", "tail"), 0, 0, tiled=True)
    slots = backward(plan)(back, last, twist, second)

    held = {index: slots[index] for index in range(quarters)}
    bit = 1
    while bit < quarters:
        sent = sorted(index for index in held if index & bit)
        arrived = swapped(jnp.stack([held[index] for index in sent]), bit)
        held = {index ^ bit: held[index ^ bit] + arrived[where] for where, index in enumerate(sent)}
        bit *= 2
    return held[0].reshape(divisor.shape)


def solution(mesh):
    in_specs = (P(None, None, "acc", None), P(("blk", "tail"), "acc"))
    out_specs = P(("blk", "tail"), "acc")
    return jax.shard_map(per_device, mesh=mesh, in_specs=in_specs, out_specs=out_specs, check_vma=False)
```

```python
import math

import jax
import jax.numpy as jnp
import numpy as np
from jax import lax
from jax.experimental import pallas as pl
from jax.experimental.pallas import tpu as pltpu
from jax.sharding import PartitionSpec as P


LANES = 128
TILE = 8
PIECES = 2
GRANT = 16 * 1024 * 1024
STRIDE = 2


class Plan:
    def __init__(self, freq_rows, plane, quarters, groups, rounds):
        self.rounds = rounds
        self.quarters = quarters
        self.groups = groups
        self.freq_rows = freq_rows
        self.radix = freq_rows * quarters
        self.length = self.radix * plane
        self.side = math.isqrt(self.length)
        self.half = self.side // 2
        self.m_los = self.side // self.radix
        self.m_his = self.radix // self.m_los
        self.rows = self.m_los * freq_rows
        self.n1s = self.side // 2
        self.chunk = self.n1s // quarters
        self.cols = self.side // LANES
        self.half_cols = self.half // LANES
        self.slice_rows = self.rows // groups
        self.per = groups // self.m_los
        self.packed = 2 * self.half_cols * self.slice_rows


def tables(plan):
    row = (np.arange(plan.m_los)[:, None] * plan.radix + np.arange(plan.freq_rows)[None, :]).reshape(-1)
    part = np.arange(plan.quarters) * plan.freq_rows
    n1 = np.arange(plan.n1s)
    n2 = np.arange(plan.side)
    f2 = (np.arange(plan.m_his)[:, None] + plan.m_los * np.arange(plan.radix // 2)[None, :]).reshape(-1)

    def wave(first, second, modulus):
        angle = (first[:, None] * second[None, :] % modulus) * (-2.0 * math.pi / modulus)
        return np.stack([np.cos(angle), np.sin(angle)])

    first_rows = wave(row, n1, plan.side)
    first_part = wave(part, n1, plan.side)
    twist_rows = wave(row, n2, plan.length)
    twist_part = wave(part, n2, plan.length)
    cosine, sine = wave(n2, f2, plan.side)
    second = np.concatenate([cosine, -sine], axis=1)
    second_high = second.astype(jnp.bfloat16)
    second_low = (second - second_high.astype(np.float64)).astype(jnp.bfloat16)
    single = lambda value: value.astype(np.float32)
    return (
        single(first_rows),
        single(first_part.transpose(1, 0, 2)),
        single(twist_rows),
        single(twist_part.transpose(1, 0, 2)),
        np.stack([second_high, second_low]),
    )


def spot(plan):
    place = lax.axis_index("acc")
    group = lax.axis_index("blk") * lax.axis_size("tail") + lax.axis_index("tail")
    if plan.per == 1:
        return place, group, 0
    return place, lax.div(group, plan.per), lax.rem(group, plan.per) * plan.slice_rows


def rim_m_lo(plan, place, m_lo):
    return jnp.where(place == 0, lax.rem(plan.m_los - m_lo, plan.m_los), plan.m_los - 1 - m_lo)


def far(value):
    return pltpu.with_memory_space_constraint(value, pltpu.HBM)


def split(value):
    high = value.astype(jnp.bfloat16)
    low = (value - high.astype(jnp.float32)).astype(jnp.bfloat16)
    return high, low


def product(first, second, transposed=False):
    dims = (((1,), (1 if transposed else 0,)), ((), ()))
    dot = lambda a, b: lax.dot_general(a, b, dims, preferred_element_type=jnp.float32)
    return dot(first[0], second[0]) + (dot(first[1], second[0]) + dot(first[0], second[1]))


def call(kernel, out_shape, memory, scratch=(), result="vmem", flops=1_000_000, moved=1_000_000):
    where = {"vmem": pltpu.VMEM, "hbm": pltpu.HBM}
    out_spec = pl.BlockSpec(memory_space=where[result])
    return pl.pallas_call(
        kernel,
        out_shape=out_shape,
        in_specs=[pl.BlockSpec(memory_space=where[kind]) for kind in memory],
        out_specs=jax.tree.map(lambda _: out_spec, out_shape),
        scratch_shapes=scratch,
        cost_estimate=pl.CostEstimate(flops=flops, bytes_accessed=moved, transcendentals=0),
        compiler_params=pltpu.CompilerParams(vmem_limit_bytes=GRANT),
    )


def fetch(plan, spectra, held, sems, m_lo, rows):
    copies = []
    for m_hi in range(plan.m_his):
        start = pl.multiple_of((m_hi * plan.m_los + m_lo) * plan.radix // LANES * LANES, LANES)
        source = spectra.at[:, pl.ds(0, rows), pl.ds(start, LANES)]
        copies.append(pltpu.make_async_copy(source, held.at[m_hi], sems.at[m_hi]))
    return copies


def gathered(plan, held, index, column, within, count):
    piece_lanes = plan.radix // 2
    each = LANES // piece_lanes
    lane = lax.broadcasted_iota(jnp.int32, (count, LANES), 1)
    value = jnp.zeros((count, LANES), jnp.float32)
    for piece in range(each):
        tile = held[column * each + piece, index, :count]
        turned = pltpu.roll(tile, (piece * piece_lanes - within + LANES) % LANES, 1)
        value = jnp.where((lane >= piece * piece_lanes) & (lane < (piece + 1) * piece_lanes), turned, value)
    return value


def held_shape(plan, rows):
    return jax.ShapeDtypeStruct((plan.m_his, 2 * plan.rounds, rows, LANES), jnp.float32)


def bundle(plan):
    def kernel(near, held, out, rim):
        place, m_lo, _ = spot(plan)
        within = rim_m_lo(plan, place, m_lo) * plan.radix % LANES + plan.radix // 2
        base = plan.chunk * plan.cols
        out[:base] = near[...]
        for index in range(2 * plan.rounds):
            for column in range(plan.half_cols):
                row = index * plan.half_cols + column
                value = gathered(plan, held, index, column, within, 1)
                out[base + row : base + row + 1] = value
                rim[index : index + 1, column * LANES : (column + 1) * LANES] = value

    shape = jax.ShapeDtypeStruct
    rows = plan.chunk * plan.cols + 2 * plan.rounds * plan.half_cols
    out_shape = (shape((rows, LANES), jnp.float32), shape((2 * plan.rounds, plan.half), jnp.float32))
    return call(kernel, out_shape, ["vmem"] * 2)


def flipped(plan, value):
    row = lax.broadcasted_iota(jnp.int32, (plan.half, plan.half), 0)
    column = lax.broadcasted_iota(jnp.int32, (plan.half, plan.half), 1)
    flip = jnp.where(row + column == plan.half - 1, 1.0, 0.0).astype(jnp.bfloat16)
    high, low = value
    dot = lambda a: jnp.dot(a, flip, preferred_element_type=jnp.float32)
    return dot(high) + dot(low)


def opposite(plan):
    def kernel(held, other, out, stack):
        m_lo = plan.m_los - 1 - spot(plan)[1]
        within = m_lo * plan.radix % LANES + plan.radix // 2
        base = plan.chunk * plan.cols
        rows = plan.freq_rows
        for index in range(2 * plan.rounds):
            for column in range(plan.half_cols):
                lanes = slice(column * LANES, (column + 1) * LANES)
                stack[index * rows : (index + 1) * rows, lanes] = gathered(plan, held, index, column, within, rows)
                row = base + index * plan.half_cols + column
                stack[index * rows : index * rows + 1, lanes] = other[row : row + 1]
        count = 2 * plan.rounds * rows
        row = lax.broadcasted_iota(jnp.int32, (count, count), 0)
        column = lax.broadcasted_iota(jnp.int32, (count, count), 1)
        inside = row % rows
        target = jnp.where(inside == 0, row, 2 * (row - inside) + rows - row)
        turn = jnp.where(column == target, 1.0, 0.0).astype(jnp.bfloat16)
        dot = lambda a: jnp.dot(turn, a, preferred_element_type=jnp.float32).astype(jnp.bfloat16)
        high, low = split(stack[...])
        out[...] = flipped(plan, (dot(high), dot(low))).reshape(out.shape)

    shape = jax.ShapeDtypeStruct((2 * plan.rounds, plan.freq_rows, plan.half), jnp.float32)
    scratch = [pltpu.VMEM((2 * plan.rounds * plan.freq_rows, plan.half), jnp.float32)]
    return call(kernel, shape, ["vmem"] * 2, scratch)


def prepare(plan):
    def kernel(*refs):
        first, twist, second, near, held, facing, rim = refs[7:14]
        first_rows, first_part, twist_rows, twist_part = refs[14:18]
        sems, held_sems, facing_sems, rim_sems = refs[18:]
        place, m_lo, _ = spot(plan)
        targets = (first_rows, first_part, twist_rows, twist_part, second, near)
        copies = [
            pltpu.make_async_copy(source, target, sems.at[index])
            for index, (source, target) in enumerate(zip(refs[:6], targets))
        ]
        copies += fetch(plan, refs[6], facing, facing_sems, plan.m_los - 1 - m_lo, plan.freq_rows)
        copies += fetch(plan, refs[6], held, held_sems, m_lo, plan.freq_rows)
        copies += fetch(plan, refs[6], rim, rim_sems, rim_m_lo(plan, place, m_lo), TILE)
        for copy in copies:
            copy.start()
        copies[0].wait()
        copies[1].wait()
        part_cos = first_part[pl.ds(place, 1), 0, :]
        part_sin = first_part[pl.ds(place, 1), 1, :]
        rows = plan.rows
        first[0, :rows], first[1, :rows] = split(first_rows[0] * part_cos - first_rows[1] * part_sin)
        first[0, rows:], first[1, rows:] = split(first_rows[0] * part_sin + first_rows[1] * part_cos)
        copies[2].wait()
        copies[3].wait()
        part_cos = twist_part[pl.ds(place, 1), 0, :]
        part_sin = twist_part[pl.ds(place, 1), 1, :]
        twist[0] = twist_rows[0] * part_cos - twist_rows[1] * part_sin
        twist[1] = twist_rows[0] * part_sin + twist_rows[1] * part_cos
        for copy in copies[4:]:
            copy.wait()

    shape = jax.ShapeDtypeStruct
    out_shape = (
        shape((2, 2 * plan.rows, plan.n1s), jnp.bfloat16),
        shape((2, plan.rows, plan.side), jnp.float32),
        shape((2, plan.side, 2 * plan.half), jnp.bfloat16),
        shape((plan.chunk * plan.cols, LANES), jnp.float32),
        held_shape(plan, plan.freq_rows),
        held_shape(plan, plan.freq_rows),
        held_shape(plan, TILE),
    )
    scratch = [
        pltpu.VMEM((2, plan.rows, plan.n1s), jnp.float32),
        pltpu.VMEM((plan.quarters, 2, plan.n1s), jnp.float32),
        pltpu.VMEM((2, plan.rows, plan.side), jnp.float32),
        pltpu.VMEM((plan.quarters, 2, plan.side), jnp.float32),
        pltpu.SemaphoreType.DMA((6,)),
        pltpu.SemaphoreType.DMA((plan.m_his,)),
        pltpu.SemaphoreType.DMA((plan.m_his,)),
        pltpu.SemaphoreType.DMA((plan.m_his,)),
    ]
    return call(kernel, out_shape, ["hbm"] * 7, scratch)


def resident(plan):
    def kernel(first, held, rim, last, own, edge):
        place, m_lo, _ = spot(plan)
        last[0], last[1] = split((first[0].astype(jnp.float32) + first[1].astype(jnp.float32)).T)
        within = m_lo * plan.radix % LANES
        for index in range(2 * plan.rounds):
            for column in range(plan.half_cols):
                own[index, column] = gathered(plan, held, index, column, within, plan.freq_rows)
        value = flipped(plan, split(rim[...]))
        lane = lax.broadcasted_iota(jnp.int32, value.shape, 1)
        later = pltpu.roll(value, plan.radix // 2, 1)
        later = jnp.where(lane < plan.radix // 2, pltpu.roll(later, 1, 1), later)
        edge[...] = jnp.where((place == 0) & (m_lo == 0), later, value)

    shape = jax.ShapeDtypeStruct
    out_shape = (
        shape((2, plan.n1s, 2 * plan.rows), jnp.bfloat16),
        shape((2 * plan.rounds, plan.half_cols, plan.freq_rows, LANES), jnp.float32),
        shape((2 * plan.rounds, plan.half), jnp.float32),
    )
    return call(kernel, out_shape, ["vmem"] * 3)


def blend(plan, rides):
    def kernel(own, arrived, edge, rim, out):
        place, m_lo, _ = spot(plan)
        corner = lax.broadcasted_iota(jnp.int32, (plan.freq_rows, LANES), 0)
        top = corner == 0
        corner = top & (lax.broadcasted_iota(jnp.int32, (plan.freq_rows, LANES), 1) == 0)
        corner = corner & ((place == 0) & (m_lo == 0))
        if rides:
            top = top & (lax.rem(place, 2) == 0)
        scale = 1.0 / plan.length
        for step in range(plan.rounds):
            for column in range(plan.half_cols):
                lanes = slice(column * LANES, (column + 1) * LANES)
                whole = []
                for part in range(2):
                    index = 2 * step + part
                    there = jnp.where(top, edge[index : index + 1, lanes], arrived[index, :, lanes])
                    here = own[index, column]
                    if column == 0:
                        there = jnp.where(corner, here if part else 0.0, there)
                    whole.append((here - there if part else here + there) * scale)
                out[3 * step, column] = whole[0]
                out[3 * step + 1, column] = whole[1]
                if column == 0:
                    whole[0] = jnp.where(corner, rim[2 * step : 2 * step + 1, lanes] * scale, whole[0])
                out[3 * step + 2, column] = whole[0]

    shape = jax.ShapeDtypeStruct((3 * plan.rounds, plan.half_cols, plan.freq_rows, LANES), jnp.float32)
    return call(kernel, shape, ["vmem"] * 4)


def alternating(plan, count):
    lane = lax.broadcasted_iota(jnp.int32, (count, plan.side), 1)
    return jnp.where(lane % 2 == 0, 1.0, -1.0)


def packed_rows(plan, part, column):
    start = (part * plan.half_cols + column) * plan.slice_rows
    return slice(start, start + plan.slice_rows)


def forward(plan):
    def kernel(*refs):
        limbs = refs[: plan.quarters]
        first, twist, second, out, matrix, turned, packed, sems = refs[plan.quarters :]
        place = spot(plan)[0]
        for index in range(plan.quarters):
            start = pl.multiple_of((place ^ index) * plan.chunk, 8)
            for column in range(plan.cols):
                matrix[pl.ds(start, plan.chunk), column * LANES : (column + 1) * LANES] = limbs[index][
                    pl.ds(column, plan.chunk, stride=plan.cols), :
                ]
        value = product((first[0], first[1]), split(matrix[...]))
        rows = plan.rows
        real, imag = value[:rows], value[rows:]
        turned[:rows] = real * twist[0] - imag * twist[1]
        turned[rows:] = real * twist[1] + imag * twist[0]
        middle = jnp.sum(turned[:1] * alternating(plan, 1), axis=1, keepdims=True)
        middle = jnp.where(place == 0, middle, 0.0)
        corner = lax.broadcasted_iota(jnp.int32, (plan.slice_rows, LANES), 0) == 0
        corner = corner & (lax.broadcasted_iota(jnp.int32, (plan.slice_rows, LANES), 1) == 0)
        table = (second[0], second[1])
        count, groups = rows // PIECES, plan.groups // PIECES
        copies = []
        for piece in range(PIECES):
            start = piece * count
            both = jnp.concatenate([turned[start : start + count], turned[rows + start : rows + start + count]], axis=0)
            value = product(split(both), table)
            by_cos, by_sin = value[:, : plan.half], value[:, plan.half :]
            main = (by_cos[:count] + by_sin[count:], by_cos[count:] - by_sin[:count])
            for index in range(groups):
                group = piece * groups + index
                for part in range(2):
                    for column in range(plan.half_cols):
                        lanes = slice(column * LANES, (column + 1) * LANES)
                        tile = main[part][index * plan.slice_rows : (index + 1) * plan.slice_rows, lanes]
                        if (group, part, column) == (0, 1, 0):
                            tile = tile + jnp.where(corner, middle, 0.0)
                        packed[group, packed_rows(plan, part, column)] = tile
            where = pl.ds(piece * groups, groups)
            copies.append(pltpu.make_async_copy(packed.at[where], out.at[where], sems.at[piece]))
            copies[-1].start()
        for copy in copies:
            copy.wait()

    shape = jax.ShapeDtypeStruct((plan.groups, plan.packed, LANES), jnp.float32)
    scratch = [
        pltpu.VMEM((plan.n1s, plan.side), jnp.float32),
        pltpu.VMEM((2 * plan.rows, plan.side), jnp.float32),
        pltpu.VMEM((plan.groups, plan.packed, LANES), jnp.float32),
        pltpu.SemaphoreType.DMA((PIECES,)),
    ]
    return call(kernel, shape, ["vmem"] * (plan.quarters + 3), scratch, "hbm")


def combine(plan):
    def kernel(spectra, own, out):
        place, _, first_row = spot(plan)
        row = lax.broadcasted_iota(jnp.int32, (plan.slice_rows, LANES), 0) + first_row + place * plan.freq_rows
        sign = jnp.where(row % 2 == 0, 1.0, -1.0)

        def one_block(block, carry):
            sums = [jnp.zeros((plan.slice_rows, LANES), jnp.float32) for _ in range(2 * plan.half_cols)]
            for step in range(plan.rounds):
                here = lax.rem(block + (plan.rounds * STRIDE * plan.groups - step * STRIDE), plan.groups)
                before = lax.rem(here + (plan.groups - 1), plan.groups)
                for column in range(plan.half_cols):
                    real, imag = (
                        spectra[here, packed_rows(plan, part, column)]
                        + sign * spectra[before, packed_rows(plan, part, column)]
                        for part in range(2)
                    )
                    own_r, own_i, own_c = (own[3 * step + part, column] for part in range(3))
                    sums[column] = sums[column] + own_r * real - own_i * imag
                    sums[plan.half_cols + column] = sums[plan.half_cols + column] + own_c * imag + own_i * real
            for part in range(2):
                for column in range(plan.half_cols):
                    out[block, packed_rows(plan, part, column)] = sums[part * plan.half_cols + column]
            return carry

        lax.fori_loop(0, plan.groups, one_block, 0)

    shape = jax.ShapeDtypeStruct((plan.groups, plan.packed, LANES), jnp.float32)
    return call(kernel, shape, ["vmem"] * 2)


def backward(plan):
    def kernel(spectra, last, twist, second, out, stack, spread, matrix):
        place = spot(plan)[0]
        rows = plan.rows
        for part in range(2):
            for column in range(plan.half_cols):
                lanes = slice(column * LANES, (column + 1) * LANES)
                for group in range(plan.groups):
                    start = part * rows + group * plan.slice_rows
                    stack[start : start + plan.slice_rows, lanes] = spectra[group, packed_rows(plan, part, column)]
        value = split(stack[...])
        by_cos = product(value, (second[0, :, : plan.half], second[1, :, : plan.half]), True)
        by_sin = product(value, (second[0, :, plan.half :], second[1, :, plan.half :]), True)
        spread[:rows] = by_cos[:rows] - by_sin[rows:]
        spread[rows:] = by_cos[rows:] + by_sin[:rows]
        middle = jnp.where(place == 0, stack[rows : rows + 1, :1], 0.0)
        spread[:1] = spread[:1] + middle * alternating(plan, 1)
        real, imag = spread[:rows], spread[rows:]
        turned = jnp.concatenate([real * twist[0] + imag * twist[1], imag * twist[0] - real * twist[1]], axis=0)
        matrix[...] = product((last[0], last[1]), split(turned))
        for index in range(plan.quarters):
            start = pl.multiple_of((place ^ index) * plan.chunk, 8)
            for column in range(plan.cols):
                out[index, pl.ds(column, plan.chunk, stride=plan.cols), :] = matrix[
                    pl.ds(start, plan.chunk), column * LANES : (column + 1) * LANES
                ]

    shape = jax.ShapeDtypeStruct((plan.quarters, plan.chunk * plan.cols, LANES), jnp.float32)
    scratch = [
        pltpu.VMEM((2 * plan.rows, plan.half), jnp.float32),
        pltpu.VMEM((2 * plan.rows, plan.side), jnp.float32),
        pltpu.VMEM((plan.n1s, plan.side), jnp.float32),
    ]
    return call(kernel, shape, ["vmem"] * 4, scratch)


def swapped(value, bit):
    count = lax.axis_size("acc")
    return lax.ppermute(value, "acc", [(source, source ^ bit) for source in range(count)])


def per_device(reciprocal_spectra, divisor):
    rounds, _, freq_rows, plane = reciprocal_spectra.shape
    quarters = lax.axis_size("acc")
    groups = lax.axis_size("blk") * lax.axis_size("tail")
    plan = Plan(freq_rows, plane, quarters, groups, rounds)
    constants = [jnp.asarray(table) for table in tables(plan)]

    limbs = divisor.reshape(plan.chunk * plan.cols, LANES)
    spectra = reciprocal_spectra.reshape(2 * rounds, freq_rows, plane)
    first, twist, second, near, held, facing, rim = prepare(plan)(*map(far, constants + [limbs, spectra]))
    bundled, rim = bundle(plan)(near, rim)
    pieces = {0: limbs}
    bit = quarters // 2
    while bit:
        for index, piece in list(pieces.items()):
            pieces[index | bit] = swapped(bundled if bit == 1 and index == 0 else piece, bit)
        bit //= 2
    pieces[0] = near
    facing = opposite(plan)(facing, pieces[1])
    facing = swapped(facing, quarters - 1)
    rides = quarters <= 4
    if not rides:
        rim = lax.ppermute(rim, "acc", [(source, -source % quarters) for source in range(quarters)])
    last, own, edge = resident(plan)(first, held, rim)

    own_spectrum = forward(plan)(*[pieces[index] for index in range(quarters)], first, twist, second)
    own = blend(plan, rides)(own, facing, edge, rim)
    if plan.per > 1:
        first_row = lax.axis_index(("blk", "tail")) % plan.per * plan.slice_rows
        own = lax.dynamic_slice_in_dim(own, first_row, plan.slice_rows, 2)
    every = lax.all_to_all(own_spectrum, ("blk", "tail"), 0, 0, tiled=True)
    sums = combine(plan)(every, own)
    back = lax.all_to_all(sums, ("blk", "tail"), 0, 0, tiled=True)
    slots = backward(plan)(back, last, twist, second)

    held = {index: slots[index] for index in range(quarters)}
    bit = 1
    while bit < quarters:
        sent = sorted(index for index in held if index & bit)
        arrived = swapped(jnp.stack([held[index] for index in sent]), bit)
        held = {index ^ bit: held[index ^ bit] + arrived[where] for where, index in enumerate(sent)}
        bit *= 2
    return held[0].reshape(divisor.shape)


def solution(mesh):
    in_specs = (P(None, None, "acc", None), P(("blk", "tail"), "acc"))
    out_specs = P(("blk", "tail"), "acc")
    return jax.shard_map(per_device, mesh=mesh, in_specs=in_specs, out_specs=out_specs, check_vma=False)
```

```python
import math

import jax
import jax.numpy as jnp
import numpy as np
from jax import lax
from jax.experimental import pallas as pl
from jax.experimental.pallas import tpu as pltpu
from jax.sharding import PartitionSpec as P


LANES = 128
TILE = 8
PIECES = 2
GRANT = 16 * 1024 * 1024
STRIDE = 2


class Plan:
    def __init__(self, freq_rows, plane, quarters, groups, rounds):
        self.rounds = rounds
        self.quarters = quarters
        self.groups = groups
        self.freq_rows = freq_rows
        self.radix = freq_rows * quarters
        self.length = self.radix * plane
        self.side = math.isqrt(self.length)
        self.half = self.side // 2
        self.m_los = self.side // self.radix
        self.m_his = self.radix // self.m_los
        self.rows = self.m_los * freq_rows
        self.n1s = self.side // 2
        self.chunk = self.n1s // quarters
        self.cols = self.side // LANES
        self.half_cols = self.half // LANES
        self.slice_rows = self.rows // groups
        self.per = groups // self.m_los
        self.packed = 2 * self.half_cols * self.slice_rows


def tables(plan):
    row = (np.arange(plan.m_los)[:, None] * plan.radix + np.arange(plan.freq_rows)[None, :]).reshape(-1)
    part = np.arange(plan.quarters) * plan.freq_rows
    n1 = np.arange(plan.n1s)
    n2 = np.arange(plan.side)
    f2 = (np.arange(plan.m_his)[:, None] + plan.m_los * np.arange(plan.radix // 2)[None, :]).reshape(-1)

    def wave(first, second, modulus):
        angle = (first[:, None] * second[None, :] % modulus) * (-2.0 * math.pi / modulus)
        return np.stack([np.cos(angle), np.sin(angle)])

    first_rows = wave(row, n1, plan.side)
    first_part = wave(part, n1, plan.side)
    twist_rows = wave(row, n2, plan.length)
    twist_part = wave(part, n2, plan.length)
    cosine, sine = wave(n2, f2, plan.side)
    second = np.concatenate([cosine, -sine], axis=1)
    second_high = second.astype(jnp.bfloat16)
    second_low = (second - second_high.astype(np.float64)).astype(jnp.bfloat16)
    single = lambda value: value.astype(np.float32)
    return (
        single(first_rows),
        single(first_part.transpose(1, 0, 2)),
        single(twist_rows),
        single(twist_part.transpose(1, 0, 2)),
        np.stack([second_high, second_low]),
    )


def spot(plan):
    place = lax.axis_index("acc")
    group = lax.axis_index("blk") * lax.axis_size("tail") + lax.axis_index("tail")
    if plan.per == 1:
        return place, group, 0
    return place, lax.div(group, plan.per), lax.rem(group, plan.per) * plan.slice_rows


def rim_m_lo(plan, place, m_lo):
    return jnp.where(place == 0, lax.rem(plan.m_los - m_lo, plan.m_los), plan.m_los - 1 - m_lo)


def far(value):
    return pltpu.with_memory_space_constraint(value, pltpu.HBM)


def split(value):
    high = value.astype(jnp.bfloat16)
    low = (value - high.astype(jnp.float32)).astype(jnp.bfloat16)
    return high, low


def product(first, second, transposed=False):
    dims = (((1,), (1 if transposed else 0,)), ((), ()))
    dot = lambda a, b: lax.dot_general(a, b, dims, preferred_element_type=jnp.float32)
    return dot(first[0], second[0]) + (dot(first[1], second[0]) + dot(first[0], second[1]))


def call(kernel, out_shape, memory, scratch=(), result="vmem", flops=1_000_000, moved=1_000_000):
    where = {"vmem": pltpu.VMEM, "hbm": pltpu.HBM}
    out_spec = pl.BlockSpec(memory_space=where[result])
    return pl.pallas_call(
        kernel,
        out_shape=out_shape,
        in_specs=[pl.BlockSpec(memory_space=where[kind]) for kind in memory],
        out_specs=jax.tree.map(lambda _: out_spec, out_shape),
        scratch_shapes=scratch,
        cost_estimate=pl.CostEstimate(flops=flops, bytes_accessed=moved, transcendentals=0),
        compiler_params=pltpu.CompilerParams(vmem_limit_bytes=GRANT),
    )


def fetch(plan, spectra, held, sems, m_lo, rows):
    copies = []
    for m_hi in range(plan.m_his):
        start = pl.multiple_of((m_hi * plan.m_los + m_lo) * plan.radix // LANES * LANES, LANES)
        source = spectra.at[:, pl.ds(0, rows), pl.ds(start, LANES)]
        copies.append(pltpu.make_async_copy(source, held.at[m_hi], sems.at[m_hi]))
    return copies


def gathered(plan, held, index, column, within, count):
    piece_lanes = plan.radix // 2
    each = LANES // piece_lanes
    lane = lax.broadcasted_iota(jnp.int32, (count, LANES), 1)
    value = jnp.zeros((count, LANES), jnp.float32)
    for piece in range(each):
        tile = held[column * each + piece, index, :count]
        turned = pltpu.roll(tile, (piece * piece_lanes - within + LANES) % LANES, 1)
        value = jnp.where((lane >= piece * piece_lanes) & (lane < (piece + 1) * piece_lanes), turned, value)
    return value


def held_shape(plan, rows):
    return jax.ShapeDtypeStruct((plan.m_his, 2 * plan.rounds, rows, LANES), jnp.float32)


def bundle(plan):
    def kernel(near, held, out, rim):
        place, m_lo, _ = spot(plan)
        within = rim_m_lo(plan, place, m_lo) * plan.radix % LANES + plan.radix // 2
        base = plan.chunk * plan.cols
        out[:base] = near[...]
        for index in range(2 * plan.rounds):
            for column in range(plan.half_cols):
                row = index * plan.half_cols + column
                value = gathered(plan, held, index, column, within, 1)
                out[base + row : base + row + 1] = value
                rim[index : index + 1, column * LANES : (column + 1) * LANES] = value

    shape = jax.ShapeDtypeStruct
    rows = plan.chunk * plan.cols + 2 * plan.rounds * plan.half_cols
    out_shape = (shape((rows, LANES), jnp.float32), shape((2 * plan.rounds, plan.half), jnp.float32))
    return call(kernel, out_shape, ["vmem"] * 2)


def flipped(plan, value):
    row = lax.broadcasted_iota(jnp.int32, (plan.half, plan.half), 0)
    column = lax.broadcasted_iota(jnp.int32, (plan.half, plan.half), 1)
    flip = jnp.where(row + column == plan.half - 1, 1.0, 0.0).astype(jnp.bfloat16)
    high, low = value
    dot = lambda a: jnp.dot(a, flip, preferred_element_type=jnp.float32)
    return dot(high) + dot(low)


def opposite(plan):
    def kernel(held, other, out, stack):
        m_lo = plan.m_los - 1 - spot(plan)[1]
        within = m_lo * plan.radix % LANES + plan.radix // 2
        base = plan.chunk * plan.cols
        rows = plan.freq_rows
        for index in range(2 * plan.rounds):
            for column in range(plan.half_cols):
                lanes = slice(column * LANES, (column + 1) * LANES)
                stack[index * rows : (index + 1) * rows, lanes] = gathered(plan, held, index, column, within, rows)
                row = base + index * plan.half_cols + column
                stack[index * rows : index * rows + 1, lanes] = other[row : row + 1]
        count = 2 * plan.rounds * rows
        row = lax.broadcasted_iota(jnp.int32, (count, count), 0)
        column = lax.broadcasted_iota(jnp.int32, (count, count), 1)
        inside = row % rows
        target = jnp.where(inside == 0, row, 2 * (row - inside) + rows - row)
        turn = jnp.where(column == target, 1.0, 0.0).astype(jnp.bfloat16)
        dot = lambda a: jnp.dot(turn, a, preferred_element_type=jnp.float32).astype(jnp.bfloat16)
        high, low = split(stack[...])
        out[...] = flipped(plan, (dot(high), dot(low))).reshape(out.shape)

    shape = jax.ShapeDtypeStruct((2 * plan.rounds, plan.freq_rows, plan.half), jnp.float32)
    scratch = [pltpu.VMEM((2 * plan.rounds * plan.freq_rows, plan.half), jnp.float32)]
    return call(kernel, shape, ["vmem"] * 2, scratch)


def prepare(plan):
    def kernel(*refs):
        first, twist, second, near, facing, rim = refs[7:13]
        first_rows, first_part, twist_rows, twist_part = refs[13:17]
        sems, facing_sems, rim_sems = refs[17:]
        place, m_lo, _ = spot(plan)
        targets = (first_rows, first_part, twist_rows, twist_part, second, near)
        copies = [
            pltpu.make_async_copy(source, target, sems.at[index])
            for index, (source, target) in enumerate(zip(refs[:6], targets))
        ]
        copies += fetch(plan, refs[6], facing, facing_sems, plan.m_los - 1 - m_lo, plan.freq_rows)
        copies += fetch(plan, refs[6], rim, rim_sems, rim_m_lo(plan, place, m_lo), TILE)
        for copy in copies:
            copy.start()
        copies[0].wait()
        copies[1].wait()
        part_cos = first_part[pl.ds(place, 1), 0, :]
        part_sin = first_part[pl.ds(place, 1), 1, :]
        rows = plan.rows
        first[0, :rows], first[1, :rows] = split(first_rows[0] * part_cos - first_rows[1] * part_sin)
        first[0, rows:], first[1, rows:] = split(first_rows[0] * part_sin + first_rows[1] * part_cos)
        copies[2].wait()
        copies[3].wait()
        part_cos = twist_part[pl.ds(place, 1), 0, :]
        part_sin = twist_part[pl.ds(place, 1), 1, :]
        twist[0] = twist_rows[0] * part_cos - twist_rows[1] * part_sin
        twist[1] = twist_rows[0] * part_sin + twist_rows[1] * part_cos
        for copy in copies[4:]:
            copy.wait()

    shape = jax.ShapeDtypeStruct
    out_shape = (
        shape((2, 2 * plan.rows, plan.n1s), jnp.bfloat16),
        shape((2, plan.rows, plan.side), jnp.float32),
        shape((2, plan.side, 2 * plan.half), jnp.bfloat16),
        shape((plan.chunk * plan.cols, LANES), jnp.float32),
        held_shape(plan, plan.freq_rows),
        held_shape(plan, TILE),
    )
    scratch = [
        pltpu.VMEM((2, plan.rows, plan.n1s), jnp.float32),
        pltpu.VMEM((plan.quarters, 2, plan.n1s), jnp.float32),
        pltpu.VMEM((2, plan.rows, plan.side), jnp.float32),
        pltpu.VMEM((plan.quarters, 2, plan.side), jnp.float32),
        pltpu.SemaphoreType.DMA((6,)),
        pltpu.SemaphoreType.DMA((plan.m_his,)),
        pltpu.SemaphoreType.DMA((plan.m_his,)),
    ]
    return call(kernel, out_shape, ["hbm"] * 7, scratch)


def resident(plan):
    def kernel(first, spectra, rim, last, own, edge, held, sems):
        place, m_lo, _ = spot(plan)
        copies = fetch(plan, spectra, held, sems, m_lo, plan.freq_rows)
        for copy in copies:
            copy.start()
        last[0], last[1] = split((first[0].astype(jnp.float32) + first[1].astype(jnp.float32)).T)
        value = flipped(plan, split(rim[...]))
        lane = lax.broadcasted_iota(jnp.int32, value.shape, 1)
        later = pltpu.roll(value, plan.radix // 2, 1)
        later = jnp.where(lane < plan.radix // 2, pltpu.roll(later, 1, 1), later)
        edge[...] = jnp.where((place == 0) & (m_lo == 0), later, value)
        for copy in copies:
            copy.wait()
        within = m_lo * plan.radix % LANES
        for index in range(2 * plan.rounds):
            for column in range(plan.half_cols):
                own[index, column] = gathered(plan, held, index, column, within, plan.freq_rows)

    shape = jax.ShapeDtypeStruct
    out_shape = (
        shape((2, plan.n1s, 2 * plan.rows), jnp.bfloat16),
        shape((2 * plan.rounds, plan.half_cols, plan.freq_rows, LANES), jnp.float32),
        shape((2 * plan.rounds, plan.half), jnp.float32),
    )
    held = held_shape(plan, plan.freq_rows)
    scratch = [pltpu.VMEM(held.shape, held.dtype), pltpu.SemaphoreType.DMA((plan.m_his,))]
    return call(kernel, out_shape, ["vmem", "hbm", "vmem"], scratch)


def blend(plan, rides):
    def kernel(own, arrived, edge, rim, out):
        place, m_lo, _ = spot(plan)
        corner = lax.broadcasted_iota(jnp.int32, (plan.freq_rows, LANES), 0)
        top = corner == 0
        corner = top & (lax.broadcasted_iota(jnp.int32, (plan.freq_rows, LANES), 1) == 0)
        corner = corner & ((place == 0) & (m_lo == 0))
        if rides:
            top = top & (lax.rem(place, 2) == 0)
        scale = 1.0 / plan.length
        for step in range(plan.rounds):
            for column in range(plan.half_cols):
                lanes = slice(column * LANES, (column + 1) * LANES)
                whole = []
                for part in range(2):
                    index = 2 * step + part
                    there = jnp.where(top, edge[index : index + 1, lanes], arrived[index, :, lanes])
                    here = own[index, column]
                    if column == 0:
                        there = jnp.where(corner, here if part else 0.0, there)
                    whole.append((here - there if part else here + there) * scale)
                out[3 * step, column] = whole[0]
                out[3 * step + 1, column] = whole[1]
                if column == 0:
                    whole[0] = jnp.where(corner, rim[2 * step : 2 * step + 1, lanes] * scale, whole[0])
                out[3 * step + 2, column] = whole[0]

    shape = jax.ShapeDtypeStruct((3 * plan.rounds, plan.half_cols, plan.freq_rows, LANES), jnp.float32)
    return call(kernel, shape, ["vmem"] * 4)


def alternating(plan, count):
    lane = lax.broadcasted_iota(jnp.int32, (count, plan.side), 1)
    return jnp.where(lane % 2 == 0, 1.0, -1.0)


def packed_rows(plan, part, column):
    start = (part * plan.half_cols + column) * plan.slice_rows
    return slice(start, start + plan.slice_rows)


def forward(plan):
    def kernel(*refs):
        limbs = refs[: plan.quarters]
        first, twist, second, out, matrix, turned, packed, sems = refs[plan.quarters :]
        place = spot(plan)[0]
        for index in range(plan.quarters):
            start = pl.multiple_of((place ^ index) * plan.chunk, 8)
            for column in range(plan.cols):
                matrix[pl.ds(start, plan.chunk), column * LANES : (column + 1) * LANES] = limbs[index][
                    pl.ds(column, plan.chunk, stride=plan.cols), :
                ]
        value = product((first[0], first[1]), split(matrix[...]))
        rows = plan.rows
        real, imag = value[:rows], value[rows:]
        turned[:rows] = real * twist[0] - imag * twist[1]
        turned[rows:] = real * twist[1] + imag * twist[0]
        middle = jnp.sum(turned[:1] * alternating(plan, 1), axis=1, keepdims=True)
        middle = jnp.where(place == 0, middle, 0.0)
        corner = lax.broadcasted_iota(jnp.int32, (plan.slice_rows, LANES), 0) == 0
        corner = corner & (lax.broadcasted_iota(jnp.int32, (plan.slice_rows, LANES), 1) == 0)
        table = (second[0], second[1])
        count, groups = rows // PIECES, plan.groups // PIECES
        copies = []
        for piece in range(PIECES):
            start = piece * count
            both = jnp.concatenate([turned[start : start + count], turned[rows + start : rows + start + count]], axis=0)
            value = product(split(both), table)
            by_cos, by_sin = value[:, : plan.half], value[:, plan.half :]
            main = (by_cos[:count] + by_sin[count:], by_cos[count:] - by_sin[:count])
            for index in range(groups):
                group = piece * groups + index
                for part in range(2):
                    for column in range(plan.half_cols):
                        lanes = slice(column * LANES, (column + 1) * LANES)
                        tile = main[part][index * plan.slice_rows : (index + 1) * plan.slice_rows, lanes]
                        if (group, part, column) == (0, 1, 0):
                            tile = tile + jnp.where(corner, middle, 0.0)
                        packed[group, packed_rows(plan, part, column)] = tile
            where = pl.ds(piece * groups, groups)
            copies.append(pltpu.make_async_copy(packed.at[where], out.at[where], sems.at[piece]))
            copies[-1].start()
        for copy in copies:
            copy.wait()

    shape = jax.ShapeDtypeStruct((plan.groups, plan.packed, LANES), jnp.float32)
    scratch = [
        pltpu.VMEM((plan.n1s, plan.side), jnp.float32),
        pltpu.VMEM((2 * plan.rows, plan.side), jnp.float32),
        pltpu.VMEM((plan.groups, plan.packed, LANES), jnp.float32),
        pltpu.SemaphoreType.DMA((PIECES,)),
    ]
    return call(kernel, shape, ["vmem"] * (plan.quarters + 3), scratch, "hbm")


def combine(plan):
    def kernel(spectra, own, out):
        place, _, first_row = spot(plan)
        row = lax.broadcasted_iota(jnp.int32, (plan.slice_rows, LANES), 0) + first_row + place * plan.freq_rows
        sign = jnp.where(row % 2 == 0, 1.0, -1.0)

        def one_block(block, carry):
            sums = [jnp.zeros((plan.slice_rows, LANES), jnp.float32) for _ in range(2 * plan.half_cols)]
            for step in range(plan.rounds):
                here = lax.rem(block + (plan.rounds * STRIDE * plan.groups - step * STRIDE), plan.groups)
                before = lax.rem(here + (plan.groups - 1), plan.groups)
                for column in range(plan.half_cols):
                    real, imag = (
                        spectra[here, packed_rows(plan, part, column)]
                        + sign * spectra[before, packed_rows(plan, part, column)]
                        for part in range(2)
                    )
                    own_r, own_i, own_c = (own[3 * step + part, column] for part in range(3))
                    sums[column] = sums[column] + own_r * real - own_i * imag
                    sums[plan.half_cols + column] = sums[plan.half_cols + column] + own_c * imag + own_i * real
            for part in range(2):
                for column in range(plan.half_cols):
                    out[block, packed_rows(plan, part, column)] = sums[part * plan.half_cols + column]
            return carry

        lax.fori_loop(0, plan.groups, one_block, 0)

    shape = jax.ShapeDtypeStruct((plan.groups, plan.packed, LANES), jnp.float32)
    return call(kernel, shape, ["vmem"] * 2)


def into_slots(plan, place, odd, last, turned, out, matrix):
    where = [pl.ds(pl.multiple_of((place ^ (2 * slot + odd)) * plan.chunk, 16), plan.chunk) for slot in range(plan.quarters // 2)]
    rows = [jnp.concatenate([last[part, at, :] for at in where], axis=0) for part in range(2)]
    matrix[...] = product(rows, turned)
    for slot in range(plan.quarters // 2):
        for column in range(plan.cols):
            out[slot, pl.ds(column, plan.chunk, stride=plan.cols), :] = matrix[
                slot * plan.chunk : (slot + 1) * plan.chunk, column * LANES : (column + 1) * LANES
            ]


def backward(plan):
    def kernel(spectra, last, twist, second, out, turned, stack, spread, matrix):
        place = spot(plan)[0]
        rows = plan.rows
        for part in range(2):
            for column in range(plan.half_cols):
                lanes = slice(column * LANES, (column + 1) * LANES)
                for group in range(plan.groups):
                    start = part * rows + group * plan.slice_rows
                    stack[start : start + plan.slice_rows, lanes] = spectra[group, packed_rows(plan, part, column)]
        value = split(stack[...])
        by_cos = product(value, (second[0, :, : plan.half], second[1, :, : plan.half]), True)
        by_sin = product(value, (second[0, :, plan.half :], second[1, :, plan.half :]), True)
        spread[:rows] = by_cos[:rows] - by_sin[rows:]
        spread[rows:] = by_cos[rows:] + by_sin[:rows]
        middle = jnp.where(place == 0, stack[rows : rows + 1, :1], 0.0)
        spread[:1] = spread[:1] + middle * alternating(plan, 1)
        real, imag = spread[:rows], spread[rows:]
        high, low = split(
            jnp.concatenate([real * twist[0] + imag * twist[1], imag * twist[0] - real * twist[1]], axis=0)
        )
        turned[0], turned[1] = high, low
        into_slots(plan, place, 1, last, (high, low), out, matrix)

    shape = (
        jax.ShapeDtypeStruct((plan.quarters // 2, plan.chunk * plan.cols, LANES), jnp.float32),
        jax.ShapeDtypeStruct((2, 2 * plan.rows, plan.side), jnp.bfloat16),
    )
    scratch = [
        pltpu.VMEM((2 * plan.rows, plan.half), jnp.float32),
        pltpu.VMEM((2 * plan.rows, plan.side), jnp.float32),
        pltpu.VMEM((plan.n1s // 2, plan.side), jnp.float32),
    ]
    return call(kernel, shape, ["vmem"] * 4, scratch)


def finish(plan):
    def kernel(last, turned, out, matrix):
        into_slots(plan, spot(plan)[0], 0, last, (turned[0], turned[1]), out, matrix)

    shape = jax.ShapeDtypeStruct((plan.quarters // 2, plan.chunk * plan.cols, LANES), jnp.float32)
    scratch = [pltpu.VMEM((plan.n1s // 2, plan.side), jnp.float32)]
    return call(kernel, shape, ["vmem"] * 2, scratch)


def swapped(value, bit):
    count = lax.axis_size("acc")
    return lax.ppermute(value, "acc", [(source, source ^ bit) for source in range(count)])


def per_device(reciprocal_spectra, divisor):
    rounds, _, freq_rows, plane = reciprocal_spectra.shape
    quarters = lax.axis_size("acc")
    groups = lax.axis_size("blk") * lax.axis_size("tail")
    plan = Plan(freq_rows, plane, quarters, groups, rounds)
    constants = [jnp.asarray(table) for table in tables(plan)]

    limbs = divisor.reshape(plan.chunk * plan.cols, LANES)
    spectra = reciprocal_spectra.reshape(2 * rounds, freq_rows, plane)
    first, twist, second, near, facing, rim = prepare(plan)(*map(far, constants + [limbs, spectra]))
    bundled, rim = bundle(plan)(near, rim)
    pieces = {0: limbs}
    bit = quarters // 2
    while bit:
        for index, piece in list(pieces.items()):
            pieces[index | bit] = swapped(bundled if bit == 1 and index == 0 else piece, bit)
        bit //= 2
    pieces[0] = near
    facing = opposite(plan)(facing, pieces[1])
    facing = swapped(facing, quarters - 1)
    rides = quarters <= 4
    if not rides:
        rim = lax.ppermute(rim, "acc", [(source, -source % quarters) for source in range(quarters)])
    last, own, edge = resident(plan)(first, far(spectra), rim)

    own_spectrum = forward(plan)(*[pieces[index] for index in range(quarters)], first, twist, second)
    own = blend(plan, rides)(own, facing, edge, rim)
    if plan.per > 1:
        first_row = lax.axis_index(("blk", "tail")) % plan.per * plan.slice_rows
        own = lax.dynamic_slice_in_dim(own, first_row, plan.slice_rows, 2)
    every = lax.all_to_all(own_spectrum, ("blk", "tail"), 0, 0, tiled=True)
    sums = combine(plan)(every, own)
    back = lax.all_to_all(sums, ("blk", "tail"), 0, 0, tiled=True)
    odd, turned = backward(plan)(back, last, twist, second)
    arrived = swapped(odd, 1)
    even = finish(plan)(last, turned)
    held = {2 * slot: even[slot] + arrived[slot] for slot in range(quarters // 2)}
    bit = 2
    while bit < quarters:
        sent = sorted(index for index in held if index & bit)
        arrived = swapped(jnp.stack([held[index] for index in sent]), bit)
        held = {index ^ bit: held[index ^ bit] + arrived[where] for where, index in enumerate(sent)}
        bit *= 2
    return held[0].reshape(divisor.shape)


def solution(mesh):
    in_specs = (P(None, None, "acc", None), P(("blk", "tail"), "acc"))
    out_specs = P(("blk", "tail"), "acc")
    return jax.shard_map(per_device, mesh=mesh, in_specs=in_specs, out_specs=out_specs, check_vma=False)
```

```python
import math

import jax
import jax.numpy as jnp
import numpy as np
from jax import lax
from jax.experimental import pallas as pl
from jax.experimental.pallas import tpu as pltpu
from jax.sharding import PartitionSpec as P


LANES = 128
TILE = 8
PIECES = 2
GRANT = 16 * 1024 * 1024
STRIDE = 2


class Plan:
    def __init__(self, freq_rows, plane, quarters, groups, rounds):
        self.rounds = rounds
        self.quarters = quarters
        self.groups = groups
        self.freq_rows = freq_rows
        self.radix = freq_rows * quarters
        self.length = self.radix * plane
        self.side = math.isqrt(self.length)
        self.half = self.side // 2
        self.m_los = self.side // self.radix
        self.m_his = self.radix // self.m_los
        self.rows = self.m_los * freq_rows
        self.n1s = self.side // 2
        self.chunk = self.n1s // quarters
        self.cols = self.side // LANES
        self.half_cols = self.half // LANES
        self.slice_rows = self.rows // groups
        self.per = groups // self.m_los
        self.packed = 2 * self.half_cols * self.slice_rows


def tables(plan):
    row = (np.arange(plan.m_los)[:, None] * plan.radix + np.arange(plan.freq_rows)[None, :]).reshape(-1)
    part = np.arange(plan.quarters) * plan.freq_rows
    n1 = np.arange(plan.n1s)
    n2 = np.arange(plan.side)
    f2 = (np.arange(plan.m_his)[:, None] + plan.m_los * np.arange(plan.radix // 2)[None, :]).reshape(-1)

    def wave(first, second, modulus):
        angle = (first[:, None] * second[None, :] % modulus) * (-2.0 * math.pi / modulus)
        return np.stack([np.cos(angle), np.sin(angle)])

    first_rows = wave(row, n1, plan.side)
    first_part = wave(part, n1, plan.side)
    twist_rows = wave(row, n2, plan.length)
    twist_part = wave(part, n2, plan.length)
    cosine, sine = wave(n2, f2, plan.side)
    second = np.concatenate([cosine, -sine], axis=1)
    second_high = second.astype(jnp.bfloat16)
    second_low = (second - second_high.astype(np.float64)).astype(jnp.bfloat16)
    single = lambda value: value.astype(np.float32)
    return (
        single(first_rows),
        single(first_part.transpose(1, 0, 2)),
        single(twist_rows),
        single(twist_part.transpose(1, 0, 2)),
        np.stack([second_high, second_low]),
    )


def spot(plan):
    place = lax.axis_index("acc")
    group = lax.axis_index("blk") * lax.axis_size("tail") + lax.axis_index("tail")
    if plan.per == 1:
        return place, group, 0
    return place, lax.div(group, plan.per), lax.rem(group, plan.per) * plan.slice_rows


def rim_m_lo(plan, place, m_lo):
    return jnp.where(place == 0, lax.rem(plan.m_los - m_lo, plan.m_los), plan.m_los - 1 - m_lo)


def far(value):
    return pltpu.with_memory_space_constraint(value, pltpu.HBM)


def split(value):
    high = value.astype(jnp.bfloat16)
    low = (value - high.astype(jnp.float32)).astype(jnp.bfloat16)
    return high, low


def product(first, second, transposed=False):
    dims = (((1,), (1 if transposed else 0,)), ((), ()))
    dot = lambda a, b: lax.dot_general(a, b, dims, preferred_element_type=jnp.float32)
    return dot(first[0], second[0]) + (dot(first[1], second[0]) + dot(first[0], second[1]))


def call(kernel, out_shape, memory, scratch=(), result="vmem", flops=1_000_000, moved=1_000_000):
    where = {"vmem": pltpu.VMEM, "hbm": pltpu.HBM}
    out_spec = pl.BlockSpec(memory_space=where[result])
    return pl.pallas_call(
        kernel,
        out_shape=out_shape,
        in_specs=[pl.BlockSpec(memory_space=where[kind]) for kind in memory],
        out_specs=jax.tree.map(lambda _: out_spec, out_shape),
        scratch_shapes=scratch,
        cost_estimate=pl.CostEstimate(flops=flops, bytes_accessed=moved, transcendentals=0),
        compiler_params=pltpu.CompilerParams(vmem_limit_bytes=GRANT),
    )


def fetch(plan, spectra, held, sems, m_lo, rows):
    copies = []
    for m_hi in range(plan.m_his):
        start = pl.multiple_of((m_hi * plan.m_los + m_lo) * plan.radix // LANES * LANES, LANES)
        source = spectra.at[:, pl.ds(0, rows), pl.ds(start, LANES)]
        copies.append(pltpu.make_async_copy(source, held.at[m_hi], sems.at[m_hi]))
    return copies


def gathered(plan, held, index, column, within, count):
    piece_lanes = plan.radix // 2
    each = LANES // piece_lanes
    lane = lax.broadcasted_iota(jnp.int32, (count, LANES), 1)
    value = jnp.zeros((count, LANES), jnp.float32)
    for piece in range(each):
        tile = held[column * each + piece, index, :count]
        turned = pltpu.roll(tile, (piece * piece_lanes - within + LANES) % LANES, 1)
        value = jnp.where((lane >= piece * piece_lanes) & (lane < (piece + 1) * piece_lanes), turned, value)
    return value


def held_shape(plan, rows):
    return jax.ShapeDtypeStruct((plan.m_his, 2 * plan.rounds, rows, LANES), jnp.float32)


def bundle(plan):
    def kernel(near, held, out, rim):
        place, m_lo, _ = spot(plan)
        within = rim_m_lo(plan, place, m_lo) * plan.radix % LANES + plan.radix // 2
        base = plan.chunk * plan.cols
        out[:base] = near[...]
        for index in range(2 * plan.rounds):
            for column in range(plan.half_cols):
                row = index * plan.half_cols + column
                value = gathered(plan, held, index, column, within, 1)
                out[base + row : base + row + 1] = value
                rim[index : index + 1, column * LANES : (column + 1) * LANES] = value

    shape = jax.ShapeDtypeStruct
    rows = plan.chunk * plan.cols + 2 * plan.rounds * plan.half_cols
    out_shape = (shape((rows, LANES), jnp.float32), shape((2 * plan.rounds, plan.half), jnp.float32))
    return call(kernel, out_shape, ["vmem"] * 2)


def flipped(plan, value):
    row = lax.broadcasted_iota(jnp.int32, (plan.half, plan.half), 0)
    column = lax.broadcasted_iota(jnp.int32, (plan.half, plan.half), 1)
    flip = jnp.where(row + column == plan.half - 1, 1.0, 0.0).astype(jnp.bfloat16)
    high, low = value
    dot = lambda a: jnp.dot(a, flip, preferred_element_type=jnp.float32)
    return dot(high) + dot(low)


def opposite(plan):
    def kernel(held, other, out, stack):
        m_lo = plan.m_los - 1 - spot(plan)[1]
        within = m_lo * plan.radix % LANES + plan.radix // 2
        base = plan.chunk * plan.cols
        rows = plan.freq_rows
        for index in range(2 * plan.rounds):
            for column in range(plan.half_cols):
                lanes = slice(column * LANES, (column + 1) * LANES)
                stack[index * rows : (index + 1) * rows, lanes] = gathered(plan, held, index, column, within, rows)
                row = base + index * plan.half_cols + column
                stack[index * rows : index * rows + 1, lanes] = other[row : row + 1]
        count = 2 * plan.rounds * rows
        row = lax.broadcasted_iota(jnp.int32, (count, count), 0)
        column = lax.broadcasted_iota(jnp.int32, (count, count), 1)
        inside = row % rows
        target = jnp.where(inside == 0, row, 2 * (row - inside) + rows - row)
        turn = jnp.where(column == target, 1.0, 0.0).astype(jnp.bfloat16)
        dot = lambda a: jnp.dot(turn, a, preferred_element_type=jnp.float32).astype(jnp.bfloat16)
        high, low = split(stack[...])
        out[...] = flipped(plan, (dot(high), dot(low))).reshape(out.shape)

    shape = jax.ShapeDtypeStruct((2 * plan.rounds, plan.freq_rows, plan.half), jnp.float32)
    scratch = [pltpu.VMEM((2 * plan.rounds * plan.freq_rows, plan.half), jnp.float32)]
    return call(kernel, shape, ["vmem"] * 2, scratch)


def prepare(plan):
    def kernel(*refs):
        first, twist, second, near, facing, rim = refs[7:13]
        first_rows, first_part, twist_rows, twist_part = refs[13:17]
        sems, facing_sems, rim_sems = refs[17:]
        place, m_lo, _ = spot(plan)
        targets = (first_rows, first_part, twist_rows, twist_part, second, near)
        copies = [
            pltpu.make_async_copy(source, target, sems.at[index])
            for index, (source, target) in enumerate(zip(refs[:6], targets))
        ]
        copies += fetch(plan, refs[6], facing, facing_sems, plan.m_los - 1 - m_lo, plan.freq_rows)
        copies += fetch(plan, refs[6], rim, rim_sems, rim_m_lo(plan, place, m_lo), TILE)
        for copy in copies:
            copy.start()
        copies[0].wait()
        copies[1].wait()
        part_cos = first_part[pl.ds(place, 1), 0, :]
        part_sin = first_part[pl.ds(place, 1), 1, :]
        rows = plan.rows
        first[0, :rows], first[1, :rows] = split(first_rows[0] * part_cos - first_rows[1] * part_sin)
        first[0, rows:], first[1, rows:] = split(first_rows[0] * part_sin + first_rows[1] * part_cos)
        copies[2].wait()
        copies[3].wait()
        part_cos = twist_part[pl.ds(place, 1), 0, :]
        part_sin = twist_part[pl.ds(place, 1), 1, :]
        twist[0] = twist_rows[0] * part_cos - twist_rows[1] * part_sin
        twist[1] = twist_rows[0] * part_sin + twist_rows[1] * part_cos
        for copy in copies[4:]:
            copy.wait()

    shape = jax.ShapeDtypeStruct
    out_shape = (
        shape((2, 2 * plan.rows, plan.n1s), jnp.bfloat16),
        shape((2, plan.rows, plan.side), jnp.float32),
        shape((2, plan.side, 2 * plan.half), jnp.bfloat16),
        shape((plan.chunk * plan.cols, LANES), jnp.float32),
        held_shape(plan, plan.freq_rows),
        held_shape(plan, TILE),
    )
    scratch = [
        pltpu.VMEM((2, plan.rows, plan.n1s), jnp.float32),
        pltpu.VMEM((plan.quarters, 2, plan.n1s), jnp.float32),
        pltpu.VMEM((2, plan.rows, plan.side), jnp.float32),
        pltpu.VMEM((plan.quarters, 2, plan.side), jnp.float32),
        pltpu.SemaphoreType.DMA((6,)),
        pltpu.SemaphoreType.DMA((plan.m_his,)),
        pltpu.SemaphoreType.DMA((plan.m_his,)),
    ]
    return call(kernel, out_shape, ["hbm"] * 7, scratch)


def resident(plan):
    def kernel(first, spectra, rim, last, own, edge, held, sems):
        place, m_lo, _ = spot(plan)
        copies = fetch(plan, spectra, held, sems, m_lo, plan.freq_rows)
        for copy in copies:
            copy.start()
        last[0], last[1] = split((first[0].astype(jnp.float32) + first[1].astype(jnp.float32)).T)
        value = flipped(plan, split(rim[...]))
        lane = lax.broadcasted_iota(jnp.int32, value.shape, 1)
        later = pltpu.roll(value, plan.radix // 2, 1)
        later = jnp.where(lane < plan.radix // 2, pltpu.roll(later, 1, 1), later)
        edge[...] = jnp.where((place == 0) & (m_lo == 0), later, value)
        for copy in copies:
            copy.wait()
        within = m_lo * plan.radix % LANES
        for index in range(2 * plan.rounds):
            for column in range(plan.half_cols):
                own[index, column] = gathered(plan, held, index, column, within, plan.freq_rows)

    shape = jax.ShapeDtypeStruct
    out_shape = (
        shape((2, plan.n1s, 2 * plan.rows), jnp.bfloat16),
        shape((2 * plan.rounds, plan.half_cols, plan.freq_rows, LANES), jnp.float32),
        shape((2 * plan.rounds, plan.half), jnp.float32),
    )
    held = held_shape(plan, plan.freq_rows)
    scratch = [pltpu.VMEM(held.shape, held.dtype), pltpu.SemaphoreType.DMA((plan.m_his,))]
    return call(kernel, out_shape, ["vmem", "hbm", "vmem"], scratch)


def blend(plan, rides):
    def kernel(own, arrived, edge, rim, out):
        place, m_lo, _ = spot(plan)
        corner = lax.broadcasted_iota(jnp.int32, (plan.freq_rows, LANES), 0)
        top = corner == 0
        corner = top & (lax.broadcasted_iota(jnp.int32, (plan.freq_rows, LANES), 1) == 0)
        corner = corner & ((place == 0) & (m_lo == 0))
        if rides:
            top = top & (lax.rem(place, 2) == 0)
        scale = 1.0 / plan.length
        for step in range(plan.rounds):
            for column in range(plan.half_cols):
                lanes = slice(column * LANES, (column + 1) * LANES)
                whole = []
                for part in range(2):
                    index = 2 * step + part
                    there = jnp.where(top, edge[index : index + 1, lanes], arrived[index, :, lanes])
                    here = own[index, column]
                    if column == 0:
                        there = jnp.where(corner, here if part else 0.0, there)
                    whole.append((here - there if part else here + there) * scale)
                out[3 * step, column] = whole[0]
                out[3 * step + 1, column] = whole[1]
                if column == 0:
                    whole[0] = jnp.where(corner, rim[2 * step : 2 * step + 1, lanes] * scale, whole[0])
                out[3 * step + 2, column] = whole[0]

    shape = jax.ShapeDtypeStruct((3 * plan.rounds, plan.half_cols, plan.freq_rows, LANES), jnp.float32)
    return call(kernel, shape, ["vmem"] * 4)


def alternating(plan, count):
    lane = lax.broadcasted_iota(jnp.int32, (count, plan.side), 1)
    return jnp.where(lane % 2 == 0, 1.0, -1.0)


def packed_rows(plan, part, column):
    start = (part * plan.half_cols + column) * plan.slice_rows
    return slice(start, start + plan.slice_rows)


def forward(plan):
    def kernel(*refs):
        limbs = refs[: plan.quarters]
        first, twist, second, out, matrix, turned, packed, sems = refs[plan.quarters :]
        place = spot(plan)[0]
        for index in range(plan.quarters):
            start = pl.multiple_of((place ^ index) * plan.chunk, 8)
            for column in range(plan.cols):
                matrix[pl.ds(start, plan.chunk), column * LANES : (column + 1) * LANES] = limbs[index][
                    pl.ds(column, plan.chunk, stride=plan.cols), :
                ]
        value = product((first[0], first[1]), split(matrix[...]))
        rows = plan.rows
        real, imag = value[:rows], value[rows:]
        turned[:rows] = real * twist[0] - imag * twist[1]
        turned[rows:] = real * twist[1] + imag * twist[0]
        middle = jnp.sum(turned[:1] * alternating(plan, 1), axis=1, keepdims=True)
        middle = jnp.where(place == 0, middle, 0.0)
        corner = lax.broadcasted_iota(jnp.int32, (plan.slice_rows, LANES), 0) == 0
        corner = corner & (lax.broadcasted_iota(jnp.int32, (plan.slice_rows, LANES), 1) == 0)
        table = (second[0], second[1])
        count, groups = rows // PIECES, plan.groups // PIECES
        copies = []
        for piece in range(PIECES):
            start = piece * count
            both = jnp.concatenate([turned[start : start + count], turned[rows + start : rows + start + count]], axis=0)
            value = product(split(both), table)
            by_cos, by_sin = value[:, : plan.half], value[:, plan.half :]
            main = (by_cos[:count] + by_sin[count:], by_cos[count:] - by_sin[:count])
            for index in range(groups):
                group = piece * groups + index
                for part in range(2):
                    for column in range(plan.half_cols):
                        lanes = slice(column * LANES, (column + 1) * LANES)
                        tile = main[part][index * plan.slice_rows : (index + 1) * plan.slice_rows, lanes]
                        if (group, part, column) == (0, 1, 0):
                            tile = tile + jnp.where(corner, middle, 0.0)
                        packed[group, packed_rows(plan, part, column)] = tile
            where = pl.ds(piece * groups, groups)
            copies.append(pltpu.make_async_copy(packed.at[where], out.at[where], sems.at[piece]))
            copies[-1].start()
        for copy in copies:
            copy.wait()

    shape = jax.ShapeDtypeStruct((plan.groups, plan.packed, LANES), jnp.float32)
    scratch = [
        pltpu.VMEM((plan.n1s, plan.side), jnp.float32),
        pltpu.VMEM((2 * plan.rows, plan.side), jnp.float32),
        pltpu.VMEM((plan.groups, plan.packed, LANES), jnp.float32),
        pltpu.SemaphoreType.DMA((PIECES,)),
    ]
    return call(kernel, shape, ["vmem"] * (plan.quarters + 3), scratch, "hbm")


def combine(plan):
    def kernel(spectra, own, out):
        place, _, first_row = spot(plan)
        row = lax.broadcasted_iota(jnp.int32, (plan.slice_rows, LANES), 0) + first_row + place * plan.freq_rows
        sign = jnp.where(row % 2 == 0, 1.0, -1.0)

        def one_block(block, carry):
            sums = [jnp.zeros((plan.slice_rows, LANES), jnp.float32) for _ in range(2 * plan.half_cols)]
            for step in range(plan.rounds):
                here = lax.rem(block + (plan.rounds * STRIDE * plan.groups - step * STRIDE), plan.groups)
                before = lax.rem(here + (plan.groups - 1), plan.groups)
                for column in range(plan.half_cols):
                    real, imag = (
                        spectra[here, packed_rows(plan, part, column)]
                        + sign * spectra[before, packed_rows(plan, part, column)]
                        for part in range(2)
                    )
                    own_r, own_i, own_c = (own[3 * step + part, column] for part in range(3))
                    sums[column] = sums[column] + own_r * real - own_i * imag
                    sums[plan.half_cols + column] = sums[plan.half_cols + column] + own_c * imag + own_i * real
            for part in range(2):
                for column in range(plan.half_cols):
                    out[block, packed_rows(plan, part, column)] = sums[part * plan.half_cols + column]
            return carry

        lax.fori_loop(0, plan.groups, one_block, 0)

    shape = jax.ShapeDtypeStruct((plan.groups, plan.packed, LANES), jnp.float32)
    return call(kernel, shape, ["vmem"] * 2)


def into_slots(plan, slots, last, turned, out, matrix):
    place = spot(plan)[0]
    where = [pl.ds(pl.multiple_of((place ^ slot) * plan.chunk, 16), plan.chunk) for slot in slots]
    rows = [jnp.concatenate([last[part, at, :] for at in where], axis=0) for part in range(2)]
    matrix[...] = product(rows, turned)
    for index in range(len(slots)):
        for column in range(plan.cols):
            out[index, pl.ds(column, plan.chunk, stride=plan.cols), :] = matrix[
                index * plan.chunk : (index + 1) * plan.chunk, column * LANES : (column + 1) * LANES
            ]


def backward(plan, slots):
    def kernel(spectra, last, twist, second, out, turned, stack, spread, matrix):
        place = spot(plan)[0]
        rows = plan.rows
        for part in range(2):
            for column in range(plan.half_cols):
                lanes = slice(column * LANES, (column + 1) * LANES)
                for group in range(plan.groups):
                    start = part * rows + group * plan.slice_rows
                    stack[start : start + plan.slice_rows, lanes] = spectra[group, packed_rows(plan, part, column)]
        value = split(stack[...])
        by_cos = product(value, (second[0, :, : plan.half], second[1, :, : plan.half]), True)
        by_sin = product(value, (second[0, :, plan.half :], second[1, :, plan.half :]), True)
        spread[:rows] = by_cos[:rows] - by_sin[rows:]
        spread[rows:] = by_cos[rows:] + by_sin[:rows]
        middle = jnp.where(place == 0, stack[rows : rows + 1, :1], 0.0)
        spread[:1] = spread[:1] + middle * alternating(plan, 1)
        real, imag = spread[:rows], spread[rows:]
        high, low = split(
            jnp.concatenate([real * twist[0] + imag * twist[1], imag * twist[0] - real * twist[1]], axis=0)
        )
        turned[0], turned[1] = high, low
        into_slots(plan, slots, last, (high, low), out, matrix)

    shape = (
        jax.ShapeDtypeStruct((len(slots), plan.chunk * plan.cols, LANES), jnp.float32),
        jax.ShapeDtypeStruct((2, 2 * plan.rows, plan.side), jnp.bfloat16),
    )
    scratch = [
        pltpu.VMEM((2 * plan.rows, plan.half), jnp.float32),
        pltpu.VMEM((2 * plan.rows, plan.side), jnp.float32),
        pltpu.VMEM((len(slots) * plan.chunk, plan.side), jnp.float32),
    ]
    return call(kernel, shape, ["vmem"] * 4, scratch)


def finish(plan, slots):
    def kernel(last, turned, out, matrix):
        into_slots(plan, slots, last, (turned[0], turned[1]), out, matrix)

    shape = jax.ShapeDtypeStruct((len(slots), plan.chunk * plan.cols, LANES), jnp.float32)
    scratch = [pltpu.VMEM((len(slots) * plan.chunk, plan.side), jnp.float32)]
    return call(kernel, shape, ["vmem"] * 2, scratch)


def swapped(value, bit):
    count = lax.axis_size("acc")
    return lax.ppermute(value, "acc", [(source, source ^ bit) for source in range(count)])


def per_device(reciprocal_spectra, divisor):
    rounds, _, freq_rows, plane = reciprocal_spectra.shape
    quarters = lax.axis_size("acc")
    groups = lax.axis_size("blk") * lax.axis_size("tail")
    plan = Plan(freq_rows, plane, quarters, groups, rounds)
    constants = [jnp.asarray(table) for table in tables(plan)]

    limbs = divisor.reshape(plan.chunk * plan.cols, LANES)
    spectra = reciprocal_spectra.reshape(2 * rounds, freq_rows, plane)
    first, twist, second, near, facing, rim = prepare(plan)(*map(far, constants + [limbs, spectra]))
    bundled, rim = bundle(plan)(near, rim)
    pieces = {0: limbs}
    bit = quarters // 2
    while bit:
        for index, piece in list(pieces.items()):
            pieces[index | bit] = swapped(bundled if bit == 1 and index == 0 else piece, bit)
        bit //= 2
    pieces[0] = near
    facing = opposite(plan)(facing, pieces[1])
    facing = swapped(facing, quarters - 1)
    rides = quarters <= 4
    if not rides:
        rim = lax.ppermute(rim, "acc", [(source, -source % quarters) for source in range(quarters)])
    last, own, edge = resident(plan)(first, far(spectra), rim)

    own_spectrum = forward(plan)(*[pieces[index] for index in range(quarters)], first, twist, second)
    own = blend(plan, rides)(own, facing, edge, rim)
    if plan.per > 1:
        first_row = lax.axis_index(("blk", "tail")) % plan.per * plan.slice_rows
        own = lax.dynamic_slice_in_dim(own, first_row, plan.slice_rows, 2)
    every = lax.all_to_all(own_spectrum, ("blk", "tail"), 0, 0, tiled=True)
    sums = combine(plan)(every, own)
    back = lax.all_to_all(sums, ("blk", "tail"), 0, 0, tiled=True)
    first_sent = [index for index in range(quarters) if index & 1 and (index & 2 or quarters == 2)]
    others = [index for index in range(quarters) if index not in first_sent]
    sent, turned = backward(plan, first_sent)(back, last, twist, second)
    arrived = swapped(sent, 1)
    rest = finish(plan, others)(last, turned)
    slot = {index: rest[where] for where, index in enumerate(others)}
    held = {index ^ 1: slot[index ^ 1] + arrived[where] for where, index in enumerate(first_sent)}
    later = [index for index in others if index & 1]
    if later:
        arrived = swapped(jnp.stack([slot[index] for index in later]), 1)
        held.update({index ^ 1: slot[index ^ 1] + arrived[where] for where, index in enumerate(later)})
    bit = 2
    while bit < quarters:
        sent = sorted(index for index in held if index & bit)
        arrived = swapped(jnp.stack([held[index] for index in sent]), bit)
        held = {index ^ bit: held[index ^ bit] + arrived[where] for where, index in enumerate(sent)}
        bit *= 2
    return held[0].reshape(divisor.shape)


def solution(mesh):
    in_specs = (P(None, None, "acc", None), P(("blk", "tail"), "acc"))
    out_specs = P(("blk", "tail"), "acc")
    return jax.shard_map(per_device, mesh=mesh, in_specs=in_specs, out_specs=out_specs, check_vma=False)
```

```python
import math

import jax
import jax.numpy as jnp
import numpy as np
from jax import lax
from jax.experimental import pallas as pl
from jax.experimental.pallas import tpu as pltpu
from jax.sharding import PartitionSpec as P


LANES = 128
TILE = 8
PIECES = 2
GRANT = 16 * 1024 * 1024
STRIDE = 2


class Plan:
    def __init__(self, freq_rows, plane, quarters, groups, rounds):
        self.rounds = rounds
        self.quarters = quarters
        self.groups = groups
        self.freq_rows = freq_rows
        self.radix = freq_rows * quarters
        self.length = self.radix * plane
        self.side = math.isqrt(self.length)
        self.half = self.side // 2
        self.m_los = self.side // self.radix
        self.m_his = self.radix // self.m_los
        self.rows = self.m_los * freq_rows
        self.n1s = self.side // 2
        self.chunk = self.n1s // quarters
        self.cols = self.side // LANES
        self.half_cols = self.half // LANES
        self.slice_rows = self.rows // groups
        self.per = groups // self.m_los
        self.packed = 2 * self.half_cols * self.slice_rows


def tables(plan):
    row = (np.arange(plan.m_los)[:, None] * plan.radix + np.arange(plan.freq_rows)[None, :]).reshape(-1)
    part = np.arange(plan.quarters) * plan.freq_rows
    n1 = np.arange(plan.n1s)
    n2 = np.arange(plan.side)
    f2 = (np.arange(plan.m_his)[:, None] + plan.m_los * np.arange(plan.radix // 2)[None, :]).reshape(-1)

    def wave(first, second, modulus):
        angle = (first[:, None] * second[None, :] % modulus) * (-2.0 * math.pi / modulus)
        return np.stack([np.cos(angle), np.sin(angle)])

    first_rows = wave(row, n1, plan.side)
    first_part = wave(part, n1, plan.side)
    twist_rows = wave(row, n2, plan.length)
    twist_part = wave(part, n2, plan.length)
    cosine, sine = wave(n2, f2, plan.side)
    second = np.concatenate([cosine, -sine], axis=1)
    second_high = second.astype(jnp.bfloat16)
    second_low = (second - second_high.astype(np.float64)).astype(jnp.bfloat16)
    single = lambda value: value.astype(np.float32)
    return (
        single(first_rows),
        single(first_part.transpose(1, 0, 2)),
        single(twist_rows),
        single(twist_part.transpose(1, 0, 2)),
        np.stack([second_high, second_low]),
    )


def spot(plan):
    place = lax.axis_index("acc")
    group = lax.axis_index("blk") * lax.axis_size("tail") + lax.axis_index("tail")
    if plan.per == 1:
        return place, group, 0
    return place, lax.div(group, plan.per), lax.rem(group, plan.per) * plan.slice_rows


def rim_m_lo(plan, place, m_lo):
    return jnp.where(place == 0, lax.rem(plan.m_los - m_lo, plan.m_los), plan.m_los - 1 - m_lo)


def far(value):
    return pltpu.with_memory_space_constraint(value, pltpu.HBM)


def split(value):
    high = value.astype(jnp.bfloat16)
    low = (value - high.astype(jnp.float32)).astype(jnp.bfloat16)
    return high, low


def product(first, second, transposed=False):
    dims = (((1,), (1 if transposed else 0,)), ((), ()))
    dot = lambda a, b: lax.dot_general(a, b, dims, preferred_element_type=jnp.float32)
    return dot(first[0], second[0]) + (dot(first[1], second[0]) + dot(first[0], second[1]))


def call(kernel, out_shape, memory, scratch=(), result="vmem", flops=1_000_000, moved=1_000_000):
    where = {"vmem": pltpu.VMEM, "hbm": pltpu.HBM}
    out_spec = pl.BlockSpec(memory_space=where[result])
    return pl.pallas_call(
        kernel,
        out_shape=out_shape,
        in_specs=[pl.BlockSpec(memory_space=where[kind]) for kind in memory],
        out_specs=jax.tree.map(lambda _: out_spec, out_shape),
        scratch_shapes=scratch,
        cost_estimate=pl.CostEstimate(flops=flops, bytes_accessed=moved, transcendentals=0),
        compiler_params=pltpu.CompilerParams(vmem_limit_bytes=GRANT),
    )


def fetch(plan, spectra, held, sems, m_lo, rows):
    copies = []
    for m_hi in range(plan.m_his):
        start = pl.multiple_of((m_hi * plan.m_los + m_lo) * plan.radix // LANES * LANES, LANES)
        source = spectra.at[:, pl.ds(0, rows), pl.ds(start, LANES)]
        copies.append(pltpu.make_async_copy(source, held.at[m_hi], sems.at[m_hi]))
    return copies


def gathered(plan, held, index, column, within, count):
    piece_lanes = plan.radix // 2
    each = LANES // piece_lanes
    lane = lax.broadcasted_iota(jnp.int32, (count, LANES), 1)
    value = jnp.zeros((count, LANES), jnp.float32)
    for piece in range(each):
        tile = held[column * each + piece, index, :count]
        turned = pltpu.roll(tile, (piece * piece_lanes - within + LANES) % LANES, 1)
        value = jnp.where((lane >= piece * piece_lanes) & (lane < (piece + 1) * piece_lanes), turned, value)
    return value


def held_shape(plan, rows):
    return jax.ShapeDtypeStruct((plan.m_his, 2 * plan.rounds, rows, LANES), jnp.float32)


def bundle(plan):
    def kernel(near, held, out, rim):
        place, m_lo, _ = spot(plan)
        within = rim_m_lo(plan, place, m_lo) * plan.radix % LANES + plan.radix // 2
        base = plan.chunk * plan.cols
        out[:base] = near[...]
        for index in range(2 * plan.rounds):
            for column in range(plan.half_cols):
                row = index * plan.half_cols + column
                value = gathered(plan, held, index, column, within, 1)
                out[base + row : base + row + 1] = value
                rim[index : index + 1, column * LANES : (column + 1) * LANES] = value

    shape = jax.ShapeDtypeStruct
    rows = plan.chunk * plan.cols + 2 * plan.rounds * plan.half_cols
    out_shape = (shape((rows, LANES), jnp.float32), shape((2 * plan.rounds, plan.half), jnp.float32))
    return call(kernel, out_shape, ["vmem"] * 2)


def flipped(plan, value):
    row = lax.broadcasted_iota(jnp.int32, (plan.half, plan.half), 0)
    column = lax.broadcasted_iota(jnp.int32, (plan.half, plan.half), 1)
    flip = jnp.where(row + column == plan.half - 1, 1.0, 0.0).astype(jnp.bfloat16)
    high, low = value
    dot = lambda a: jnp.dot(a, flip, preferred_element_type=jnp.float32)
    return dot(high) + dot(low)


def opposite(plan):
    def kernel(held, other, out, stack):
        m_lo = plan.m_los - 1 - spot(plan)[1]
        within = m_lo * plan.radix % LANES + plan.radix // 2
        base = plan.chunk * plan.cols
        rows = plan.freq_rows
        for index in range(2 * plan.rounds):
            for column in range(plan.half_cols):
                lanes = slice(column * LANES, (column + 1) * LANES)
                stack[index * rows : (index + 1) * rows, lanes] = gathered(plan, held, index, column, within, rows)
                row = base + index * plan.half_cols + column
                stack[index * rows : index * rows + 1, lanes] = other[row : row + 1]
        count = 2 * plan.rounds * rows
        row = lax.broadcasted_iota(jnp.int32, (count, count), 0)
        column = lax.broadcasted_iota(jnp.int32, (count, count), 1)
        inside = row % rows
        target = jnp.where(inside == 0, row, 2 * (row - inside) + rows - row)
        turn = jnp.where(column == target, 1.0, 0.0).astype(jnp.bfloat16)
        dot = lambda a: jnp.dot(turn, a, preferred_element_type=jnp.float32).astype(jnp.bfloat16)
        high, low = split(stack[...])
        out[...] = flipped(plan, (dot(high), dot(low))).reshape(out.shape)

    shape = jax.ShapeDtypeStruct((2 * plan.rounds, plan.freq_rows, plan.half), jnp.float32)
    scratch = [pltpu.VMEM((2 * plan.rounds * plan.freq_rows, plan.half), jnp.float32)]
    return call(kernel, shape, ["vmem"] * 2, scratch)


def prepare(plan):
    def kernel(*refs):
        first, twist, second, near, facing, rim, tail = refs[7:14]
        first_rows, first_part, twist_rows, twist_part = refs[14:18]
        sems, facing_sems, rim_sems = refs[18:]
        place, m_lo, _ = spot(plan)
        targets = (first_rows, first_part, twist_rows, twist_part, second, near)
        copies = [
            pltpu.make_async_copy(source, target, sems.at[index])
            for index, (source, target) in enumerate(zip(refs[:6], targets))
        ]
        copies += fetch(plan, refs[6], facing, facing_sems, plan.m_los - 1 - m_lo, plan.freq_rows)
        copies += fetch(plan, refs[6], rim, rim_sems, rim_m_lo(plan, place, m_lo), TILE)
        for copy in copies:
            copy.start()
        copies[0].wait()
        copies[1].wait()
        part_cos = first_part[pl.ds(place, 1), 0, :]
        part_sin = first_part[pl.ds(place, 1), 1, :]
        rows = plan.rows
        start = (place ^ (plan.quarters - 1)) * plan.chunk
        real = first_rows[0] * part_cos - first_rows[1] * part_sin
        imag = first_rows[0] * part_sin + first_rows[1] * part_cos
        for part, value in enumerate((real, imag)):
            some = slice(part * rows, (part + 1) * rows)
            first[0, some], first[1, some] = split(value)
            tail[0, some], tail[1, some] = split(pltpu.roll(value, plan.n1s - start, 1)[:, : plan.chunk])
        copies[2].wait()
        copies[3].wait()
        part_cos = twist_part[pl.ds(place, 1), 0, :]
        part_sin = twist_part[pl.ds(place, 1), 1, :]
        twist[0] = twist_rows[0] * part_cos - twist_rows[1] * part_sin
        twist[1] = twist_rows[0] * part_sin + twist_rows[1] * part_cos
        for copy in copies[4:]:
            copy.wait()

    shape = jax.ShapeDtypeStruct
    out_shape = (
        shape((2, 2 * plan.rows, plan.n1s), jnp.bfloat16),
        shape((2, plan.rows, plan.side), jnp.float32),
        shape((2, plan.side, 2 * plan.half), jnp.bfloat16),
        shape((plan.chunk * plan.cols, LANES), jnp.float32),
        held_shape(plan, plan.freq_rows),
        held_shape(plan, TILE),
        shape((2, 2 * plan.rows, plan.chunk), jnp.bfloat16),
    )
    scratch = [
        pltpu.VMEM((2, plan.rows, plan.n1s), jnp.float32),
        pltpu.VMEM((plan.quarters, 2, plan.n1s), jnp.float32),
        pltpu.VMEM((2, plan.rows, plan.side), jnp.float32),
        pltpu.VMEM((plan.quarters, 2, plan.side), jnp.float32),
        pltpu.SemaphoreType.DMA((6,)),
        pltpu.SemaphoreType.DMA((plan.m_his,)),
        pltpu.SemaphoreType.DMA((plan.m_his,)),
    ]
    return call(kernel, out_shape, ["hbm"] * 7, scratch)


def resident(plan):
    def kernel(first, spectra, rim, last, own, edge, held, sems):
        place, m_lo, _ = spot(plan)
        copies = fetch(plan, spectra, held, sems, m_lo, plan.freq_rows)
        for copy in copies:
            copy.start()
        last[0], last[1] = split((first[0].astype(jnp.float32) + first[1].astype(jnp.float32)).T)
        value = flipped(plan, split(rim[...]))
        lane = lax.broadcasted_iota(jnp.int32, value.shape, 1)
        later = pltpu.roll(value, plan.radix // 2, 1)
        later = jnp.where(lane < plan.radix // 2, pltpu.roll(later, 1, 1), later)
        edge[...] = jnp.where((place == 0) & (m_lo == 0), later, value)
        for copy in copies:
            copy.wait()
        within = m_lo * plan.radix % LANES
        for index in range(2 * plan.rounds):
            for column in range(plan.half_cols):
                own[index, column] = gathered(plan, held, index, column, within, plan.freq_rows)

    shape = jax.ShapeDtypeStruct
    out_shape = (
        shape((2, plan.n1s, 2 * plan.rows), jnp.bfloat16),
        shape((2 * plan.rounds, plan.half_cols, plan.freq_rows, LANES), jnp.float32),
        shape((2 * plan.rounds, plan.half), jnp.float32),
    )
    held = held_shape(plan, plan.freq_rows)
    scratch = [pltpu.VMEM(held.shape, held.dtype), pltpu.SemaphoreType.DMA((plan.m_his,))]
    return call(kernel, out_shape, ["vmem", "hbm", "vmem"], scratch)


def blend(plan, rides):
    def kernel(own, arrived, edge, rim, out):
        place, m_lo, _ = spot(plan)
        corner = lax.broadcasted_iota(jnp.int32, (plan.freq_rows, LANES), 0)
        top = corner == 0
        corner = top & (lax.broadcasted_iota(jnp.int32, (plan.freq_rows, LANES), 1) == 0)
        corner = corner & ((place == 0) & (m_lo == 0))
        if rides:
            top = top & (lax.rem(place, 2) == 0)
        scale = 1.0 / plan.length
        for step in range(plan.rounds):
            for column in range(plan.half_cols):
                lanes = slice(column * LANES, (column + 1) * LANES)
                whole = []
                for part in range(2):
                    index = 2 * step + part
                    there = jnp.where(top, edge[index : index + 1, lanes], arrived[index, :, lanes])
                    here = own[index, column]
                    if column == 0:
                        there = jnp.where(corner, here if part else 0.0, there)
                    whole.append((here - there if part else here + there) * scale)
                out[3 * step, column] = whole[0]
                out[3 * step + 1, column] = whole[1]
                if column == 0:
                    whole[0] = jnp.where(corner, rim[2 * step : 2 * step + 1, lanes] * scale, whole[0])
                out[3 * step + 2, column] = whole[0]

    shape = jax.ShapeDtypeStruct((3 * plan.rounds, plan.half_cols, plan.freq_rows, LANES), jnp.float32)
    return call(kernel, shape, ["vmem"] * 4)


def alternating(plan, count):
    lane = lax.broadcasted_iota(jnp.int32, (count, plan.side), 1)
    return jnp.where(lane % 2 == 0, 1.0, -1.0)


def packed_rows(plan, part, column):
    start = (part * plan.half_cols + column) * plan.slice_rows
    return slice(start, start + plan.slice_rows)


def begin(plan):
    def kernel(*refs):
        limbs = refs[: plan.quarters - 1]
        first, out, matrix = refs[plan.quarters - 1 :]
        place = spot(plan)[0]
        for index in range(plan.quarters):
            start = pl.multiple_of((place ^ index) * plan.chunk, 8)
            for column in range(plan.cols):
                lanes = slice(column * LANES, (column + 1) * LANES)
                if index < plan.quarters - 1:
                    value = limbs[index][pl.ds(column, plan.chunk, stride=plan.cols), :]
                else:
                    value = jnp.zeros((plan.chunk, LANES), jnp.float32)
                matrix[pl.ds(start, plan.chunk), lanes] = value
        out[...] = product((first[0], first[1]), split(matrix[...]))

    shape = jax.ShapeDtypeStruct((2 * plan.rows, plan.side), jnp.float32)
    scratch = [pltpu.VMEM((plan.n1s, plan.side), jnp.float32)]
    return call(kernel, shape, ["vmem"] * plan.quarters, scratch)


def forward(plan):
    def kernel(limbs, begun, tail, twist, second, out, matrix, turned, packed, sems):
        place = spot(plan)[0]
        for column in range(plan.cols):
            rows = pl.ds(column, plan.chunk, stride=plan.cols)
            matrix[:, column * LANES : (column + 1) * LANES] = limbs[rows, :]
        value = begun[...] + product((tail[0], tail[1]), split(matrix[...]))
        rows = plan.rows
        real, imag = value[:rows], value[rows:]
        turned[:rows] = real * twist[0] - imag * twist[1]
        turned[rows:] = real * twist[1] + imag * twist[0]
        middle = jnp.sum(turned[:1] * alternating(plan, 1), axis=1, keepdims=True)
        middle = jnp.where(place == 0, middle, 0.0)
        corner = lax.broadcasted_iota(jnp.int32, (plan.slice_rows, LANES), 0) == 0
        corner = corner & (lax.broadcasted_iota(jnp.int32, (plan.slice_rows, LANES), 1) == 0)
        table = (second[0], second[1])
        count, groups = rows // PIECES, plan.groups // PIECES
        copies = []
        for piece in range(PIECES):
            start = piece * count
            both = jnp.concatenate([turned[start : start + count], turned[rows + start : rows + start + count]], axis=0)
            value = product(split(both), table)
            by_cos, by_sin = value[:, : plan.half], value[:, plan.half :]
            main = (by_cos[:count] + by_sin[count:], by_cos[count:] - by_sin[:count])
            for index in range(groups):
                group = piece * groups + index
                for part in range(2):
                    for column in range(plan.half_cols):
                        lanes = slice(column * LANES, (column + 1) * LANES)
                        tile = main[part][index * plan.slice_rows : (index + 1) * plan.slice_rows, lanes]
                        if (group, part, column) == (0, 1, 0):
                            tile = tile + jnp.where(corner, middle, 0.0)
                        packed[group, packed_rows(plan, part, column)] = tile
            where = pl.ds(piece * groups, groups)
            copies.append(pltpu.make_async_copy(packed.at[where], out.at[where], sems.at[piece]))
            copies[-1].start()
        for copy in copies:
            copy.wait()

    shape = jax.ShapeDtypeStruct((plan.groups, plan.packed, LANES), jnp.float32)
    scratch = [
        pltpu.VMEM((plan.chunk, plan.side), jnp.float32),
        pltpu.VMEM((2 * plan.rows, plan.side), jnp.float32),
        pltpu.VMEM((plan.groups, plan.packed, LANES), jnp.float32),
        pltpu.SemaphoreType.DMA((PIECES,)),
    ]
    return call(kernel, shape, ["vmem"] * 5, scratch, "hbm")


def combine(plan):
    def kernel(spectra, own, out):
        place, _, first_row = spot(plan)
        row = lax.broadcasted_iota(jnp.int32, (plan.slice_rows, LANES), 0) + first_row + place * plan.freq_rows
        sign = jnp.where(row % 2 == 0, 1.0, -1.0)

        def one_block(block, carry):
            sums = [jnp.zeros((plan.slice_rows, LANES), jnp.float32) for _ in range(2 * plan.half_cols)]
            for step in range(plan.rounds):
                here = lax.rem(block + (plan.rounds * STRIDE * plan.groups - step * STRIDE), plan.groups)
                before = lax.rem(here + (plan.groups - 1), plan.groups)
                for column in range(plan.half_cols):
                    real, imag = (
                        spectra[here, packed_rows(plan, part, column)]
                        + sign * spectra[before, packed_rows(plan, part, column)]
                        for part in range(2)
                    )
                    own_r, own_i, own_c = (own[3 * step + part, column] for part in range(3))
                    sums[column] = sums[column] + own_r * real - own_i * imag
                    sums[plan.half_cols + column] = sums[plan.half_cols + column] + own_c * imag + own_i * real
            for part in range(2):
                for column in range(plan.half_cols):
                    out[block, packed_rows(plan, part, column)] = sums[part * plan.half_cols + column]
            return carry

        lax.fori_loop(0, plan.groups, one_block, 0, unroll=4)

    shape = jax.ShapeDtypeStruct((plan.groups, plan.packed, LANES), jnp.float32)
    return call(kernel, shape, ["vmem"] * 2)


def into_slots(plan, slots, last, turned, out, matrix):
    place = spot(plan)[0]
    where = [pl.ds(pl.multiple_of((place ^ slot) * plan.chunk, 16), plan.chunk) for slot in slots]
    rows = [jnp.concatenate([last[part, at, :] for at in where], axis=0) for part in range(2)]
    matrix[...] = product(rows, turned)
    for index in range(len(slots)):
        for column in range(plan.cols):
            out[index, pl.ds(column, plan.chunk, stride=plan.cols), :] = matrix[
                index * plan.chunk : (index + 1) * plan.chunk, column * LANES : (column + 1) * LANES
            ]


def backward(plan, slots):
    def kernel(spectra, last, twist, second, out, turned, stack, spread, matrix):
        place = spot(plan)[0]
        rows = plan.rows
        for part in range(2):
            for column in range(plan.half_cols):
                lanes = slice(column * LANES, (column + 1) * LANES)
                for group in range(plan.groups):
                    start = part * rows + group * plan.slice_rows
                    stack[start : start + plan.slice_rows, lanes] = spectra[group, packed_rows(plan, part, column)]
        value = split(stack[...])
        high, low = value
        paired = lambda half: jnp.concatenate(
            [jnp.concatenate([half[:rows], -half[rows:]], axis=1), jnp.concatenate([half[rows:], half[:rows]], axis=1)],
            axis=0,
        )
        spread[...] = product((paired(high), paired(low)), (second[0], second[1]), True)
        middle = jnp.where(place == 0, stack[rows : rows + 1, :1], 0.0)
        spread[:1] = spread[:1] + middle * alternating(plan, 1)
        real, imag = spread[:rows], spread[rows:]
        high, low = split(
            jnp.concatenate([real * twist[0] + imag * twist[1], imag * twist[0] - real * twist[1]], axis=0)
        )
        turned[0], turned[1] = high, low
        into_slots(plan, slots, last, (high, low), out, matrix)

    shape = (
        jax.ShapeDtypeStruct((len(slots), plan.chunk * plan.cols, LANES), jnp.float32),
        jax.ShapeDtypeStruct((2, 2 * plan.rows, plan.side), jnp.bfloat16),
    )
    scratch = [
        pltpu.VMEM((2 * plan.rows, plan.half), jnp.float32),
        pltpu.VMEM((2 * plan.rows, plan.side), jnp.float32),
        pltpu.VMEM((len(slots) * plan.chunk, plan.side), jnp.float32),
    ]
    return call(kernel, shape, ["vmem"] * 4, scratch)


def finish(plan, slots):
    def kernel(last, turned, out, matrix):
        into_slots(plan, slots, last, (turned[0], turned[1]), out, matrix)

    shape = jax.ShapeDtypeStruct((len(slots), plan.chunk * plan.cols, LANES), jnp.float32)
    scratch = [pltpu.VMEM((len(slots) * plan.chunk, plan.side), jnp.float32)]
    return call(kernel, shape, ["vmem"] * 2, scratch)


def swapped(value, bit):
    count = lax.axis_size("acc")
    return lax.ppermute(value, "acc", [(source, source ^ bit) for source in range(count)])


def per_device(reciprocal_spectra, divisor):
    rounds, _, freq_rows, plane = reciprocal_spectra.shape
    quarters = lax.axis_size("acc")
    groups = lax.axis_size("blk") * lax.axis_size("tail")
    plan = Plan(freq_rows, plane, quarters, groups, rounds)
    constants = [jnp.asarray(table) for table in tables(plan)]

    limbs = divisor.reshape(plan.chunk * plan.cols, LANES)
    spectra = reciprocal_spectra.reshape(2 * rounds, freq_rows, plane)
    first, twist, second, near, facing, rim, tail = prepare(plan)(*map(far, constants + [limbs, spectra]))
    bundled, rim = bundle(plan)(near, rim)
    pieces = {0: limbs}
    bit = quarters // 2
    while bit:
        for index, piece in list(pieces.items()):
            pieces[index | bit] = swapped(bundled if bit == 1 and index == 0 else piece, bit)
        bit //= 2
    pieces[0] = near
    facing = opposite(plan)(facing, pieces[1])
    facing = swapped(facing, quarters - 1)
    rides = quarters <= 4
    if not rides:
        rim = lax.ppermute(rim, "acc", [(source, -source % quarters) for source in range(quarters)])
    last, own, edge = resident(plan)(first, far(spectra), rim)

    begun = begin(plan)(*[pieces[index] for index in range(quarters - 1)], first)
    own_spectrum = forward(plan)(pieces[quarters - 1], begun, tail, twist, second)
    own = blend(plan, rides)(own, facing, edge, rim)
    if plan.per > 1:
        first_row = lax.axis_index(("blk", "tail")) % plan.per * plan.slice_rows
        own = lax.dynamic_slice_in_dim(own, first_row, plan.slice_rows, 2)
    every = lax.all_to_all(own_spectrum, ("blk", "tail"), 0, 0, tiled=True)
    sums = combine(plan)(every, own)
    back = lax.all_to_all(sums, ("blk", "tail"), 0, 0, tiled=True)
    first_sent = [index for index in range(quarters) if index & 1 and (index & 2 or quarters == 2)]
    others = [index for index in range(quarters) if index not in first_sent]
    sent, turned = backward(plan, first_sent)(back, last, twist, second)
    arrived = swapped(sent, 1)
    rest = finish(plan, others)(last, turned)
    slot = {index: rest[where] for where, index in enumerate(others)}
    held = {index ^ 1: slot[index ^ 1] + arrived[where] for where, index in enumerate(first_sent)}
    later = [index for index in others if index & 1]
    if later:
        arrived = swapped(jnp.stack([slot[index] for index in later]), 1)
        sums = {index ^ 1: slot[index ^ 1] + arrived[where] for where, index in enumerate(later)}
        held.update(lax.optimization_barrier(sums))
    bit = 2
    while bit < quarters:
        sent = sorted(index for index in held if index & bit)
        arrived = swapped(jnp.stack([held[index] for index in sent]), bit)
        held = {index ^ bit: held[index ^ bit] + arrived[where] for where, index in enumerate(sent)}
        bit *= 2
    return held[0].reshape(divisor.shape)


def solution(mesh):
    in_specs = (P(None, None, "acc", None), P(("blk", "tail"), "acc"))
    out_specs = P(("blk", "tail"), "acc")
    return jax.shard_map(per_device, mesh=mesh, in_specs=in_specs, out_specs=out_specs, check_vma=False)
```

```python
import math

import jax
import jax.numpy as jnp
import numpy as np
from jax import lax
from jax.experimental import pallas as pl
from jax.experimental.pallas import tpu as pltpu
from jax.sharding import PartitionSpec as P


LANES = 128
TILE = 8
PIECES = 2
GRANT = 16 * 1024 * 1024
STRIDE = 2


class Plan:
    def __init__(self, freq_rows, plane, quarters, groups, rounds):
        self.rounds = rounds
        self.quarters = quarters
        self.groups = groups
        self.freq_rows = freq_rows
        self.radix = freq_rows * quarters
        self.length = self.radix * plane
        self.side = math.isqrt(self.length)
        self.half = self.side // 2
        self.m_los = self.side // self.radix
        self.m_his = self.radix // self.m_los
        self.rows = self.m_los * freq_rows
        self.n1s = self.side // 2
        self.chunk = self.n1s // quarters
        self.cols = self.side // LANES
        self.half_cols = self.half // LANES
        self.slice_rows = self.rows // groups
        self.per = groups // self.m_los
        self.packed = 2 * self.half_cols * self.slice_rows


def tables(plan):
    row = (np.arange(plan.m_los)[:, None] * plan.radix + np.arange(plan.freq_rows)[None, :]).reshape(-1)
    part = np.arange(plan.quarters) * plan.freq_rows
    n1 = np.arange(plan.n1s)
    n2 = np.arange(plan.side)
    f2 = (np.arange(plan.m_his)[:, None] + plan.m_los * np.arange(plan.radix // 2)[None, :]).reshape(-1)

    def wave(first, second, modulus):
        angle = (first[:, None] * second[None, :] % modulus) * (-2.0 * math.pi / modulus)
        return np.stack([np.cos(angle), np.sin(angle)])

    first_rows = wave(row, n1, plan.side)
    first_part = wave(part, n1, plan.side)
    twist_rows = wave(row, n2, plan.length)
    twist_part = wave(part, n2, plan.length)
    cosine, sine = wave(n2, f2, plan.side)
    second = np.concatenate([cosine, -sine], axis=1)
    second_high = second.astype(jnp.bfloat16)
    second_low = (second - second_high.astype(np.float64)).astype(jnp.bfloat16)
    single = lambda value: value.astype(np.float32)
    return (
        single(first_rows),
        single(first_part.transpose(1, 0, 2)),
        single(twist_rows),
        single(twist_part.transpose(1, 0, 2)),
        np.stack([second_high, second_low]),
    )


def spot(plan):
    place = lax.axis_index("acc")
    group = lax.axis_index("blk") * lax.axis_size("tail") + lax.axis_index("tail")
    if plan.per == 1:
        return place, group, 0
    return place, lax.div(group, plan.per), lax.rem(group, plan.per) * plan.slice_rows


def rim_m_lo(plan, place, m_lo):
    return jnp.where(place == 0, lax.rem(plan.m_los - m_lo, plan.m_los), plan.m_los - 1 - m_lo)


def far(value):
    return pltpu.with_memory_space_constraint(value, pltpu.HBM)


def split(value):
    high = value.astype(jnp.bfloat16)
    low = (value - high.astype(jnp.float32)).astype(jnp.bfloat16)
    return high, low


def product(first, second, transposed=False):
    dims = (((1,), (1 if transposed else 0,)), ((), ()))
    dot = lambda a, b: lax.dot_general(a, b, dims, preferred_element_type=jnp.float32)
    return dot(first[0], second[0]) + (dot(first[1], second[0]) + dot(first[0], second[1]))


def call(kernel, out_shape, memory, scratch=(), result="vmem", flops=1_000_000, moved=1_000_000):
    where = {"vmem": pltpu.VMEM, "hbm": pltpu.HBM}
    out_spec = pl.BlockSpec(memory_space=where[result])
    return pl.pallas_call(
        kernel,
        out_shape=out_shape,
        in_specs=[pl.BlockSpec(memory_space=where[kind]) for kind in memory],
        out_specs=jax.tree.map(lambda _: out_spec, out_shape),
        scratch_shapes=scratch,
        cost_estimate=pl.CostEstimate(flops=flops, bytes_accessed=moved, transcendentals=0),
        compiler_params=pltpu.CompilerParams(vmem_limit_bytes=GRANT),
    )


def fetch(plan, spectra, held, sems, m_lo, rows):
    copies = []
    for m_hi in range(plan.m_his):
        start = pl.multiple_of((m_hi * plan.m_los + m_lo) * plan.radix // LANES * LANES, LANES)
        source = spectra.at[:, pl.ds(0, rows), pl.ds(start, LANES)]
        copies.append(pltpu.make_async_copy(source, held.at[m_hi], sems.at[m_hi]))
    return copies


def gathered(plan, held, index, column, within, count):
    piece_lanes = plan.radix // 2
    each = LANES // piece_lanes
    lane = lax.broadcasted_iota(jnp.int32, (count, LANES), 1)
    value = jnp.zeros((count, LANES), jnp.float32)
    for piece in range(each):
        tile = held[column * each + piece, index, :count]
        turned = pltpu.roll(tile, (piece * piece_lanes - within + LANES) % LANES, 1)
        value = jnp.where((lane >= piece * piece_lanes) & (lane < (piece + 1) * piece_lanes), turned, value)
    return value


def held_shape(plan, rows):
    return jax.ShapeDtypeStruct((plan.m_his, 2 * plan.rounds, rows, LANES), jnp.float32)


def bundle(plan):
    def kernel(near, held, out, rim):
        place, m_lo, _ = spot(plan)
        within = rim_m_lo(plan, place, m_lo) * plan.radix % LANES + plan.radix // 2
        base = plan.chunk * plan.cols
        out[:base] = near[...]
        for index in range(2 * plan.rounds):
            for column in range(plan.half_cols):
                row = index * plan.half_cols + column
                value = gathered(plan, held, index, column, within, 1)
                out[base + row : base + row + 1] = value
                rim[index : index + 1, column * LANES : (column + 1) * LANES] = value

    shape = jax.ShapeDtypeStruct
    rows = plan.chunk * plan.cols + 2 * plan.rounds * plan.half_cols
    out_shape = (shape((rows, LANES), jnp.float32), shape((2 * plan.rounds, plan.half), jnp.float32))
    return call(kernel, out_shape, ["vmem"] * 2)


def flipped(plan, value):
    row = lax.broadcasted_iota(jnp.int32, (plan.half, plan.half), 0)
    column = lax.broadcasted_iota(jnp.int32, (plan.half, plan.half), 1)
    flip = jnp.where(row + column == plan.half - 1, 1.0, 0.0).astype(jnp.bfloat16)
    high, low = value
    dot = lambda a: jnp.dot(a, flip, preferred_element_type=jnp.float32)
    return dot(high) + dot(low)


def opposite(plan):
    def kernel(held, other, out, stack):
        m_lo = plan.m_los - 1 - spot(plan)[1]
        within = m_lo * plan.radix % LANES + plan.radix // 2
        base = plan.chunk * plan.cols
        rows = plan.freq_rows
        for index in range(2 * plan.rounds):
            for column in range(plan.half_cols):
                lanes = slice(column * LANES, (column + 1) * LANES)
                stack[index * rows : (index + 1) * rows, lanes] = gathered(plan, held, index, column, within, rows)
                row = base + index * plan.half_cols + column
                stack[index * rows : index * rows + 1, lanes] = other[row : row + 1]
        count = 2 * plan.rounds * rows
        row = lax.broadcasted_iota(jnp.int32, (count, count), 0)
        column = lax.broadcasted_iota(jnp.int32, (count, count), 1)
        inside = row % rows
        target = jnp.where(inside == 0, row, 2 * (row - inside) + rows - row)
        turn = jnp.where(column == target, 1.0, 0.0).astype(jnp.bfloat16)
        dot = lambda a: jnp.dot(turn, a, preferred_element_type=jnp.float32).astype(jnp.bfloat16)
        high, low = split(stack[...])
        out[...] = flipped(plan, (dot(high), dot(low))).reshape(out.shape)

    shape = jax.ShapeDtypeStruct((2 * plan.rounds, plan.freq_rows, plan.half), jnp.float32)
    scratch = [pltpu.VMEM((2 * plan.rounds * plan.freq_rows, plan.half), jnp.float32)]
    return call(kernel, shape, ["vmem"] * 2, scratch)


def prepare(plan):
    def kernel(*refs):
        first, twist, second, near, facing, rim, tail = refs[7:14]
        first_rows, first_part, twist_rows, twist_part = refs[14:18]
        sems, facing_sems, rim_sems = refs[18:]
        place, m_lo, _ = spot(plan)
        targets = (first_rows, first_part, twist_rows, twist_part, second, near)
        copies = [
            pltpu.make_async_copy(source, target, sems.at[index])
            for index, (source, target) in enumerate(zip(refs[:6], targets))
        ]
        copies += fetch(plan, refs[6], facing, facing_sems, plan.m_los - 1 - m_lo, plan.freq_rows)
        copies += fetch(plan, refs[6], rim, rim_sems, rim_m_lo(plan, place, m_lo), TILE)
        for copy in copies:
            copy.start()
        copies[0].wait()
        copies[1].wait()
        part_cos = first_part[pl.ds(place, 1), 0, :]
        part_sin = first_part[pl.ds(place, 1), 1, :]
        rows = plan.rows
        start = (place ^ (plan.quarters - 1)) * plan.chunk
        real = first_rows[0] * part_cos - first_rows[1] * part_sin
        imag = first_rows[0] * part_sin + first_rows[1] * part_cos
        for part, value in enumerate((real, imag)):
            some = slice(part * rows, (part + 1) * rows)
            first[0, some], first[1, some] = split(value)
            tail[0, some], tail[1, some] = split(pltpu.roll(value, plan.n1s - start, 1)[:, : plan.chunk])
        copies[2].wait()
        copies[3].wait()
        part_cos = twist_part[pl.ds(place, 1), 0, :]
        part_sin = twist_part[pl.ds(place, 1), 1, :]
        twist[0] = twist_rows[0] * part_cos - twist_rows[1] * part_sin
        twist[1] = twist_rows[0] * part_sin + twist_rows[1] * part_cos
        for copy in copies[4:]:
            copy.wait()

    shape = jax.ShapeDtypeStruct
    out_shape = (
        shape((2, 2 * plan.rows, plan.n1s), jnp.bfloat16),
        shape((2, plan.rows, plan.side), jnp.float32),
        shape((2, plan.side, 2 * plan.half), jnp.bfloat16),
        shape((plan.chunk * plan.cols, LANES), jnp.float32),
        held_shape(plan, plan.freq_rows),
        held_shape(plan, TILE),
        shape((2, 2 * plan.rows, plan.chunk), jnp.bfloat16),
    )
    scratch = [
        pltpu.VMEM((2, plan.rows, plan.n1s), jnp.float32),
        pltpu.VMEM((plan.quarters, 2, plan.n1s), jnp.float32),
        pltpu.VMEM((2, plan.rows, plan.side), jnp.float32),
        pltpu.VMEM((plan.quarters, 2, plan.side), jnp.float32),
        pltpu.SemaphoreType.DMA((6,)),
        pltpu.SemaphoreType.DMA((plan.m_his,)),
        pltpu.SemaphoreType.DMA((plan.m_his,)),
    ]
    return call(kernel, out_shape, ["hbm"] * 7, scratch)


def resident(plan):
    def kernel(first, spectra, rim, last, own, edge, held, sems):
        place, m_lo, _ = spot(plan)
        copies = fetch(plan, spectra, held, sems, m_lo, plan.freq_rows)
        for copy in copies:
            copy.start()
        last[0], last[1] = split((first[0].astype(jnp.float32) + first[1].astype(jnp.float32)).T)
        value = flipped(plan, split(rim[...]))
        lane = lax.broadcasted_iota(jnp.int32, value.shape, 1)
        later = pltpu.roll(value, plan.radix // 2, 1)
        later = jnp.where(lane < plan.radix // 2, pltpu.roll(later, 1, 1), later)
        edge[...] = jnp.where((place == 0) & (m_lo == 0), later, value)
        for copy in copies:
            copy.wait()
        within = m_lo * plan.radix % LANES
        for index in range(2 * plan.rounds):
            for column in range(plan.half_cols):
                own[index, column] = gathered(plan, held, index, column, within, plan.freq_rows)

    shape = jax.ShapeDtypeStruct
    out_shape = (
        shape((2, plan.n1s, 2 * plan.rows), jnp.bfloat16),
        shape((2 * plan.rounds, plan.half_cols, plan.freq_rows, LANES), jnp.float32),
        shape((2 * plan.rounds, plan.half), jnp.float32),
    )
    held = held_shape(plan, plan.freq_rows)
    scratch = [pltpu.VMEM(held.shape, held.dtype), pltpu.SemaphoreType.DMA((plan.m_his,))]
    return call(kernel, out_shape, ["vmem", "hbm", "vmem"], scratch)


def blend(plan, rides):
    def kernel(own, arrived, edge, rim, out):
        place, m_lo, _ = spot(plan)
        corner = lax.broadcasted_iota(jnp.int32, (plan.freq_rows, LANES), 0)
        top = corner == 0
        corner = top & (lax.broadcasted_iota(jnp.int32, (plan.freq_rows, LANES), 1) == 0)
        corner = corner & ((place == 0) & (m_lo == 0))
        if rides:
            top = top & (lax.rem(place, 2) == 0)
        scale = 1.0 / plan.length
        for step in range(plan.rounds):
            for column in range(plan.half_cols):
                lanes = slice(column * LANES, (column + 1) * LANES)
                whole = []
                for part in range(2):
                    index = 2 * step + part
                    there = jnp.where(top, edge[index : index + 1, lanes], arrived[index, :, lanes])
                    here = own[index, column]
                    if column == 0:
                        there = jnp.where(corner, here if part else 0.0, there)
                    whole.append((here - there if part else here + there) * scale)
                out[3 * step, column] = whole[0]
                out[3 * step + 1, column] = whole[1]
                if column == 0:
                    whole[0] = jnp.where(corner, rim[2 * step : 2 * step + 1, lanes] * scale, whole[0])
                out[3 * step + 2, column] = whole[0]

    shape = jax.ShapeDtypeStruct((3 * plan.rounds, plan.half_cols, plan.freq_rows, LANES), jnp.float32)
    return call(kernel, shape, ["vmem"] * 4)


def alternating(plan, count):
    lane = lax.broadcasted_iota(jnp.int32, (count, plan.side), 1)
    return jnp.where(lane % 2 == 0, 1.0, -1.0)


def packed_rows(plan, part, column):
    start = (part * plan.half_cols + column) * plan.slice_rows
    return slice(start, start + plan.slice_rows)


def begin(plan):
    def kernel(*refs):
        limbs = refs[: plan.quarters - 1]
        first, out, matrix = refs[plan.quarters - 1 :]
        place = spot(plan)[0]
        for index in range(plan.quarters):
            start = pl.multiple_of((place ^ index) * plan.chunk, 8)
            for column in range(plan.cols):
                lanes = slice(column * LANES, (column + 1) * LANES)
                if index < plan.quarters - 1:
                    value = limbs[index][pl.ds(column, plan.chunk, stride=plan.cols), :]
                else:
                    value = jnp.zeros((plan.chunk, LANES), jnp.float32)
                matrix[pl.ds(start, plan.chunk), lanes] = value
        out[...] = product((first[0], first[1]), split(matrix[...]))

    shape = jax.ShapeDtypeStruct((2 * plan.rows, plan.side), jnp.float32)
    scratch = [pltpu.VMEM((plan.n1s, plan.side), jnp.float32)]
    return call(kernel, shape, ["vmem"] * plan.quarters, scratch)


def forward(plan):
    def kernel(limbs, begun, tail, twist, second, out, matrix, turned, packed, sems):
        place = spot(plan)[0]
        for column in range(plan.cols):
            rows = pl.ds(column, plan.chunk, stride=plan.cols)
            matrix[:, column * LANES : (column + 1) * LANES] = limbs[rows, :]
        value = begun[...] + product((tail[0], tail[1]), split(matrix[...]))
        rows = plan.rows
        real, imag = value[:rows], value[rows:]
        turned[:rows] = real * twist[0] - imag * twist[1]
        turned[rows:] = real * twist[1] + imag * twist[0]
        middle = jnp.sum(turned[:1] * alternating(plan, 1), axis=1, keepdims=True)
        middle = jnp.where(place == 0, middle, 0.0)
        corner = lax.broadcasted_iota(jnp.int32, (plan.slice_rows, LANES), 0) == 0
        corner = corner & (lax.broadcasted_iota(jnp.int32, (plan.slice_rows, LANES), 1) == 0)
        table = (second[0], second[1])
        count, groups = rows // PIECES, plan.groups // PIECES
        copies = []
        for piece in range(PIECES):
            start = piece * count
            both = jnp.concatenate([turned[start : start + count], turned[rows + start : rows + start + count]], axis=0)
            value = product(split(both), table)
            by_cos, by_sin = value[:, : plan.half], value[:, plan.half :]
            main = (by_cos[:count] + by_sin[count:], by_cos[count:] - by_sin[:count])
            for index in range(groups):
                group = piece * groups + index
                for part in range(2):
                    for column in range(plan.half_cols):
                        lanes = slice(column * LANES, (column + 1) * LANES)
                        tile = main[part][index * plan.slice_rows : (index + 1) * plan.slice_rows, lanes]
                        if (group, part, column) == (0, 1, 0):
                            tile = tile + jnp.where(corner, middle, 0.0)
                        packed[group, packed_rows(plan, part, column)] = tile
            where = pl.ds(piece * groups, groups)
            copies.append(pltpu.make_async_copy(packed.at[where], out.at[where], sems.at[piece]))
            copies[-1].start()
        for copy in copies:
            copy.wait()

    shape = jax.ShapeDtypeStruct((plan.groups, plan.packed, LANES), jnp.float32)
    scratch = [
        pltpu.VMEM((plan.chunk, plan.side), jnp.float32),
        pltpu.VMEM((2 * plan.rows, plan.side), jnp.float32),
        pltpu.VMEM((plan.groups, plan.packed, LANES), jnp.float32),
        pltpu.SemaphoreType.DMA((PIECES,)),
    ]
    return call(kernel, shape, ["vmem"] * 5, scratch, "hbm")


def combine(plan):
    def kernel(spectra, own, out):
        place, _, first_row = spot(plan)
        row = lax.broadcasted_iota(jnp.int32, (plan.slice_rows, LANES), 0) + first_row + place * plan.freq_rows
        sign = jnp.where(row % 2 == 0, 1.0, -1.0)

        def one_block(block, carry):
            sums = [jnp.zeros((plan.slice_rows, LANES), jnp.float32) for _ in range(2 * plan.half_cols)]
            for step in range(plan.rounds):
                here = lax.rem(block + (plan.rounds * STRIDE * plan.groups - step * STRIDE), plan.groups)
                before = lax.rem(here + (plan.groups - 1), plan.groups)
                for column in range(plan.half_cols):
                    real, imag = (
                        spectra[here, packed_rows(plan, part, column)]
                        + sign * spectra[before, packed_rows(plan, part, column)]
                        for part in range(2)
                    )
                    own_r, own_i, own_c = (own[3 * step + part, column] for part in range(3))
                    sums[column] = sums[column] + own_r * real - own_i * imag
                    sums[plan.half_cols + column] = sums[plan.half_cols + column] + own_c * imag + own_i * real
            for part in range(2):
                for column in range(plan.half_cols):
                    out[block, packed_rows(plan, part, column)] = sums[part * plan.half_cols + column]
            return carry

        lax.fori_loop(0, plan.groups, one_block, 0, unroll=8)

    shape = jax.ShapeDtypeStruct((plan.groups, plan.packed, LANES), jnp.float32)
    return call(kernel, shape, ["vmem"] * 2)


def into_slots(plan, slots, last, turned, out, matrix):
    place = spot(plan)[0]
    where = [pl.ds(pl.multiple_of((place ^ slot) * plan.chunk, 16), plan.chunk) for slot in slots]
    rows = [jnp.concatenate([last[part, at, :] for at in where], axis=0) for part in range(2)]
    matrix[...] = product(rows, turned)
    for index in range(len(slots)):
        for column in range(plan.cols):
            out[index, pl.ds(column, plan.chunk, stride=plan.cols), :] = matrix[
                index * plan.chunk : (index + 1) * plan.chunk, column * LANES : (column + 1) * LANES
            ]


def backward(plan, slots):
    def kernel(spectra, last, twist, second, out, turned, stack, spread, matrix):
        place = spot(plan)[0]
        rows = plan.rows
        for part in range(2):
            for column in range(plan.half_cols):
                lanes = slice(column * LANES, (column + 1) * LANES)
                for group in range(plan.groups):
                    start = part * rows + group * plan.slice_rows
                    stack[start : start + plan.slice_rows, lanes] = spectra[group, packed_rows(plan, part, column)]
        value = split(stack[...])
        by_cos = product(value, (second[0, :, : plan.half], second[1, :, : plan.half]), True)
        by_sin = product(value, (second[0, :, plan.half :], second[1, :, plan.half :]), True)
        spread[:rows] = by_cos[:rows] - by_sin[rows:]
        spread[rows:] = by_cos[rows:] + by_sin[:rows]
        middle = jnp.where(place == 0, stack[rows : rows + 1, :1], 0.0)
        spread[:1] = spread[:1] + middle * alternating(plan, 1)
        real, imag = spread[:rows], spread[rows:]
        high, low = split(
            jnp.concatenate([real * twist[0] + imag * twist[1], imag * twist[0] - real * twist[1]], axis=0)
        )
        turned[0], turned[1] = high, low
        into_slots(plan, slots, last, (high, low), out, matrix)

    shape = (
        jax.ShapeDtypeStruct((len(slots), plan.chunk * plan.cols, LANES), jnp.float32),
        jax.ShapeDtypeStruct((2, 2 * plan.rows, plan.side), jnp.bfloat16),
    )
    scratch = [
        pltpu.VMEM((2 * plan.rows, plan.half), jnp.float32),
        pltpu.VMEM((2 * plan.rows, plan.side), jnp.float32),
        pltpu.VMEM((len(slots) * plan.chunk, plan.side), jnp.float32),
    ]
    return call(kernel, shape, ["vmem"] * 4, scratch)


def finish(plan, slots):
    def kernel(last, turned, out, matrix):
        into_slots(plan, slots, last, (turned[0], turned[1]), out, matrix)

    shape = jax.ShapeDtypeStruct((len(slots), plan.chunk * plan.cols, LANES), jnp.float32)
    scratch = [pltpu.VMEM((len(slots) * plan.chunk, plan.side), jnp.float32)]
    return call(kernel, shape, ["vmem"] * 2, scratch)


def swapped(value, bit):
    count = lax.axis_size("acc")
    return lax.ppermute(value, "acc", [(source, source ^ bit) for source in range(count)])


def per_device(reciprocal_spectra, divisor):
    rounds, _, freq_rows, plane = reciprocal_spectra.shape
    quarters = lax.axis_size("acc")
    groups = lax.axis_size("blk") * lax.axis_size("tail")
    plan = Plan(freq_rows, plane, quarters, groups, rounds)
    constants = [jnp.asarray(table) for table in tables(plan)]

    limbs = divisor.reshape(plan.chunk * plan.cols, LANES)
    spectra = reciprocal_spectra.reshape(2 * rounds, freq_rows, plane)
    first, twist, second, near, facing, rim, tail = prepare(plan)(*map(far, constants + [limbs, spectra]))
    bundled, rim = bundle(plan)(near, rim)
    pieces = {0: limbs}
    bit = quarters // 2
    while bit:
        for index, piece in list(pieces.items()):
            pieces[index | bit] = swapped(bundled if bit == 1 and index == 0 else piece, bit)
        bit //= 2
    pieces[0] = near
    facing = opposite(plan)(facing, pieces[1])
    facing = swapped(facing, quarters - 1)
    rides = quarters <= 4
    if not rides:
        rim = lax.ppermute(rim, "acc", [(source, -source % quarters) for source in range(quarters)])
    last, own, edge = resident(plan)(first, far(spectra), rim)

    begun = begin(plan)(*[pieces[index] for index in range(quarters - 1)], first)
    own_spectrum = forward(plan)(pieces[quarters - 1], begun, tail, twist, second)
    own = blend(plan, rides)(own, facing, edge, rim)
    if plan.per > 1:
        first_row = lax.axis_index(("blk", "tail")) % plan.per * plan.slice_rows
        own = lax.dynamic_slice_in_dim(own, first_row, plan.slice_rows, 2)
    every = lax.all_to_all(own_spectrum, ("blk", "tail"), 0, 0, tiled=True)
    sums = combine(plan)(every, own)
    back = lax.all_to_all(sums, ("blk", "tail"), 0, 0, tiled=True)
    first_sent = [index for index in range(quarters) if index & 1 and (index & 2 or quarters == 2)]
    others = [index for index in range(quarters) if index not in first_sent]
    sent, turned = backward(plan, first_sent)(back, last, twist, second)
    arrived = swapped(sent, 1)
    rest = finish(plan, others)(last, turned)
    slot = {index: rest[where] for where, index in enumerate(others)}
    held = {index ^ 1: slot[index ^ 1] + arrived[where] for where, index in enumerate(first_sent)}
    later = [index for index in others if index & 1]
    if later:
        arrived = swapped(jnp.stack([slot[index] for index in later]), 1)
        sums = {index ^ 1: slot[index ^ 1] + arrived[where] for where, index in enumerate(later)}
        held.update(lax.optimization_barrier(sums))
    bit = 2
    while bit < quarters:
        sent = sorted(index for index in held if index & bit)
        arrived = swapped(jnp.stack([held[index] for index in sent]), bit)
        held = {index ^ bit: held[index ^ bit] + arrived[where] for where, index in enumerate(sent)}
        bit *= 2
    return held[0].reshape(divisor.shape)


def solution(mesh):
    in_specs = (P(None, None, "acc", None), P(("blk", "tail"), "acc"))
    out_specs = P(("blk", "tail"), "acc")
    return jax.shard_map(per_device, mesh=mesh, in_specs=in_specs, out_specs=out_specs, check_vma=False)
```
